8 devices in a mesh: dp: 1 (over z), tp: 2 (over y), ep: 4 (over x, core).
Axes of the slice: x: 2, y: 2, z: 1, core: 2. Of those that a mesh axis runs over, the one named last changes fastest.
Arguments:
- tokens: bfloat16 [8192, 768], P(('dp', 'ep'))
- grad_out: bfloat16 [8192, 768], P(('dp', 'ep'))
- w_router: bfloat16 [768, 8], replicated
- w_in: bfloat16 [8, 768, 3072], P('ep', None, 'tp')
- w_out: bfloat16 [8, 3072, 768], P('ep', 'tp')
- expert_ids: int32 [8192], P(('dp', 'ep'))
Outputs:
- output 1: bfloat16 [8192, 768], P(('dp', 'ep'))
- output 2: bfloat16 [8192, 768], P(('dp', 'ep'))
- output 3: float32 [8, 768, 3072], P(('dp', 'ep'), None, 'tp')
- output 4: float32 [8, 3072, 768], P(('dp', 'ep'), 'tp')
- output 5: float32 [768, 8], P('dp')
All inputs are finite; a program needn't handle non-finite values.
Results may differ from the reference program's by a relative error of at most 0.00617232.
Values are sent between devices in bfloat16 or wider.
A program may use at most 1 GiB of HBM per device.

```python
import jax
import jax.numpy as jnp
from jax import lax

D_MODEL = 768
D_FF = 3072
EXPERTS = 8
TOKENS_DEV = 2048
EP_RANKS = 4

CAPACITY = (6 * TOKENS_DEV + 5 * EXPERTS - 1) // (5 * EXPERTS)
N_TOKENS = EP_RANKS * TOKENS_DEV
N_SLOTS = EXPERTS * CAPACITY


def draw_routes(route_key):
    key_hot, key_order, key_rest = jax.random.split(route_key, 3)
    hot_expert = jax.random.randint(key_hot, (EP_RANKS, 1), 0, EXPERTS)
    rest_ids = jax.random.randint(key_rest, (EP_RANKS, TOKENS_DEV), 0, EXPERTS)
    order_keys = jax.random.split(key_order, EP_RANKS)
    rank_of = jax.vmap(lambda one_key: jax.random.permutation(one_key, TOKENS_DEV))(order_keys)
    hot_count = CAPACITY + CAPACITY // 2 + 1
    cover_ids = (rank_of - hot_count) % EXPERTS
    route_ids = jnp.where(rank_of < hot_count, hot_expert, jnp.where(rank_of < hot_count + EXPERTS, cover_ids, rest_ids))
    return route_ids.reshape(N_TOKENS).astype(jnp.int32)


def setup_inputs(seed: int = 0, part: int = 0) -> dict:
    part_key = jax.random.fold_in(jax.random.key(seed), part)
    rand_keys = jax.random.split(part_key, 3)
    weight_keys = jax.random.split(jax.random.key(seed + 1), 3)
    tokens = jax.random.normal(rand_keys[0], (N_TOKENS, D_MODEL), jnp.float32)
    grad_out = jax.random.normal(rand_keys[1], (N_TOKENS, D_MODEL), jnp.float32)
    w_router = jax.random.normal(weight_keys[0], (D_MODEL, EXPERTS), jnp.float32) * D_MODEL ** -0.5
    w_in = jax.random.normal(weight_keys[1], (EXPERTS, D_MODEL, D_FF), jnp.float32) * D_MODEL ** -0.5
    w_out = jax.random.normal(weight_keys[2], (EXPERTS, D_FF, D_MODEL), jnp.float32) * D_FF ** -0.5
    return {
        "tokens": tokens.astype(jnp.bfloat16),
        "grad_out": grad_out.astype(jnp.bfloat16),
        "w_router": w_router.astype(jnp.bfloat16),
        "w_in": w_in.astype(jnp.bfloat16),
        "w_out": w_out.astype(jnp.bfloat16),
        "expert_ids": draw_routes(rand_keys[2]),
    }


def dispatch(rows, slot_index):
    slot_buf = jnp.zeros((N_SLOTS + 1, D_MODEL), rows.dtype).at[slot_index].set(rows)
    return slot_buf[:N_SLOTS]


def combine(slot_buf, slot_index):
    padded = jnp.concatenate([slot_buf, jnp.zeros((1, D_MODEL), slot_buf.dtype)], axis=0)
    return jnp.take(padded, slot_index, axis=0)


def by_expert(source_bufs):
    return source_bufs.reshape(EP_RANKS, EXPERTS, CAPACITY, D_MODEL).transpose(1, 0, 2, 3).reshape(EXPERTS, EP_RANKS * CAPACITY, D_MODEL)


def by_source(expert_bufs):
    return expert_bufs.reshape(EXPERTS, EP_RANKS, CAPACITY, D_MODEL).transpose(1, 0, 2, 3).reshape(EP_RANKS, N_SLOTS, D_MODEL)


def expert_step(operands):
    slot_rows, dy_rows, w_in_e, w_out_e = operands
    pre_act = jnp.dot(slot_rows, w_in_e, preferred_element_type=jnp.float32)
    act_val, act_vjp = jax.vjp(jax.nn.gelu, pre_act)
    hidden = act_val.astype(jnp.bfloat16)
    y_rows = jnp.dot(hidden, w_out_e, preferred_element_type=jnp.float32).astype(jnp.bfloat16)
    d_hidden = jnp.dot(dy_rows, w_out_e.T, preferred_element_type=jnp.float32)
    d_pre = act_vjp(d_hidden)[0].astype(jnp.bfloat16)
    grad_out_e = jnp.dot(hidden.T, dy_rows, preferred_element_type=jnp.float32)
    grad_in_e = jnp.dot(slot_rows.T, d_pre, preferred_element_type=jnp.float32)
    d_slot = jnp.dot(d_pre, w_in_e.T, preferred_element_type=jnp.float32).astype(jnp.bfloat16)
    return y_rows, d_slot, grad_in_e, grad_out_e


def reference(tokens, grad_out, w_router, w_in, w_out, expert_ids):
    route_ids = expert_ids.reshape(EP_RANKS, TOKENS_DEV)
    one_hot = (route_ids[:, :, None] == jnp.arange(EXPERTS)[None, None, :]).astype(jnp.int32)
    position = jnp.sum(jnp.cumsum(one_hot, axis=1) * one_hot, axis=2) - 1
    slot_index = jnp.where(position < CAPACITY, route_ids * CAPACITY + position, N_SLOTS)
    chosen = expert_ids[:, None] == jnp.arange(EXPERTS)[None, :]
    logits = jnp.dot(tokens, w_router, preferred_element_type=jnp.float32)
    router_prob = jax.nn.softmax(logits, axis=-1)
    gate_prob = jnp.sum(jnp.where(chosen, router_prob, 0.0), axis=1)
    dy_tok = (gate_prob[:, None] * grad_out.astype(jnp.float32)).astype(jnp.bfloat16)
    slot_rows = jax.vmap(dispatch)(tokens.reshape(EP_RANKS, TOKENS_DEV, D_MODEL), slot_index)
    dy_rows = jax.vmap(dispatch)(dy_tok.reshape(EP_RANKS, TOKENS_DEV, D_MODEL), slot_index)
    y_rows, d_slot, grad_w_in, grad_w_out = lax.map(expert_step, (by_expert(slot_rows), by_expert(dy_rows), w_in, w_out))
    y_tok = jax.vmap(combine)(by_source(y_rows), slot_index).reshape(N_TOKENS, D_MODEL)
    dx_moe = jax.vmap(combine)(by_source(d_slot), slot_index).reshape(N_TOKENS, D_MODEL)
    moe_out = (gate_prob[:, None] * y_tok.astype(jnp.float32)).astype(jnp.bfloat16)
    d_gate = jnp.sum(grad_out.astype(jnp.float32) * y_tok.astype(jnp.float32), axis=1)
    d_logits = (d_gate[:, None] * router_prob * (chosen.astype(jnp.float32) - gate_prob[:, None])).astype(jnp.bfloat16)
    router_grad = jnp.dot(d_logits, w_router.T, preferred_element_type=jnp.float32)
    grad_tokens = (dx_moe.astype(jnp.float32) + router_grad).astype(jnp.bfloat16)
    grad_w_router = jnp.dot(tokens.T, d_logits, preferred_element_type=jnp.float32)
    return moe_out, grad_tokens, grad_w_in, grad_w_out, grad_w_router
```

```python
import functools

import jax
import jax.numpy as jnp
from jax import lax
from jax.experimental import pallas as pl
from jax.experimental.pallas import tpu as pltpu
from jax.sharding import PartitionSpec as P


GELU_C = 0.7978845608028654
GELU_K = 0.044715
BF16 = jnp.bfloat16
F32 = jnp.float32
VMEM_LIMIT = 56 * 2**20


def nn(a, b):
    return jnp.dot(a, b, preferred_element_type=F32)


def nt(a, b):
    return lax.dot_general(a, b, (((1,), (1,)), ((), ())), preferred_element_type=F32)


def tn(a, b):
    return lax.dot_general(a, b, (((0,), (0,)), ((), ())), preferred_element_type=F32)


def gelu_and_slope(a):
    sq = a * a
    th = jnp.tanh(GELU_C * a * (1.0 + GELU_K * sq))
    cdf = 0.5 * (1.0 + th)
    slope = cdf + (0.5 * GELU_C) * a * (1.0 - th * th) * (1.0 + 3.0 * GELU_K * sq)
    return a * cdf, slope


def params(dims, **kw):
    return pltpu.CompilerParams(dimension_semantics=("arbitrary",) * dims, vmem_limit_bytes=VMEM_LIMIT, **kw)


def dispatch_rows(meta, slot_row, rows, first, count, cap):
    n_tok, d_model = rows.shape

    def body(meta_ref, slot_ref, rows_ref, out_ref):
        dest = jnp.bitwise_xor(meta_ref[1], first + pl.program_id(0))
        base = (dest * 2 + pl.program_id(1)) * cap
        codes = lax.broadcasted_iota(jnp.int32, (cap, n_tok), 0) + base
        pick = jnp.where(slot_ref[...] == codes, 1.0, 0.0).astype(BF16)
        out_ref[0, 0] = nn(pick, rows_ref[...]).astype(BF16)

    return pl.pallas_call(
        body,
        grid_spec=pltpu.PrefetchScalarGridSpec(
            num_scalar_prefetch=1,
            grid=(count, 2),
            in_specs=[
                pl.BlockSpec((1, n_tok), lambda d, k, m: (0, 0)),
                pl.BlockSpec((n_tok, d_model), lambda d, k, m: (0, 0)),
            ],
            out_specs=pl.BlockSpec((1, 1, cap, d_model), lambda d, k, m: (d, k, 0, 0)),
        ),
        out_shape=jax.ShapeDtypeStruct((count, 2, cap, d_model), BF16),
        compiler_params=params(2),
        cost_estimate=pl.CostEstimate(flops=4 * count * cap * n_tok * d_model, bytes_accessed=8 * 2**20, transcendentals=0),
        name="dispatch",
    )(meta, slot_row, rows)


def own_half(meta, xs, dys, w_in, w_out, cap, chunk):
    _, d_model, width = w_in.shape
    rows = 2 * cap
    steps = width // chunk

    def body(meta_ref, xa, xb, dya, dyb, wi, wo, h_ref, da_ref, y_ref, s_ref, x_ref, dy_ref):
        j, c = pl.program_id(0), pl.program_id(1)

        @pl.when(c == 0)
        def _():
            x_ref[0, :cap] = xa[0]
            x_ref[0, cap:] = xb[0]
            dy_ref[0, :cap] = dya[0]
            dy_ref[0, cap:] = dyb[0]

        a = nn(x_ref[0], wi[0])
        dh = nt(dy_ref[0], wo[0])
        act, slope = gelu_and_slope(a)
        h = act.astype(BF16)
        da = (dh * slope).astype(BF16)
        h_ref[0] = h
        da_ref[0] = da

        @pl.when(jnp.logical_and(j == 0, c == 0))
        def _():
            y_ref[...] = nn(h, wo[0])
            s_ref[...] = nt(da, wi[0])

        @pl.when(jnp.logical_and(j == 0, c > 0))
        def _():
            y_ref[...] += nn(h, wo[0])
            s_ref[...] += nt(da, wi[0])

    def pick(j, m):
        return jnp.bitwise_xor(m[0], j)

    row_in = pl.BlockSpec((1, cap, d_model), lambda j, c, m: (pick(j, m), 0, 0))
    full = pl.BlockSpec((rows, d_model), lambda j, c, m: (0, 0))
    row_out = pl.BlockSpec((1, rows, d_model), lambda j, c, m: (pick(j, m), 0, 0))
    hid = pl.BlockSpec((1, rows, chunk), lambda j, c, m: (pick(j, m), 0, c))
    return pl.pallas_call(
        body,
        grid_spec=pltpu.PrefetchScalarGridSpec(
            num_scalar_prefetch=1,
            grid=(2, steps),
            in_specs=[
                row_in,
                row_in,
                row_in,
                row_in,
                pl.BlockSpec((1, d_model, chunk), lambda j, c, m: (pick(j, m), 0, c)),
                pl.BlockSpec((1, chunk, d_model), lambda j, c, m: (pick(j, m), c, 0)),
            ],
            out_specs=[hid, hid, full, full, row_out, row_out],
        ),
        out_shape=[
            jax.ShapeDtypeStruct((2, rows, width), BF16),
            jax.ShapeDtypeStruct((2, rows, width), BF16),
            jax.ShapeDtypeStruct((rows, d_model), F32),
            jax.ShapeDtypeStruct((rows, d_model), F32),
            jax.ShapeDtypeStruct((2, rows, d_model), BF16),
            jax.ShapeDtypeStruct((2, rows, d_model), BF16),
        ],
        compiler_params=params(2),
        cost_estimate=pl.CostEstimate(flops=12 * rows * width * d_model, bytes_accessed=36 * 2**20, transcendentals=0),
        name="own_half",
    )(meta, xs[0], xs[1], dys[0], dys[1], w_in, w_out)


def other_half(meta, x, dy, wi_far, wo_far, y_own, s_own, cap, chunk):
    d_model, width = wi_far.shape
    rows = 2 * cap
    steps = width // chunk

    def body(meta_ref, x_ref, dy_ref, wi, wo, y0, s0, ya, yb, sa, sb, y_acc, s_acc):
        c = pl.program_id(0)
        a = nn(x_ref[0], wi[...])
        dh = nt(dy_ref[0], wo[...])
        act, slope = gelu_and_slope(a)
        h = act.astype(BF16)
        da = (dh * slope).astype(BF16)
        y_new = nn(h, wo[...])
        s_new = nt(da, wi[...])

        @pl.when(c == 0)
        def _():
            y_acc[...] = y0[...] + y_new
            s_acc[...] = s0[...] + s_new

        @pl.when(c > 0)
        def _():
            y_acc[...] += y_new
            s_acc[...] += s_new

        @pl.when(c == steps - 1)
        def _():
            ya[...] = y_acc[:cap].astype(BF16)
            yb[...] = y_acc[cap:].astype(BF16)
            sa[...] = s_acc[:cap].astype(BF16)
            sb[...] = s_acc[cap:].astype(BF16)

    row_in = pl.BlockSpec((1, rows, d_model), lambda c, m: (m[0], 0, 0))
    full = pl.BlockSpec((rows, d_model), lambda c, m: (0, 0))
    part = pl.BlockSpec((cap, d_model), lambda c, m: (0, 0))
    return pl.pallas_call(
        body,
        grid_spec=pltpu.PrefetchScalarGridSpec(
            num_scalar_prefetch=1,
            grid=(steps,),
            in_specs=[
                row_in,
                row_in,
                pl.BlockSpec((d_model, chunk), lambda c, m: (0, c)),
                pl.BlockSpec((chunk, d_model), lambda c, m: (c, 0)),
                full,
                full,
            ],
            out_specs=[part] * 4,
            scratch_shapes=[pltpu.VMEM((rows, d_model), F32)] * 2,
        ),
        out_shape=[jax.ShapeDtypeStruct((cap, d_model), BF16)] * 4,
        compiler_params=params(1),
        cost_estimate=pl.CostEstimate(flops=8 * rows * width * d_model, bytes_accessed=16 * 2**20, transcendentals=0),
        name="other_half",
    )(meta, x, dy, wi_far, wo_far, y_own, s_own)


def weight_grads(near, far, chunk):
    x, dy, h, da = near
    _, rows, d_model = x.shape
    width = h.shape[2]

    def body(x0, x1, dy0, dy1, h0, h1, da0, da1, gi, go):
        gi[0] = tn(x0[0], da0[0]) + tn(x1[0], da1[0])
        go[0] = tn(h0[0], dy0[0]) + tn(h1[0], dy1[0])

    row_in = pl.BlockSpec((1, rows, d_model), lambda e, c: (e, 0, 0))
    hid = pl.BlockSpec((1, rows, chunk), lambda e, c: (e, 0, c))
    return pl.pallas_call(
        body,
        grid=(2, width // chunk),
        in_specs=[row_in] * 4 + [hid] * 4,
        out_specs=[
            pl.BlockSpec((1, d_model, chunk), lambda e, c: (e, 0, c)),
            pl.BlockSpec((1, chunk, d_model), lambda e, c: (e, c, 0)),
        ],
        out_shape=[
            jax.ShapeDtypeStruct((2, d_model, width), F32),
            jax.ShapeDtypeStruct((2, width, d_model), F32),
        ],
        compiler_params=params(2),
        cost_estimate=pl.CostEstimate(flops=16 * rows * width * d_model, bytes_accessed=50 * 2**20, transcendentals=0),
        name="weight_grads",
    )(x, far[0], dy, far[1], h, far[2], da, far[3])


def combine_y(pieces, slot_col, codes, ids_col, prob, tokens, grad_out, block):
    n_tok, d_model = tokens.shape
    cap = pieces[0].shape[0]
    n_experts = prob.shape[1]
    slots = cap * len(pieces)

    def body(*refs):
        parts = refs[: len(pieces)]
        slot_ref, codes_ref, ids_ref, prob_ref, x_ref, gy_ref, out_ref, dlog_ref, dwg_ref, all_rows = refs[len(pieces) :]

        @pl.when(pl.program_id(0) == 0)
        def _():
            for p, part in enumerate(parts):
                all_rows[p * cap : (p + 1) * cap, :] = part[...]

        pick = jnp.where(slot_ref[...] == codes_ref[...], 1.0, 0.0).astype(BF16)
        y = nn(pick, all_rows[...])
        prob_v = prob_ref[...]
        hot = ids_ref[...] == lax.broadcasted_iota(jnp.int32, prob_v.shape, 1)
        gate = jnp.sum(jnp.where(hot, prob_v, 0.0), axis=1, keepdims=True)
        out_ref[...] = (gate * y).astype(BF16)
        d_gate = jnp.sum(gy_ref[...].astype(F32) * y, axis=1, keepdims=True)
        dlog = (d_gate * prob_v * (jnp.where(hot, 1.0, 0.0) - gate)).astype(BF16)
        dlog_ref[...] = dlog
        dwg = tn(dlog, x_ref[...])

        @pl.when(pl.program_id(0) == 0)
        def _():
            dwg_ref[...] = dwg

        @pl.when(pl.program_id(0) > 0)
        def _():
            dwg_ref[...] += dwg

    tok = pl.BlockSpec((block, d_model), lambda b: (b, 0))
    return pl.pallas_call(
        body,
        grid=(n_tok // block,),
        in_specs=[pl.BlockSpec((cap, d_model), lambda b: (0, 0))] * len(pieces)
        + [
            pl.BlockSpec((block, 1), lambda b: (b, 0)),
            pl.BlockSpec((1, slots), lambda b: (0, 0)),
            pl.BlockSpec((block, 1), lambda b: (b, 0)),
            pl.BlockSpec((block, n_experts), lambda b: (b, 0)),
            tok,
            tok,
        ],
        out_specs=[
            tok,
            pl.BlockSpec((block, n_experts), lambda b: (b, 0)),
            pl.BlockSpec((n_experts, d_model), lambda b: (0, 0)),
        ],
        out_shape=[
            jax.ShapeDtypeStruct((n_tok, d_model), BF16),
            jax.ShapeDtypeStruct((n_tok, n_experts), BF16),
            jax.ShapeDtypeStruct((n_experts, d_model), F32),
        ],
        scratch_shapes=[pltpu.VMEM((slots, d_model), BF16)],
        compiler_params=params(1),
        cost_estimate=pl.CostEstimate(flops=2 * n_tok * slots * d_model, bytes_accessed=16 * 2**20, transcendentals=0),
        name="combine_y",
    )(*pieces, slot_col, codes, ids_col, prob, tokens, grad_out)


def combine_s(pieces, slot_col, codes, dlog, w_router, block):
    n_tok = slot_col.shape[0]
    cap, d_model = pieces[0].shape
    n_experts = dlog.shape[1]
    slots = cap * len(pieces)

    def body(*refs):
        parts = refs[: len(pieces)]
        slot_ref, codes_ref, dlog_ref, wg_ref, dx_ref, all_rows = refs[len(pieces) :]

        @pl.when(pl.program_id(0) == 0)
        def _():
            for p, part in enumerate(parts):
                all_rows[p * cap : (p + 1) * cap, :] = part[...]

        pick = jnp.where(slot_ref[...] == codes_ref[...], 1.0, 0.0).astype(BF16)
        s = nn(pick, all_rows[...])
        dx_ref[...] = (s + nt(dlog_ref[...], wg_ref[...])).astype(BF16)

    return pl.pallas_call(
        body,
        grid=(n_tok // block,),
        in_specs=[pl.BlockSpec((cap, d_model), lambda b: (0, 0))] * len(pieces)
        + [
            pl.BlockSpec((block, 1), lambda b: (b, 0)),
            pl.BlockSpec((1, slots), lambda b: (0, 0)),
            pl.BlockSpec((block, n_experts), lambda b: (b, 0)),
            pl.BlockSpec((d_model, n_experts), lambda b: (0, 0)),
        ],
        out_specs=pl.BlockSpec((block, d_model), lambda b: (b, 0)),
        out_shape=jax.ShapeDtypeStruct((n_tok, d_model), BF16),
        scratch_shapes=[pltpu.VMEM((slots, d_model), BF16)],
        compiler_params=params(1),
        cost_estimate=pl.CostEstimate(flops=2 * n_tok * slots * d_model, bytes_accessed=10 * 2**20, transcendentals=0),
        name="combine_s",
    )(*pieces, slot_col, codes, dlog, w_router)


def solution(mesh):
    ep_size = mesh.shape["ep"]
    row_spec = P(("dp", "ep"), None)
    swap = [(0, 1), (1, 0)]

    def to_ep(v, d):
        return lax.ppermute(v, "ep", [(i, i ^ d) for i in range(ep_size)])

    def local_block(tokens, grad_out, w_router, w_in, w_out, expert_ids):
        n_tok, d_model = tokens.shape
        n_experts = w_router.shape[1]
        width = w_in.shape[2]
        capacity = (6 * n_tok + 5 * n_experts - 1) // (5 * n_experts)
        cap = (capacity + 15) // 16 * 16
        chunk = width // 3
        tp, ep = lax.axis_index("tp"), lax.axis_index("ep")
        meta = jnp.where(jnp.arange(2) == 0, tp, ep).astype(jnp.int32)

        wi_far = lax.ppermute(lax.dynamic_index_in_dim(w_in, 1 - tp, 0, False), "tp", swap)
        wo_far = lax.ppermute(lax.dynamic_index_in_dim(w_out, 1 - tp, 0, False), "tp", swap)

        chosen = expert_ids[:, None] == jnp.arange(n_experts)[None, :]
        one_hot = chosen.astype(jnp.int32)
        position = jnp.sum(jnp.cumsum(one_hot, axis=0) * one_hot, axis=1) - 1
        slot = jnp.where(position < capacity, expert_ids * cap + position, -1)
        slot_row, slot_col = slot[None, :], slot[:, None]

        x_away = dispatch_rows(meta, slot_row, tokens, 2, 2, cap)
        x2, x3 = to_ep(x_away[0], 2), to_ep(x_away[1], 3)

        logits = jnp.dot(tokens, w_router, preferred_element_type=F32)
        prob = jax.nn.softmax(logits, axis=-1)
        gate = jnp.sum(jnp.where(chosen, prob, 0.0), axis=1)
        dy_tok = (gate[:, None] * grad_out.astype(F32)).astype(BF16)

        dy_away = dispatch_rows(meta, slot_row, dy_tok, 2, 2, cap)
        dy2, dy3 = to_ep(dy_away[0], 2), to_ep(dy_away[1], 3)
        x_here = dispatch_rows(meta, slot_row, tokens, 0, 2, cap)
        x1 = to_ep(x_here[1], 1)
        dy_here = dispatch_rows(meta, slot_row, dy_tok, 0, 2, cap)
        dy1 = to_ep(dy_here[1], 1)

        h_n, da_n, y_n, s_n, x_n, dy_n = own_half(meta, (x_here[0], x1), (dy_here[0], dy1), w_in, w_out, cap, chunk)
        y0, y1, s0, s1 = other_half(meta, x_n, dy_n, wi_far, wo_far, y_n, s_n, cap, chunk)
        h_f, da_f, y_f, s_f, x_f, dy_f = own_half(meta, (x2, x3), (dy2, dy3), w_in, w_out, cap, chunk)
        y2, y3, s2, s3 = other_half(meta, x_f, dy_f, wi_far, wo_far, y_f, s_f, cap, chunk)

        def collect(parts):
            mine = [parts[0]] + [to_ep(part, d + 1) for d, part in enumerate(parts[1:])]
            return mine, [lax.ppermute(part, "tp", swap) for part in mine]

        y_mine, y_twin = collect([y0, y1, y2, y3])
        s_mine, s_twin = collect([s0, s1, s2, s3])
        grad_w_in, grad_w_out = weight_grads((x_n, dy_n, h_n, da_n), (x_f, dy_f, h_f, da_f), chunk)

        piece = jnp.arange(8)
        owner = jnp.bitwise_xor(ep, piece % 4) * 2 + jnp.bitwise_xor(tp, piece // 4)
        codes = (owner[:, None] * cap + jnp.arange(cap)[None, :]).reshape(1, 8 * cap).astype(jnp.int32)
        moe_out, dlog, dwg = combine_y(
            y_mine + y_twin, slot_col, codes, expert_ids[:, None], prob, tokens, grad_out, n_tok // 4
        )
        dwg = dwg + to_ep(dwg, 1)
        dwg = dwg + to_ep(dwg, 2)
        grad_tokens = combine_s(s_mine + s_twin, slot_col, codes, dlog, w_router, n_tok // 4)
        return moe_out, grad_tokens, grad_w_in, grad_w_out, dwg.T

    in_specs = (row_spec, row_spec, P(None, None), P("ep", None, "tp"), P("ep", "tp", None), P(("dp", "ep")))
    out_specs = (row_spec, row_spec, P(("dp", "ep"), None, "tp"), P(("dp", "ep"), "tp", None), P("dp", None))
    return jax.shard_map(local_block, mesh=mesh, in_specs=in_specs, out_specs=out_specs, check_vma=False)
```

```python
import jax
import jax.numpy as jnp
from jax import lax
from jax.experimental import pallas as pl
from jax.experimental.pallas import tpu as pltpu
from jax.sharding import PartitionSpec as P


GELU_C = 0.7978845608028654
GELU_K = 0.044715
BF16 = jnp.bfloat16
F32 = jnp.float32
VMEM_LIMIT = 56 * 2**20
INFO_ROWS = 16


def nn(a, b):
    return jnp.dot(a, b, preferred_element_type=F32)


def nt(a, b):
    return lax.dot_general(a, b, (((1,), (1,)), ((), ())), preferred_element_type=F32)


def tn(a, b):
    return lax.dot_general(a, b, (((0,), (0,)), ((), ())), preferred_element_type=F32)


def gelu_and_slope(a):
    sq = a * a
    th = jnp.tanh(GELU_C * a * (1.0 + GELU_K * sq))
    cdf = 0.5 * (1.0 + th)
    slope = cdf + (0.5 * GELU_C) * a * (1.0 - th * th) * (1.0 + 3.0 * GELU_K * sq)
    return a * cdf, slope


def hidden_grads(x, dy, wi, wo):
    a = nn(x, wi)
    dh = nt(dy, wo)
    act, slope = gelu_and_slope(a)
    return act.astype(BF16), (dh * slope).astype(BF16)


def params(dims):
    return pltpu.CompilerParams(dimension_semantics=("arbitrary",) * dims, vmem_limit_bytes=VMEM_LIMIT)


def cost(flops, mib):
    return pl.CostEstimate(flops=int(flops), bytes_accessed=int(mib * 2**20), transcendentals=0)


def shape(dims, dtype=BF16):
    return jax.ShapeDtypeStruct(dims, dtype)


def whole(dims):
    return pl.BlockSpec(dims, lambda *_: (0,) * len(dims))


def route(ids_row, tokens, wg_t, capacity, cap):
    n_experts = wg_t.shape[0]
    n_tok = tokens.shape[0]
    step = 256

    def body(ids_ref, x_ref, wg_ref, info_ref):
        ids = ids_ref[...]
        logits = nt(wg_ref[...], x_ref[...])
        raised = jnp.exp(logits - jnp.max(logits, axis=0, keepdims=True))
        prob = raised / jnp.sum(raised, axis=0, keepdims=True)
        hot = ids == lax.broadcasted_iota(jnp.int32, (n_experts, n_tok), 0)
        hot_f = jnp.where(hot, 1.0, 0.0)
        upper = lax.broadcasted_iota(jnp.int32, (step, step), 0) <= lax.broadcasted_iota(jnp.int32, (step, step), 1)
        upper = jnp.where(upper, 1.0, 0.0).astype(BF16)
        carry = jnp.zeros((n_experts, 1), F32)
        for b in range(n_tok // step):
            cols = slice(b * step, (b + 1) * step)
            seen = nn(hot_f[:, cols].astype(BF16), upper) + carry
            carry = seen[:, step - 1 : step]
            pos = jnp.sum(seen * hot_f[:, cols], axis=0, keepdims=True) - 1.0
            slot = ids[:, cols].astype(F32) * cap + pos
            info_ref[0:1, cols] = jnp.where(pos < capacity, slot, -1.0)
        info_ref[1:2, :] = jnp.sum(hot_f * prob, axis=0, keepdims=True)
        info_ref[2:3, :] = ids.astype(F32)
        info_ref[3:8, :] = jnp.zeros((5, n_tok), F32)
        info_ref[8:16, :] = prob

    return pl.pallas_call(
        body,
        grid=(1,),
        in_specs=[whole(ids_row.shape), whole(tokens.shape), whole(wg_t.shape)],
        out_specs=whole((INFO_ROWS, n_tok)),
        out_shape=shape((INFO_ROWS, n_tok), F32),
        compiler_params=params(1),
        cost_estimate=cost(2e9, 3),
        name="route",
    )(ids_row, tokens, wg_t)


def dispatch(meta, info, tokens, grad_out, first, flip, cap):
    n_tok, d_model = tokens.shape

    def body(meta_ref, info_ref, x_ref, gy_ref, out_a, out_b):
        k = jnp.bitwise_xor(meta_ref[0], flip)
        slot = info_ref[0:1, :]
        gate = info_ref[1:2, :]
        for d, out_ref in enumerate((out_a, out_b)):
            base = (jnp.bitwise_xor(meta_ref[1], first + d) * 2 + k) * cap
            codes = (lax.broadcasted_iota(jnp.int32, (cap, n_tok), 0) + base).astype(F32)
            hit = slot == codes
            pick = jnp.where(hit, 1.0, 0.0).astype(BF16)
            row_gate = jnp.sum(jnp.where(hit, gate, 0.0), axis=1, keepdims=True)
            out_ref[0] = nn(pick, x_ref[...]).astype(BF16)
            out_ref[1] = (row_gate * nn(pick, gy_ref[...])).astype(BF16)

    return pl.pallas_call(
        body,
        grid_spec=pltpu.PrefetchScalarGridSpec(
            num_scalar_prefetch=1,
            grid=(1,),
            in_specs=[whole(info.shape), whole(tokens.shape), whole(tokens.shape)],
            out_specs=[whole((2, cap, d_model))] * 2,
        ),
        out_shape=[shape((2, cap, d_model))] * 2,
        compiler_params=params(1),
        cost_estimate=cost(8 * cap * n_tok * d_model, 10),
        name="dispatch",
    )(meta, info, tokens, grad_out)


def own_half(meta, pair_a, pair_b, w_in, w_out, chunk):
    _, d_model, width = w_in.shape
    cap = pair_a.shape[1]
    rows = 2 * cap

    def body(meta_ref, pa, pb, wi, wo, h_ref, da_ref, y_ref, s_ref, x_ref, dy_ref):
        c = pl.program_id(0)

        @pl.when(c == 0)
        def _():
            x_ref[:cap] = pa[0]
            x_ref[cap:] = pb[0]
            dy_ref[:cap] = pa[1]
            dy_ref[cap:] = pb[1]

        h, da = hidden_grads(x_ref[...], dy_ref[...], wi[0], wo[0])
        h_ref[...] = h
        da_ref[...] = da
        y = nn(h, wo[0])
        s = nt(da, wi[0])

        @pl.when(c == 0)
        def _():
            y_ref[...] = y
            s_ref[...] = s

        @pl.when(c > 0)
        def _():
            y_ref[...] += y
            s_ref[...] += s

    hid = pl.BlockSpec((rows, chunk), lambda c, m: (0, c))
    return pl.pallas_call(
        body,
        grid_spec=pltpu.PrefetchScalarGridSpec(
            num_scalar_prefetch=1,
            grid=(width // chunk,),
            in_specs=[
                whole(pair_a.shape),
                whole(pair_a.shape),
                pl.BlockSpec((1, d_model, chunk), lambda c, m: (m[0], 0, c)),
                pl.BlockSpec((1, chunk, d_model), lambda c, m: (m[0], c, 0)),
            ],
            out_specs=[hid, hid] + [whole((rows, d_model))] * 4,
        ),
        out_shape=[shape((rows, width))] * 2 + [shape((rows, d_model), F32)] * 2 + [shape((rows, d_model))] * 2,
        compiler_params=params(1),
        cost_estimate=cost(8 * rows * width * d_model, 20),
        name="own_half",
    )(meta, pair_a, pair_b, w_in, w_out)


def far_half(x, dy, wi, wo, y_in, s_in, chunk, last):
    rows, d_model = x.shape
    width = wi.shape[1]
    cap = rows // 2
    steps = width // chunk

    def body(x_ref, dy_ref, wi_ref, wo_ref, y0, s0, *outs):
        c = pl.program_id(0)
        y_acc, s_acc = outs[-2:]
        h, da = hidden_grads(x_ref[...], dy_ref[...], wi_ref[...], wo_ref[...])
        y = nn(h, wo_ref[...])
        s = nt(da, wi_ref[...])

        @pl.when(c == 0)
        def _():
            y_acc[...] = y0[...] + y
            s_acc[...] = s0[...] + s

        @pl.when(c > 0)
        def _():
            y_acc[...] += y
            s_acc[...] += s

        if last:

            @pl.when(c == steps - 1)
            def _():
                outs[0][...] = y_acc[:cap].astype(BF16)
                outs[1][...] = y_acc[cap:].astype(BF16)
                outs[2][...] = s_acc[:cap].astype(BF16)
                outs[3][...] = s_acc[cap:].astype(BF16)

    full = whole((rows, d_model))
    if last:
        out_specs, out_shape = [whole((cap, d_model))] * 4, [shape((cap, d_model))] * 4
        scratch = [pltpu.VMEM((rows, d_model), F32)] * 2
    else:
        out_specs, out_shape, scratch = [full] * 2, [shape((rows, d_model), F32)] * 2, []
    return pl.pallas_call(
        body,
        grid=(steps,),
        in_specs=[
            full,
            full,
            pl.BlockSpec((d_model, chunk), lambda c: (0, c)),
            pl.BlockSpec((chunk, d_model), lambda c: (c, 0)),
            full,
            full,
        ],
        out_specs=out_specs,
        out_shape=out_shape,
        scratch_shapes=scratch,
        compiler_params=params(1),
        cost_estimate=cost(8 * rows * width * d_model, 10),
        name="far_half",
    )(x, dy, wi, wo, y_in, s_in)


def finished_grads(meta, near, far, n_local, chunk):
    x, dy, h, da = near
    rows, d_model = x.shape
    width = h.shape[1]

    def body(meta_ref, x0, x1, dy0, dy1, h0, h1, da0, da1, gi, go):
        gi[0] = tn(x0[...], da0[...]) + tn(x1[...], da1[...])
        go[0] = tn(h0[...], dy0[...]) + tn(h1[...], dy1[...])

    hid = pl.BlockSpec((rows, chunk), lambda c, m: (0, c))
    return pl.pallas_call(
        body,
        grid_spec=pltpu.PrefetchScalarGridSpec(
            num_scalar_prefetch=1,
            grid=(width // chunk,),
            in_specs=[whole((rows, d_model))] * 4 + [hid] * 4,
            out_specs=[
                pl.BlockSpec((1, d_model, chunk), lambda c, m: (m[0], 0, c)),
                pl.BlockSpec((1, chunk, d_model), lambda c, m: (m[0], c, 0)),
            ],
        ),
        out_shape=[shape((n_local, d_model, width), F32), shape((n_local, width, d_model), F32)],
        compiler_params=params(1),
        cost_estimate=cost(8 * rows * width * d_model, 25),
        name="finished_grads",
    )(meta, x, far[0], dy, far[1], h, far[2], da, far[3])


def other_grads(meta, pairs, w_in, w_out, grad_w_in, grad_w_out, chunk):
    _, d_model, width = w_in.shape
    cap = pairs[0].shape[1]
    rows = len(pairs) * cap

    def body(meta_ref, *refs):
        parts = refs[: len(pairs)]
        wi, wo, _, _, gi, go, x, dy = refs[len(pairs) :]

        @pl.when(pl.program_id(0) == 0)
        def _():
            for p, part in enumerate(parts):
                x[p * cap : (p + 1) * cap, :] = part[0]
                dy[p * cap : (p + 1) * cap, :] = part[1]

        h, da = hidden_grads(x[...], dy[...], wi[0], wo[0])
        gi[0] = tn(x[...], da)
        go[0] = tn(h, dy[...])

    def other(m):
        return 1 - m[0]

    any_spec = pl.BlockSpec(memory_space=pl.ANY)
    wi_spec = pl.BlockSpec((1, d_model, chunk), lambda c, m: (other(m), 0, c))
    wo_spec = pl.BlockSpec((1, chunk, d_model), lambda c, m: (other(m), c, 0))
    return pl.pallas_call(
        body,
        grid_spec=pltpu.PrefetchScalarGridSpec(
            num_scalar_prefetch=1,
            grid=(width // chunk,),
            in_specs=[whole(pairs[0].shape)] * len(pairs) + [wi_spec, wo_spec, any_spec, any_spec],
            out_specs=[wi_spec, wo_spec],
            scratch_shapes=[pltpu.VMEM((rows, d_model), BF16)] * 2,
        ),
        out_shape=[shape(grad_w_in.shape, F32), shape(grad_w_out.shape, F32)],
        input_output_aliases={len(pairs) + 3: 0, len(pairs) + 4: 1},
        compiler_params=params(1),
        cost_estimate=cost(8 * rows * width * d_model, 25),
        name="other_grads",
    )(meta, *pairs, w_in, w_out, grad_w_in, grad_w_out)


def stack_rows(parts, all_rows):
    @pl.when(pl.program_id(0) == 0)
    def _():
        cap = parts[0].shape[0]
        for p, part in enumerate(parts):
            all_rows[p * cap : (p + 1) * cap, :] = part[...]


def combine_y(pieces, info, codes, tokens, grad_out, block):
    n_tok, d_model = tokens.shape
    cap = pieces[0].shape[0]
    n_experts = INFO_ROWS - 8
    slots = cap * len(pieces)

    def body(*refs):
        parts = refs[: len(pieces)]
        info_ref, codes_ref, x_ref, gy_ref, out_ref, dlog_ref, dwg_ref, all_rows = refs[len(pieces) :]
        stack_rows(parts, all_rows)
        info_v = info_ref[...].T
        pick = jnp.where(info_v[:, 0:1] == codes_ref[...], 1.0, 0.0).astype(BF16)
        y = nn(pick, all_rows[...])
        gate = info_v[:, 1:2]
        prob = info_v[:, 8:16]
        hot = info_v[:, 2:3] == lax.broadcasted_iota(jnp.int32, prob.shape, 1).astype(F32)
        out_ref[...] = (gate * y).astype(BF16)
        d_gate = jnp.sum(gy_ref[...].astype(F32) * y, axis=1, keepdims=True)
        dlog = (d_gate * prob * (jnp.where(hot, 1.0, 0.0) - gate)).astype(BF16)
        dlog_ref[...] = dlog
        dwg = tn(dlog, x_ref[...])

        @pl.when(pl.program_id(0) == 0)
        def _():
            dwg_ref[...] = dwg

        @pl.when(pl.program_id(0) > 0)
        def _():
            dwg_ref[...] += dwg

    tok = pl.BlockSpec((block, d_model), lambda b: (b, 0))
    return pl.pallas_call(
        body,
        grid=(n_tok // block,),
        in_specs=[whole((cap, d_model))] * len(pieces)
        + [pl.BlockSpec((INFO_ROWS, block), lambda b: (0, b)), whole((1, slots)), tok, tok],
        out_specs=[tok, pl.BlockSpec((block, n_experts), lambda b: (b, 0)), whole((n_experts, d_model))],
        out_shape=[shape((n_tok, d_model)), shape((n_tok, n_experts)), shape((n_experts, d_model), F32)],
        scratch_shapes=[pltpu.VMEM((slots, d_model), BF16)],
        compiler_params=params(1),
        cost_estimate=cost(2 * n_tok * slots * d_model, 16),
        name="combine_y",
    )(*pieces, info, codes, tokens, grad_out)


def combine_s(pieces, info, codes, extra, block):
    n_tok = info.shape[1]
    cap, d_model = pieces[0].shape
    slots = cap * len(pieces)

    def body(*refs):
        parts = refs[: len(pieces)]
        info_ref, codes_ref, *mid, out_ref, all_rows = refs[len(pieces) :]
        stack_rows(parts, all_rows)
        info_v = info_ref[...].T
        pick = jnp.where(info_v[:, 0:1] == codes_ref[...], 1.0, 0.0).astype(BF16)
        s = nn(pick, all_rows[...])
        if extra:
            so_far, dlog_ref, wg_ref = mid
            s = s + so_far[...].astype(F32) + nt(dlog_ref[...], wg_ref[...])
        out_ref[...] = s.astype(BF16)

    tok = pl.BlockSpec((block, d_model), lambda b: (b, 0))
    extra_specs = []
    if extra:
        extra_specs = [tok, pl.BlockSpec((block, extra[1].shape[1]), lambda b: (b, 0)), whole(extra[2].shape)]
    return pl.pallas_call(
        body,
        grid=(n_tok // block,),
        in_specs=[whole((cap, d_model))] * len(pieces)
        + [pl.BlockSpec((INFO_ROWS, block), lambda b: (0, b)), whole((1, slots))]
        + extra_specs,
        out_specs=tok,
        out_shape=shape((n_tok, d_model)),
        scratch_shapes=[pltpu.VMEM((slots, d_model), BF16)],
        compiler_params=params(1),
        cost_estimate=cost(2 * n_tok * slots * d_model, 10),
        name="combine_s",
    )(*pieces, info, codes, *extra)


def solution(mesh):
    ep_size = mesh.shape["ep"]
    row_spec = P(("dp", "ep"), None)

    def to_ep(v, d):
        return lax.ppermute(v, "ep", [(i, i ^ d) for i in range(ep_size)])

    def to_twin(v):
        return lax.ppermute(v, "tp", [(0, 1), (1, 0)])

    def block(tokens, grad_out, w_router, w_in, w_out, expert_ids):
        n_tok, d_model = tokens.shape
        n_experts = w_router.shape[1]
        width = w_in.shape[2]
        capacity = (6 * n_tok + 5 * n_experts - 1) // (5 * n_experts)
        cap = (capacity + 15) // 16 * 16
        chunk = width // 3
        tp, ep = lax.axis_index("tp"), lax.axis_index("ep")
        meta = jnp.where(jnp.arange(2) == 0, tp, ep).astype(jnp.int32)

        cut = 2 * chunk
        wi_a = to_twin(lax.dynamic_slice(w_in, (1 - tp, 0, 0), (1, d_model, cut))[0])
        wo_a = to_twin(lax.dynamic_slice(w_out, (1 - tp, 0, 0), (1, cut, d_model))[0])
        wi_b = to_twin(lax.dynamic_slice(w_in, (1 - tp, 0, cut), (1, d_model, chunk))[0])
        wo_b = to_twin(lax.dynamic_slice(w_out, (1 - tp, cut, 0), (1, chunk, d_model))[0])

        info = route(expert_ids[None, :], tokens, w_router.T, capacity, cap)

        f2, f3 = dispatch(meta, info, tokens, grad_out, 2, 0, cap)
        f2, f3 = to_ep(f2, 2), to_ep(f3, 3)
        f0, f1 = dispatch(meta, info, tokens, grad_out, 0, 0, cap)
        f1 = to_ep(f1, 1)
        g2, g3 = dispatch(meta, info, tokens, grad_out, 2, 1, cap)
        g2, g3 = to_ep(g2, 2), to_ep(g3, 3)
        g0, g1 = dispatch(meta, info, tokens, grad_out, 0, 1, cap)
        g1 = to_ep(g1, 1)

        h_n, da_n, y_n, s_n, x_n, dy_n = own_half(meta, f0, f1, w_in, w_out, chunk)
        h_f, da_f, y_f, s_f, x_f, dy_f = own_half(meta, f2, f3, w_in, w_out, chunk)
        y_n, s_n = far_half(x_n, dy_n, wi_a, wo_a, y_n, s_n, chunk, False)
        y_f, s_f = far_half(x_f, dy_f, wi_a, wo_a, y_f, s_f, chunk, False)
        y0, y1, s0, s1 = far_half(x_n, dy_n, wi_b, wo_b, y_n, s_n, chunk, True)
        y2, y3, s2, s3 = far_half(x_f, dy_f, wi_b, wo_b, y_f, s_f, chunk, True)

        y1, s1 = to_ep(y1, 1), to_ep(s1, 1)
        y2, y3 = to_ep(y2, 2), to_ep(y3, 3)
        s2, s3 = to_ep(s2, 2), to_ep(s3, 3)
        y_mine, s_mine = [y0, y1, y2, y3], [s0, s1, s2, s3]
        y_twin = [to_twin(v) for v in y_mine]
        s_twin = [to_twin(v) for v in s_mine]

        grads = finished_grads(meta, (x_n, dy_n, h_n, da_n), (x_f, dy_f, h_f, da_f), w_in.shape[0], chunk)
        grad_w_in, grad_w_out = other_grads(meta, (g0, g1, g2, g3), w_in, w_out, *grads, chunk)

        piece = jnp.arange(8)
        owner = jnp.bitwise_xor(ep, piece % 4) * 2 + jnp.bitwise_xor(tp, piece // 4)
        codes = (owner[:, None] * cap + jnp.arange(cap)[None, :]).reshape(1, 8 * cap).astype(F32)
        moe_out, dlog, dwg = combine_y(y_mine + y_twin, info, codes, tokens, grad_out, n_tok // 4)
        dwg = dwg + to_ep(dwg, 1)
        dwg = dwg + to_ep(dwg, 2)
        so_far = combine_s(s_mine + s_twin[:2], info, codes[:, : 6 * cap], (), n_tok // 4)
        grad_tokens = combine_s(s_twin[2:], info, codes[:, 6 * cap :], (so_far, dlog, w_router), n_tok // 4)
        return moe_out, grad_tokens, grad_w_in, grad_w_out, dwg.T

    in_specs = (row_spec, row_spec, P(None, None), P("ep", None, "tp"), P("ep", "tp", None), P(("dp", "ep")))
    out_specs = (row_spec, row_spec, P(("dp", "ep"), None, "tp"), P(("dp", "ep"), "tp", None), P("dp", None))
    return jax.shard_map(block, mesh=mesh, in_specs=in_specs, out_specs=out_specs, check_vma=False)
```

```python
import jax
import jax.numpy as jnp
from jax import lax
from jax.experimental import pallas as pl
from jax.experimental.pallas import tpu as pltpu
from jax.sharding import PartitionSpec as P


GELU_C = 0.7978845608028654
GELU_K = 0.044715
BF16 = jnp.bfloat16
F32 = jnp.float32
VMEM_LIMIT = 56 * 2**20
INFO_ROWS = 16


def nn(a, b):
    return jnp.dot(a, b, preferred_element_type=F32)


def nt(a, b):
    return lax.dot_general(a, b, (((1,), (1,)), ((), ())), preferred_element_type=F32)


def tn(a, b):
    return lax.dot_general(a, b, (((0,), (0,)), ((), ())), preferred_element_type=F32)


def gelu_and_slope(a):
    sq = a * a
    th = jnp.tanh(a * (GELU_C + (GELU_C * GELU_K) * sq))
    up = 1.0 + th
    act = (0.5 * a) * up
    return act, 0.5 * up + act * (1.0 - th) * (GELU_C + (3.0 * GELU_C * GELU_K) * sq)


def hidden_grads(x, dy, wi, wo):
    a = nn(x, wi)
    dh = nt(dy, wo)
    act, slope = gelu_and_slope(a)
    return act.astype(BF16), (dh * slope).astype(BF16)


def params(dims):
    return pltpu.CompilerParams(dimension_semantics=("arbitrary",) * dims, vmem_limit_bytes=VMEM_LIMIT)


def cost(flops, mib):
    return pl.CostEstimate(flops=int(flops), bytes_accessed=int(mib * 2**20), transcendentals=0)


def shape(dims, dtype=BF16):
    return jax.ShapeDtypeStruct(dims, dtype)


def whole(dims):
    return pl.BlockSpec(dims, lambda *_: (0,) * len(dims))


def route(ids_row, tokens, wg_t, capacity, cap):
    n_experts = wg_t.shape[0]
    n_tok = tokens.shape[0]
    step = 256

    def body(ids_ref, x_ref, wg_ref, info_ref):
        ids = ids_ref[...]
        logits = nt(wg_ref[...], x_ref[...])
        raised = jnp.exp(logits - jnp.max(logits, axis=0, keepdims=True))
        prob = raised / jnp.sum(raised, axis=0, keepdims=True)
        hot = ids == lax.broadcasted_iota(jnp.int32, (n_experts, n_tok), 0)
        hot_f = jnp.where(hot, 1.0, 0.0)
        upper = lax.broadcasted_iota(jnp.int32, (step, step), 0) <= lax.broadcasted_iota(jnp.int32, (step, step), 1)
        upper = jnp.where(upper, 1.0, 0.0).astype(BF16)
        carry = jnp.zeros((n_experts, 1), F32)
        for b in range(n_tok // step):
            cols = slice(b * step, (b + 1) * step)
            seen = nn(hot_f[:, cols].astype(BF16), upper) + carry
            carry = seen[:, step - 1 : step]
            pos = jnp.sum(seen * hot_f[:, cols], axis=0, keepdims=True) - 1.0
            slot = ids[:, cols].astype(F32) * cap + pos
            info_ref[0:1, cols] = jnp.where(pos < capacity, slot, -1.0)
        info_ref[1:2, :] = jnp.sum(hot_f * prob, axis=0, keepdims=True)
        info_ref[2:3, :] = ids.astype(F32)
        info_ref[3:8, :] = jnp.zeros((5, n_tok), F32)
        info_ref[8:16, :] = prob

    return pl.pallas_call(
        body,
        grid=(1,),
        in_specs=[whole(ids_row.shape), whole(tokens.shape), whole(wg_t.shape)],
        out_specs=whole((INFO_ROWS, n_tok)),
        out_shape=shape((INFO_ROWS, n_tok), F32),
        compiler_params=params(1),
        cost_estimate=cost(2e9, 3),
        name="route",
    )(ids_row, tokens, wg_t)


def dispatch(meta, info, tokens, grad_out, groups, cap):
    n_tok, d_model = tokens.shape
    count = len(groups)

    def body(meta_ref, info_ref, x_ref, gy_ref, *outs):
        g = pl.program_id(0)
        first, flip = groups[0]
        for p in range(1, count):
            first = jnp.where(g == p, groups[p][0], first)
            flip = jnp.where(g == p, groups[p][1], flip)
        k = jnp.bitwise_xor(meta_ref[0], flip)
        row = lax.broadcasted_iota(jnp.int32, (2 * cap, 1), 0)
        low = row < cap
        base_a = (jnp.bitwise_xor(meta_ref[1], first) * 2 + k) * cap
        base_b = (jnp.bitwise_xor(meta_ref[1], first + 1) * 2 + k) * cap - cap
        codes = (row + jnp.where(low, base_a, base_b)).astype(F32)
        hit = info_ref[0:1, :] == codes
        pick = jnp.where(hit, 1.0, 0.0).astype(BF16)
        row_gate = jnp.sum(jnp.where(hit, info_ref[1:2, :], 0.0), axis=1, keepdims=True)
        x = nn(pick, x_ref[...]).astype(BF16)
        dy = (row_gate * nn(pick, gy_ref[...])).astype(BF16)
        for p in range(count):

            @pl.when(g == p)
            def _():
                outs[2 * p][0] = x[:cap]
                outs[2 * p][1] = dy[:cap]
                outs[2 * p + 1][0] = x[cap:]
                outs[2 * p + 1][1] = dy[cap:]

    return pl.pallas_call(
        body,
        grid_spec=pltpu.PrefetchScalarGridSpec(
            num_scalar_prefetch=1,
            grid=(count,),
            in_specs=[whole(info.shape), whole(tokens.shape), whole(tokens.shape)],
            out_specs=[whole((2, cap, d_model))] * (2 * count),
        ),
        out_shape=[shape((2, cap, d_model))] * (2 * count),
        compiler_params=params(1),
        cost_estimate=cost(8 * count * cap * n_tok * d_model, 8 + 4 * count),
        name="dispatch",
    )(meta, info, tokens, grad_out)


def own_half(meta, pair_a, pair_b, w_in, w_out, chunk, group, so_far):
    _, d_model, width = w_in.shape
    cap = pair_a.shape[1]
    rows = 2 * cap

    def body(meta_ref, pa, pb, wi, wo, *refs):
        h_ref, da_ref, y_ref, s_ref, x_ref, dy_ref = refs[-6:]
        c = pl.program_id(0)

        @pl.when(c == 0)
        def _():
            x_ref[:cap] = pa[0]
            x_ref[cap:] = pb[0]
            dy_ref[:cap] = pa[1]
            dy_ref[cap:] = pb[1]

        h, da = hidden_grads(x_ref[...], dy_ref[...], wi[0], wo[0])
        h_ref[...] = h
        da_ref[...] = da
        y = nn(h, wo[0])
        s = nt(da, wi[0])

        @pl.when(c == 0)
        def _():
            y_ref[...] = y
            s_ref[...] = s

        @pl.when(c > 0)
        def _():
            y_ref[...] += y
            s_ref[...] += s

    hid = pl.BlockSpec((rows, chunk), lambda c, m: (group, c))
    full = pl.BlockSpec((rows, d_model), lambda c, m: (group, 0))
    return pl.pallas_call(
        body,
        grid_spec=pltpu.PrefetchScalarGridSpec(
            num_scalar_prefetch=1,
            grid=(width // chunk,),
            in_specs=[
                whole(pair_a.shape),
                whole(pair_a.shape),
                pl.BlockSpec((1, d_model, chunk), lambda c, m: (m[0], 0, c)),
                pl.BlockSpec((1, chunk, d_model), lambda c, m: (m[0], c, 0)),
            ]
            + [pl.BlockSpec(memory_space=pl.ANY)] * len(so_far),
            out_specs=[hid, hid] + [full] * 4,
        ),
        out_shape=[shape((2 * rows, width))] * 2
        + [shape((2 * rows, d_model), F32)] * 2
        + [shape((2 * rows, d_model))] * 2,
        input_output_aliases={5 + i: i for i in range(len(so_far))},
        compiler_params=params(1),
        cost_estimate=cost(8 * rows * width * d_model, 20),
        name="own_half",
    )(meta, pair_a, pair_b, w_in, w_out, *so_far)


def far_half(x, dy, wi, wo, y_in, s_in, chunk, pieces):
    rows, d_model = x.shape
    width = wi.shape[1]
    steps = width // chunk

    def body(x_ref, dy_ref, wi_ref, wo_ref, y0, s0, *outs):
        c = pl.program_id(0)
        y_acc, s_acc = outs[-2:]
        h, da = hidden_grads(x_ref[...], dy_ref[...], wi_ref[...], wo_ref[...])
        y = nn(h, wo_ref[...])
        s = nt(da, wi_ref[...])
        if pieces and steps == 1:
            y_acc, s_acc = None, None
            for p in range(pieces):
                part = slice(p * rows // pieces, (p + 1) * rows // pieces)
                outs[p][...] = (y0[part] + y[part]).astype(BF16)
                outs[pieces + p][...] = (s0[part] + s[part]).astype(BF16)
            return

        @pl.when(c == 0)
        def _():
            y_acc[...] = y0[...] + y
            s_acc[...] = s0[...] + s

        @pl.when(c > 0)
        def _():
            y_acc[...] += y
            s_acc[...] += s

    full = whole((rows, d_model))
    if pieces:
        assert steps == 1
        out_specs = [whole((rows // pieces, d_model))] * (2 * pieces)
        out_shape = [shape((rows // pieces, d_model))] * (2 * pieces)
    else:
        out_specs, out_shape = [full] * 2, [shape((rows, d_model), F32)] * 2
    return pl.pallas_call(
        body,
        grid=(steps,),
        in_specs=[
            full,
            full,
            pl.BlockSpec((d_model, chunk), lambda c: (0, c)),
            pl.BlockSpec((chunk, d_model), lambda c: (c, 0)),
            full,
            full,
        ],
        out_specs=out_specs,
        out_shape=out_shape,
        compiler_params=params(1),
        cost_estimate=cost(8 * rows * width * d_model, 10),
        name="far_half",
    )(x, dy, wi, wo, y_in, s_in)


def finished_grads(meta, x, dy, h, da, n_local, chunk):
    rows, d_model = x.shape
    width = h.shape[1]

    def body(meta_ref, x_ref, dy_ref, h_ref, da_ref, gi, go):
        gi[0] = tn(x_ref[...], da_ref[...])
        go[0] = tn(h_ref[...], dy_ref[...])

    hid = pl.BlockSpec((rows, chunk), lambda c, m: (0, c))
    return pl.pallas_call(
        body,
        grid_spec=pltpu.PrefetchScalarGridSpec(
            num_scalar_prefetch=1,
            grid=(width // chunk,),
            in_specs=[whole((rows, d_model))] * 2 + [hid] * 2,
            out_specs=[
                pl.BlockSpec((1, d_model, chunk), lambda c, m: (m[0], 0, c)),
                pl.BlockSpec((1, chunk, d_model), lambda c, m: (m[0], c, 0)),
            ],
        ),
        out_shape=[shape((n_local, d_model, width), F32), shape((n_local, width, d_model), F32)],
        compiler_params=params(1),
        cost_estimate=cost(4 * rows * width * d_model, 25),
        name="finished_grads",
    )(meta, x, dy, h, da)


def other_grads(meta, pairs, w_in, w_out, grad_w_in, grad_w_out, chunk):
    _, d_model, width = w_in.shape
    cap = pairs[0].shape[1]
    rows = len(pairs) * cap

    def body(meta_ref, *refs):
        parts = refs[: len(pairs)]
        wi, wo, _, _, gi, go, x, dy = refs[len(pairs) :]

        @pl.when(pl.program_id(0) == 0)
        def _():
            for p, part in enumerate(parts):
                x[p * cap : (p + 1) * cap, :] = part[0]
                dy[p * cap : (p + 1) * cap, :] = part[1]

        h, da = hidden_grads(x[...], dy[...], wi[0], wo[0])
        gi[0] = tn(x[...], da)
        go[0] = tn(h, dy[...])

    def other(m):
        return 1 - m[0]

    any_spec = pl.BlockSpec(memory_space=pl.ANY)
    wi_spec = pl.BlockSpec((1, d_model, chunk), lambda c, m: (other(m), 0, c))
    wo_spec = pl.BlockSpec((1, chunk, d_model), lambda c, m: (other(m), c, 0))
    return pl.pallas_call(
        body,
        grid_spec=pltpu.PrefetchScalarGridSpec(
            num_scalar_prefetch=1,
            grid=(width // chunk,),
            in_specs=[whole(pairs[0].shape)] * len(pairs) + [wi_spec, wo_spec, any_spec, any_spec],
            out_specs=[wi_spec, wo_spec],
            scratch_shapes=[pltpu.VMEM((rows, d_model), BF16)] * 2,
        ),
        out_shape=[shape(grad_w_in.shape, F32), shape(grad_w_out.shape, F32)],
        input_output_aliases={len(pairs) + 3: 0, len(pairs) + 4: 1},
        compiler_params=params(1),
        cost_estimate=cost(8 * rows * width * d_model, 25),
        name="other_grads",
    )(meta, *pairs, w_in, w_out, grad_w_in, grad_w_out)


def stack_rows(parts, all_rows):
    @pl.when(pl.program_id(0) == 0)
    def _():
        cap = parts[0].shape[0]
        for p, part in enumerate(parts):
            all_rows[p * cap : (p + 1) * cap, :] = part[...]


def combine_y(pieces, info, codes, tokens, grad_out, block):
    n_tok, d_model = tokens.shape
    cap = pieces[0].shape[0]
    n_experts = INFO_ROWS - 8
    slots = cap * len(pieces)

    def body(*refs):
        parts = refs[: len(pieces)]
        info_ref, codes_ref, x_ref, gy_ref, out_ref, dlog_ref, dwg_ref, all_rows = refs[len(pieces) :]
        stack_rows(parts, all_rows)
        info_v = info_ref[...].T
        pick = jnp.where(info_v[:, 0:1] == codes_ref[...], 1.0, 0.0).astype(BF16)
        y = nn(pick, all_rows[...])
        gate = info_v[:, 1:2]
        prob = info_v[:, 8:16]
        hot = info_v[:, 2:3] == lax.broadcasted_iota(jnp.int32, prob.shape, 1).astype(F32)
        out_ref[...] = (gate * y).astype(BF16)
        d_gate = jnp.sum(gy_ref[...].astype(F32) * y, axis=1, keepdims=True)
        dlog = (d_gate * prob * (jnp.where(hot, 1.0, 0.0) - gate)).astype(BF16)
        dlog_ref[...] = dlog
        dwg = tn(dlog, x_ref[...])

        @pl.when(pl.program_id(0) == 0)
        def _():
            dwg_ref[...] = dwg

        @pl.when(pl.program_id(0) > 0)
        def _():
            dwg_ref[...] += dwg

    tok = pl.BlockSpec((block, d_model), lambda b: (b, 0))
    return pl.pallas_call(
        body,
        grid=(n_tok // block,),
        in_specs=[whole((cap, d_model))] * len(pieces)
        + [pl.BlockSpec((INFO_ROWS, block), lambda b: (0, b)), whole((1, slots)), tok, tok],
        out_specs=[tok, pl.BlockSpec((block, n_experts), lambda b: (b, 0)), whole((n_experts, d_model))],
        out_shape=[shape((n_tok, d_model)), shape((n_tok, n_experts)), shape((n_experts, d_model), F32)],
        scratch_shapes=[pltpu.VMEM((slots, d_model), BF16)],
        compiler_params=params(1),
        cost_estimate=cost(2 * n_tok * slots * d_model, 16),
        name="combine_y",
    )(*pieces, info, codes, tokens, grad_out)


def combine_s(pieces, info, codes, extra, block):
    n_tok = info.shape[1]
    cap, d_model = pieces[0].shape
    slots = cap * len(pieces)

    def body(*refs):
        parts = refs[: len(pieces)]
        info_ref, codes_ref, *mid, out_ref, all_rows = refs[len(pieces) :]
        stack_rows(parts, all_rows)
        info_v = info_ref[...].T
        pick = jnp.where(info_v[:, 0:1] == codes_ref[...], 1.0, 0.0).astype(BF16)
        s = nn(pick, all_rows[...])
        if extra:
            so_far, dlog_ref, wg_ref = mid
            s = s + so_far[...].astype(F32) + nt(dlog_ref[...], wg_ref[...])
        out_ref[...] = s.astype(BF16)

    tok = pl.BlockSpec((block, d_model), lambda b: (b, 0))
    extra_specs = []
    if extra:
        extra_specs = [tok, pl.BlockSpec((block, extra[1].shape[1]), lambda b: (b, 0)), whole(extra[2].shape)]
    return pl.pallas_call(
        body,
        grid=(n_tok // block,),
        in_specs=[whole((cap, d_model))] * len(pieces)
        + [pl.BlockSpec((INFO_ROWS, block), lambda b: (0, b)), whole((1, slots))]
        + extra_specs,
        out_specs=tok,
        out_shape=shape((n_tok, d_model)),
        scratch_shapes=[pltpu.VMEM((slots, d_model), BF16)],
        compiler_params=params(1),
        cost_estimate=cost(2 * n_tok * slots * d_model, 10),
        name="combine_s",
    )(*pieces, info, codes, *extra)


def solution(mesh):
    ep_size = mesh.shape["ep"]
    row_spec = P(("dp", "ep"), None)

    def to_ep(v, d):
        return lax.ppermute(v, "ep", [(i, i ^ d) for i in range(ep_size)])

    def to_twin(v):
        return lax.ppermute(v, "tp", [(0, 1), (1, 0)])

    def block(tokens, grad_out, w_router, w_in, w_out, expert_ids):
        n_tok, d_model = tokens.shape
        n_experts = w_router.shape[1]
        width = w_in.shape[2]
        capacity = (6 * n_tok + 5 * n_experts - 1) // (5 * n_experts)
        cap = (capacity + 15) // 16 * 16
        chunk = width // 3
        tp, ep = lax.axis_index("tp"), lax.axis_index("ep")
        meta = jnp.where(jnp.arange(2) == 0, tp, ep).astype(jnp.int32)

        cut = 2 * chunk
        wi_a = to_twin(lax.dynamic_slice(w_in, (1 - tp, 0, 0), (1, d_model, cut))[0])
        wo_a = to_twin(lax.dynamic_slice(w_out, (1 - tp, 0, 0), (1, cut, d_model))[0])
        wi_b = to_twin(lax.dynamic_slice(w_in, (1 - tp, 0, cut), (1, d_model, chunk))[0])
        wo_b = to_twin(lax.dynamic_slice(w_out, (1 - tp, cut, 0), (1, chunk, d_model))[0])

        info = route(expert_ids[None, :], tokens, w_router.T, capacity, cap)

        f2, f3 = dispatch(meta, info, tokens, grad_out, ((2, 0),), cap)
        f2, f3 = to_ep(f2, 2), to_ep(f3, 3)
        f0, f1, g2, g3, g0, g1 = dispatch(meta, info, tokens, grad_out, ((0, 0), (2, 1), (0, 1)), cap)
        f1 = to_ep(f1, 1)
        g2, g3 = to_ep(g2, 2), to_ep(g3, 3)
        g1 = to_ep(g1, 1)

        part = own_half(meta, f0, f1, w_in, w_out, chunk, 0, ())
        h, da, y, s, x, dy = own_half(meta, f2, f3, w_in, w_out, chunk, 1, part)
        y, s = far_half(x, dy, wi_a, wo_a, y, s, chunk, 0)
        y0, y1, y2, y3, s0, s1, s2, s3 = far_half(x, dy, wi_b, wo_b, y, s, chunk, 4)

        y1, s1 = to_ep(y1, 1), to_ep(s1, 1)
        y2, y3 = to_ep(y2, 2), to_ep(y3, 3)
        s2, s3 = to_ep(s2, 2), to_ep(s3, 3)
        y_mine, s_mine = [y0, y1, y2, y3], [s0, s1, s2, s3]
        y_twin = [to_twin(v) for v in y_mine]
        s_twin = [to_twin(v) for v in s_mine]

        grads = finished_grads(meta, x, dy, h, da, w_in.shape[0], chunk)
        grad_w_in, grad_w_out = other_grads(meta, (g0, g1, g2, g3), w_in, w_out, *grads, chunk)

        piece = jnp.arange(8)
        owner = jnp.bitwise_xor(ep, piece % 4) * 2 + jnp.bitwise_xor(tp, piece // 4)
        codes = (owner[:, None] * cap + jnp.arange(cap)[None, :]).reshape(1, 8 * cap).astype(F32)
        moe_out, dlog, dwg = combine_y(y_mine + y_twin, info, codes, tokens, grad_out, n_tok // 2)
        dwg = dwg + to_ep(dwg, 1)
        dwg = dwg + to_ep(dwg, 2)
        so_far = combine_s(s_mine + s_twin[:2], info, codes[:, : 6 * cap], (), n_tok // 2)
        grad_tokens = combine_s(s_twin[2:], info, codes[:, 6 * cap :], (so_far, dlog, w_router), n_tok // 2)
        return moe_out, grad_tokens, grad_w_in, grad_w_out, dwg.T

    in_specs = (row_spec, row_spec, P(None, None), P("ep", None, "tp"), P("ep", "tp", None), P(("dp", "ep")))
    out_specs = (row_spec, row_spec, P(("dp", "ep"), None, "tp"), P(("dp", "ep"), "tp", None), P("dp", None))
    return jax.shard_map(block, mesh=mesh, in_specs=in_specs, out_specs=out_specs, check_vma=False)
```

```python
import jax
import jax.numpy as jnp
from jax import lax
from jax.experimental import pallas as pl
from jax.experimental.pallas import tpu as pltpu
from jax.sharding import PartitionSpec as P


GELU_C = 0.7978845608028654
GELU_K = 0.044715
BF16 = jnp.bfloat16
F32 = jnp.float32
VMEM_LIMIT = 56 * 2**20
INFO_ROWS = 16


def nn(a, b):
    return jnp.dot(a, b, preferred_element_type=F32)


def nt(a, b):
    return lax.dot_general(a, b, (((1,), (1,)), ((), ())), preferred_element_type=F32)


def tn(a, b):
    return lax.dot_general(a, b, (((0,), (0,)), ((), ())), preferred_element_type=F32)


def gelu_and_slope(a):
    sq = a * a
    th = jnp.tanh(a * (GELU_C + (GELU_C * GELU_K) * sq))
    up = 1.0 + th
    act = (0.5 * a) * up
    return act, 0.5 * up + act * (1.0 - th) * (GELU_C + (3.0 * GELU_C * GELU_K) * sq)


def hidden_grads(x, dy, wi, wo):
    a = nn(x, wi)
    dh = nt(dy, wo)
    act, slope = gelu_and_slope(a)
    return act.astype(BF16), (dh * slope).astype(BF16)


def params(dims):
    return pltpu.CompilerParams(dimension_semantics=("arbitrary",) * dims, vmem_limit_bytes=VMEM_LIMIT)


def cost(flops, mib):
    return pl.CostEstimate(flops=int(flops), bytes_accessed=int(mib * 2**20), transcendentals=0)


def shape(dims, dtype=BF16):
    return jax.ShapeDtypeStruct(dims, dtype)


def whole(dims):
    return pl.BlockSpec(dims, lambda *_: (0,) * len(dims))


def route(ids_row, tokens, wg_t, capacity, cap):
    n_experts = wg_t.shape[0]
    n_tok = tokens.shape[0]
    step = 256

    def body(ids_ref, x_ref, wg_ref, info_ref):
        ids = ids_ref[...]
        logits = nt(wg_ref[...], x_ref[...])
        raised = jnp.exp(logits - jnp.max(logits, axis=0, keepdims=True))
        prob = raised / jnp.sum(raised, axis=0, keepdims=True)
        hot = ids == lax.broadcasted_iota(jnp.int32, (n_experts, n_tok), 0)
        hot_f = jnp.where(hot, 1.0, 0.0)
        upper = lax.broadcasted_iota(jnp.int32, (step, step), 0) <= lax.broadcasted_iota(jnp.int32, (step, step), 1)
        upper = jnp.where(upper, 1.0, 0.0).astype(BF16)
        carry = jnp.zeros((n_experts, 1), F32)
        for b in range(n_tok // step):
            cols = slice(b * step, (b + 1) * step)
            seen = nn(hot_f[:, cols].astype(BF16), upper) + carry
            carry = seen[:, step - 1 : step]
            pos = jnp.sum(seen * hot_f[:, cols], axis=0, keepdims=True) - 1.0
            slot = ids[:, cols].astype(F32) * cap + pos
            info_ref[0:1, cols] = jnp.where(pos < capacity, slot, -1.0)
        info_ref[1:2, :] = jnp.sum(hot_f * prob, axis=0, keepdims=True)
        info_ref[2:3, :] = ids.astype(F32)
        info_ref[3:8, :] = jnp.zeros((5, n_tok), F32)
        info_ref[8:16, :] = prob

    return pl.pallas_call(
        body,
        grid=(1,),
        in_specs=[whole(ids_row.shape), whole(tokens.shape), whole(wg_t.shape)],
        out_specs=whole((INFO_ROWS, n_tok)),
        out_shape=shape((INFO_ROWS, n_tok), F32),
        compiler_params=params(1),
        cost_estimate=cost(2e9, 3),
        name="route",
    )(ids_row, tokens, wg_t)


def dispatch(meta, info, tokens, grad_out, groups, cap):
    n_tok, d_model = tokens.shape
    count = len(groups)

    def body(meta_ref, info_ref, x_ref, gy_ref, *outs):
        g = pl.program_id(0)
        first, flip = groups[0]
        for p in range(1, count):
            first = jnp.where(g == p, groups[p][0], first)
            flip = jnp.where(g == p, groups[p][1], flip)
        k = jnp.bitwise_xor(meta_ref[0], flip)
        row = lax.broadcasted_iota(jnp.int32, (2 * cap, 1), 0)
        low = row < cap
        base_a = (jnp.bitwise_xor(meta_ref[1], first) * 2 + k) * cap
        base_b = (jnp.bitwise_xor(meta_ref[1], first + 1) * 2 + k) * cap - cap
        codes = (row + jnp.where(low, base_a, base_b)).astype(F32)
        hit = info_ref[0:1, :] == codes
        pick = jnp.where(hit, 1.0, 0.0).astype(BF16)
        row_gate = jnp.sum(jnp.where(hit, info_ref[1:2, :], 0.0), axis=1, keepdims=True)
        x = nn(pick, x_ref[...]).astype(BF16)
        dy = (row_gate * nn(pick, gy_ref[...])).astype(BF16)
        for p in range(count):

            @pl.when(g == p)
            def _():
                outs[2 * p][0] = x[:cap]
                outs[2 * p][1] = dy[:cap]
                outs[2 * p + 1][0] = x[cap:]
                outs[2 * p + 1][1] = dy[cap:]

    return pl.pallas_call(
        body,
        grid_spec=pltpu.PrefetchScalarGridSpec(
            num_scalar_prefetch=1,
            grid=(count,),
            in_specs=[whole(info.shape), whole(tokens.shape), whole(tokens.shape)],
            out_specs=[whole((2, cap, d_model))] * (2 * count),
        ),
        out_shape=[shape((2, cap, d_model))] * (2 * count),
        compiler_params=params(1),
        cost_estimate=cost(8 * count * cap * n_tok * d_model, 8 + 4 * count),
        name="dispatch",
    )(meta, info, tokens, grad_out)


def own_half(meta, pair_a, pair_b, w_in, w_out, chunk, group, so_far):
    _, d_model, width = w_in.shape
    cap = pair_a.shape[1]
    rows = 2 * cap

    def body(meta_ref, pa, pb, wi, wo, *refs):
        h_ref, da_ref, y_ref, s_ref, x_ref, dy_ref = refs[-6:]
        c = pl.program_id(0)

        @pl.when(c == 0)
        def _():
            x_ref[:cap] = pa[0]
            x_ref[cap:] = pb[0]
            dy_ref[:cap] = pa[1]
            dy_ref[cap:] = pb[1]

        h, da = hidden_grads(x_ref[...], dy_ref[...], wi[0], wo[0])
        h_ref[...] = h
        da_ref[...] = da
        y = nn(h, wo[0])
        s = nt(da, wi[0])

        @pl.when(c == 0)
        def _():
            y_ref[...] = y
            s_ref[...] = s

        @pl.when(c > 0)
        def _():
            y_ref[...] += y
            s_ref[...] += s

    hid = pl.BlockSpec((rows, chunk), lambda c, m: (group, c))
    full = pl.BlockSpec((rows, d_model), lambda c, m: (group, 0))
    return pl.pallas_call(
        body,
        grid_spec=pltpu.PrefetchScalarGridSpec(
            num_scalar_prefetch=1,
            grid=(width // chunk,),
            in_specs=[
                whole(pair_a.shape),
                whole(pair_a.shape),
                pl.BlockSpec((1, d_model, chunk), lambda c, m: (m[0], 0, c)),
                pl.BlockSpec((1, chunk, d_model), lambda c, m: (m[0], c, 0)),
            ]
            + [pl.BlockSpec(memory_space=pl.ANY)] * len(so_far),
            out_specs=[hid, hid] + [full] * 4,
        ),
        out_shape=[shape((2 * rows, width))] * 2
        + [shape((2 * rows, d_model), F32)] * 2
        + [shape((2 * rows, d_model))] * 2,
        input_output_aliases={5 + i: i for i in range(len(so_far))},
        compiler_params=params(1),
        cost_estimate=cost(8 * rows * width * d_model, 20),
        name="own_half",
    )(meta, pair_a, pair_b, w_in, w_out, *so_far)


def far_half(x, dy, wi, wo, y_in, s_in, chunk, group):
    rows, d_model = x.shape
    width = wi.shape[1]
    steps = width // chunk
    if group is not None:
        rows //= 2
    half = rows // 2

    def body(x_ref, dy_ref, wi_ref, wo_ref, y0, s0, *outs):
        c = pl.program_id(0)
        h, da = hidden_grads(x_ref[...], dy_ref[...], wi_ref[...], wo_ref[...])
        y = nn(h, wo_ref[...])
        s = nt(da, wi_ref[...])
        if group is not None:
            for p in range(2):
                part = slice(p * half, (p + 1) * half)
                outs[p][...] = (y0[part] + y[part]).astype(BF16)
                outs[2 + p][...] = (s0[part] + s[part]).astype(BF16)
            return

        @pl.when(c == 0)
        def _():
            outs[0][...] = y0[...] + y
            outs[1][...] = s0[...] + s

        @pl.when(c > 0)
        def _():
            outs[0][...] += y
            outs[1][...] += s

    full = pl.BlockSpec((rows, d_model), lambda c: (group or 0, 0))
    if group is not None:
        out_specs, out_shape = [whole((half, d_model))] * 4, [shape((half, d_model))] * 4
    else:
        out_specs, out_shape = [full] * 2, [shape((rows, d_model), F32)] * 2
    return pl.pallas_call(
        body,
        grid=(steps,),
        in_specs=[
            full,
            full,
            pl.BlockSpec((d_model, chunk), lambda c: (0, c)),
            pl.BlockSpec((chunk, d_model), lambda c: (c, 0)),
            full,
            full,
        ],
        out_specs=out_specs,
        out_shape=out_shape,
        compiler_params=params(1),
        cost_estimate=cost(8 * rows * width * d_model, 10),
        name="far_half",
    )(x, dy, wi, wo, y_in, s_in)


def finished_grads(meta, x, dy, h, da, n_local, chunk):
    rows, d_model = x.shape
    width = h.shape[1]

    def body(meta_ref, x_ref, dy_ref, h_ref, da_ref, gi, go):
        gi[0] = tn(x_ref[...], da_ref[...])
        go[0] = tn(h_ref[...], dy_ref[...])

    hid = pl.BlockSpec((rows, chunk), lambda c, m: (0, c))
    return pl.pallas_call(
        body,
        grid_spec=pltpu.PrefetchScalarGridSpec(
            num_scalar_prefetch=1,
            grid=(width // chunk,),
            in_specs=[whole((rows, d_model))] * 2 + [hid] * 2,
            out_specs=[
                pl.BlockSpec((1, d_model, chunk), lambda c, m: (m[0], 0, c)),
                pl.BlockSpec((1, chunk, d_model), lambda c, m: (m[0], c, 0)),
            ],
        ),
        out_shape=[shape((n_local, d_model, width), F32), shape((n_local, width, d_model), F32)],
        compiler_params=params(1),
        cost_estimate=cost(4 * rows * width * d_model, 25),
        name="finished_grads",
    )(meta, x, dy, h, da)


def other_grads(meta, pairs, w_in, w_out, grad_w_in, grad_w_out, chunk):
    _, d_model, width = w_in.shape
    cap = pairs[0].shape[1]
    rows = len(pairs) * cap

    def body(meta_ref, *refs):
        parts = refs[: len(pairs)]
        wi, wo, _, _, gi, go, x, dy = refs[len(pairs) :]

        @pl.when(pl.program_id(0) == 0)
        def _():
            for p, part in enumerate(parts):
                x[p * cap : (p + 1) * cap, :] = part[0]
                dy[p * cap : (p + 1) * cap, :] = part[1]

        h, da = hidden_grads(x[...], dy[...], wi[0], wo[0])
        gi[0] = tn(x[...], da)
        go[0] = tn(h, dy[...])

    def other(m):
        return 1 - m[0]

    any_spec = pl.BlockSpec(memory_space=pl.ANY)
    wi_spec = pl.BlockSpec((1, d_model, chunk), lambda c, m: (other(m), 0, c))
    wo_spec = pl.BlockSpec((1, chunk, d_model), lambda c, m: (other(m), c, 0))
    return pl.pallas_call(
        body,
        grid_spec=pltpu.PrefetchScalarGridSpec(
            num_scalar_prefetch=1,
            grid=(width // chunk,),
            in_specs=[whole(pairs[0].shape)] * len(pairs) + [wi_spec, wo_spec, any_spec, any_spec],
            out_specs=[wi_spec, wo_spec],
            scratch_shapes=[pltpu.VMEM((rows, d_model), BF16)] * 2,
        ),
        out_shape=[shape(grad_w_in.shape, F32), shape(grad_w_out.shape, F32)],
        input_output_aliases={len(pairs) + 3: 0, len(pairs) + 4: 1},
        compiler_params=params(1),
        cost_estimate=cost(8 * rows * width * d_model, 25),
        name="other_grads",
    )(meta, *pairs, w_in, w_out, grad_w_in, grad_w_out)


def stack_rows(parts, all_rows):
    @pl.when(pl.program_id(0) == 0)
    def _():
        cap = parts[0].shape[0]
        for p, part in enumerate(parts):
            all_rows[p * cap : (p + 1) * cap, :] = part[...]


def piece_pick(meta_ref, info_v, pieces, cap):
    lane = lax.broadcasted_iota(jnp.int32, (1, cap * len(pieces)), 1)
    codes = lane
    for p, (d, k) in enumerate(pieces):
        owner = jnp.bitwise_xor(meta_ref[1], d) * 2 + jnp.bitwise_xor(meta_ref[0], k)
        codes = jnp.where(lane >= p * cap, lane + (owner - p) * cap, codes)
    return jnp.where(info_v[:, 0:1] == codes.astype(F32), 1.0, 0.0).astype(BF16)


def combine_y(meta, pieces, info, tokens, grad_out, block):
    n_tok, d_model = tokens.shape
    keys, rows = list(pieces), list(pieces.values())
    cap = rows[0].shape[0]
    n_experts = INFO_ROWS - 8

    def body(meta_ref, *refs):
        parts = refs[: len(keys)]
        info_ref, x_ref, gy_ref, out_ref, dlog_ref, dwg_ref, all_rows = refs[len(keys) :]
        stack_rows(parts, all_rows)
        info_v = info_ref[...].T
        y = nn(piece_pick(meta_ref, info_v, keys, cap), all_rows[...])
        gate = info_v[:, 1:2]
        prob = info_v[:, 8:16]
        hot = info_v[:, 2:3] == lax.broadcasted_iota(jnp.int32, prob.shape, 1).astype(F32)
        out_ref[...] = (gate * y).astype(BF16)
        d_gate = jnp.sum(gy_ref[...].astype(F32) * y, axis=1, keepdims=True)
        dlog = (d_gate * prob * (jnp.where(hot, 1.0, 0.0) - gate)).astype(BF16)
        dlog_ref[...] = dlog
        dwg = tn(dlog, x_ref[...])

        @pl.when(pl.program_id(0) == 0)
        def _():
            dwg_ref[...] = dwg

        @pl.when(pl.program_id(0) > 0)
        def _():
            dwg_ref[...] += dwg

    tok = pl.BlockSpec((block, d_model), lambda b, m: (b, 0))
    return pl.pallas_call(
        body,
        grid_spec=pltpu.PrefetchScalarGridSpec(
            num_scalar_prefetch=1,
            grid=(n_tok // block,),
            in_specs=[whole((cap, d_model))] * len(keys)
            + [pl.BlockSpec((INFO_ROWS, block), lambda b, m: (0, b)), tok, tok],
            out_specs=[tok, pl.BlockSpec((block, n_experts), lambda b, m: (b, 0)), whole((n_experts, d_model))],
            scratch_shapes=[pltpu.VMEM((cap * len(keys), d_model), BF16)],
        ),
        out_shape=[shape((n_tok, d_model)), shape((n_tok, n_experts)), shape((n_experts, d_model), F32)],
        compiler_params=params(1),
        cost_estimate=cost(2 * n_tok * cap * len(keys) * d_model, 16),
        name="combine_y",
    )(meta, *rows, info, tokens, grad_out)


def combine_s(meta, pieces, info, extra, block):
    n_tok = info.shape[1]
    keys, rows = list(pieces), list(pieces.values())
    cap, d_model = rows[0].shape

    def body(meta_ref, *refs):
        parts = refs[: len(keys)]
        info_ref, *mid, out_ref, all_rows = refs[len(keys) :]
        stack_rows(parts, all_rows)
        s = nn(piece_pick(meta_ref, info_ref[...].T, keys, cap), all_rows[...])
        if extra:
            so_far, dlog_ref, wg_ref = mid
            s = s + so_far[...].astype(F32) + nn(dlog_ref[...], wg_ref[...])
        out_ref[...] = s.astype(BF16)

    tok = pl.BlockSpec((block, d_model), lambda b, m: (b, 0))
    extra_specs = []
    if extra:
        extra_specs = [tok, pl.BlockSpec((block, extra[1].shape[1]), lambda b, m: (b, 0)), whole(extra[2].shape)]
    return pl.pallas_call(
        body,
        grid_spec=pltpu.PrefetchScalarGridSpec(
            num_scalar_prefetch=1,
            grid=(n_tok // block,),
            in_specs=[whole((cap, d_model))] * len(keys)
            + [pl.BlockSpec((INFO_ROWS, block), lambda b, m: (0, b))]
            + extra_specs,
            out_specs=tok,
            scratch_shapes=[pltpu.VMEM((cap * len(keys), d_model), BF16)],
        ),
        out_shape=shape((n_tok, d_model)),
        compiler_params=params(1),
        cost_estimate=cost(2 * n_tok * cap * len(keys) * d_model, 10),
        name="combine_s",
    )(meta, *rows, info, *extra)


def solution(mesh):
    ep_size = mesh.shape["ep"]
    row_spec = P(("dp", "ep"), None)

    def to_ep(v, d):
        return lax.ppermute(v, "ep", [(i, i ^ d) for i in range(ep_size)])

    def to_twin(v):
        return lax.ppermute(v, "tp", [(0, 1), (1, 0)])

    def block(tokens, grad_out, w_router, w_in, w_out, expert_ids):
        n_tok, d_model = tokens.shape
        n_experts = w_router.shape[1]
        width = w_in.shape[2]
        capacity = (6 * n_tok + 5 * n_experts - 1) // (5 * n_experts)
        cap = (capacity + 15) // 16 * 16
        chunk = width // 3
        tp, ep = lax.axis_index("tp"), lax.axis_index("ep")
        meta = jnp.where(jnp.arange(2) == 0, tp, ep).astype(jnp.int32)

        far_w = {}
        for stage, lo, hi in (("a", 0, 4), ("b", 4, 5), ("c", 5, 6)):
            lo, size = lo * width // 6, (hi - lo) * width // 6
            part_in = lax.dynamic_slice(w_in, (1 - tp, 0, lo), (1, d_model, size))[0]
            part_out = lax.dynamic_slice(w_out, (1 - tp, lo, 0), (1, size, d_model))[0]
            far_w[stage] = to_twin(part_in), to_twin(part_out)

        info = route(expert_ids[None, :], tokens, w_router.T, capacity, cap)

        f2, f3 = dispatch(meta, info, tokens, grad_out, ((2, 0),), cap)
        f2, f3 = to_ep(f2, 2), to_ep(f3, 3)
        f0, f1, g2, g3, g0, g1 = dispatch(meta, info, tokens, grad_out, ((0, 0), (2, 1), (0, 1)), cap)
        f1 = to_ep(f1, 1)
        g2, g3 = to_ep(g2, 2), to_ep(g3, 3)
        g1 = to_ep(g1, 1)

        part = own_half(meta, f0, f1, w_in, w_out, chunk, 0, ())
        h, da, y, s, x, dy = own_half(meta, f2, f3, w_in, w_out, chunk, 1, part)
        y, s = far_half(x, dy, *far_w["a"], y, s, chunk, None)
        y, s = far_half(x, dy, *far_w["b"], y, s, width // 6, None)
        y0, y1, s0, s1 = far_half(x, dy, *far_w["c"], y, s, width // 6, 0)
        y2, y3, s2, s3 = far_half(x, dy, *far_w["c"], y, s, width // 6, 1)

        y1, s1 = to_ep(y1, 1), to_ep(s1, 1)
        y2, y3 = to_ep(y2, 2), to_ep(y3, 3)
        s2, s3 = to_ep(s2, 2), to_ep(s3, 3)
        y_mine, s_mine = [y0, y1, y2, y3], [s0, s1, s2, s3]
        y_twin = [to_twin(v) for v in y_mine]
        s_twin = [to_twin(v) for v in s_mine]

        grads = finished_grads(meta, x, dy, h, da, w_in.shape[0], chunk)
        grad_w_in, grad_w_out = other_grads(meta, (g0, g1, g2, g3), w_in, w_out, *grads, chunk)

        y_all = {(d, k): v for k, side in enumerate((y_mine, y_twin)) for d, v in enumerate(side)}
        s_all = {(d, k): v for k, side in enumerate((s_mine, s_twin)) for d, v in enumerate(side)}
        s_late = {key: s_all.pop(key) for key in ((2, 1), (3, 1))}
        moe_out, dlog, dwg = combine_y(meta, y_all, info, tokens, grad_out, n_tok // 8)
        dwg = dwg + to_ep(dwg, 1)
        dwg = dwg + to_ep(dwg, 2)
        so_far = combine_s(meta, s_all, info, (), n_tok // 8)
        grad_tokens = combine_s(meta, s_late, info, (so_far, dlog, w_router.T), n_tok // 8)
        return moe_out, grad_tokens, grad_w_in, grad_w_out, dwg.T

    in_specs = (row_spec, row_spec, P(None, None), P("ep", None, "tp"), P("ep", "tp", None), P(("dp", "ep")))
    out_specs = (row_spec, row_spec, P(("dp", "ep"), None, "tp"), P(("dp", "ep"), "tp", None), P("dp", None))
    return jax.shard_map(block, mesh=mesh, in_specs=in_specs, out_specs=out_specs, check_vma=False)
```

```python
import jax
import jax.numpy as jnp
from jax import lax
from jax.experimental import pallas as pl
from jax.experimental.pallas import tpu as pltpu
from jax.sharding import PartitionSpec as P


GELU_C = 0.7978845608028654
GELU_K = 0.044715
BF16 = jnp.bfloat16
F32 = jnp.float32
VMEM_LIMIT = 56 * 2**20
INFO_ROWS = 16


def nn(a, b):
    return jnp.dot(a, b, preferred_element_type=F32)


def nt(a, b):
    return lax.dot_general(a, b, (((1,), (1,)), ((), ())), preferred_element_type=F32)


def tn(a, b):
    return lax.dot_general(a, b, (((0,), (0,)), ((), ())), preferred_element_type=F32)


def gelu_and_slope(a):
    sq = a * a
    th = jnp.tanh(a * (GELU_C + (GELU_C * GELU_K) * sq))
    up = 1.0 + th
    act = (0.5 * a) * up
    return act, 0.5 * up + act * (1.0 - th) * (GELU_C + (3.0 * GELU_C * GELU_K) * sq)


def hidden_grads(x, dy, wi, wo):
    a = nn(x, wi)
    dh = nt(dy, wo)
    act, slope = gelu_and_slope(a)
    return act.astype(BF16), (dh * slope).astype(BF16)


def params(dims):
    return pltpu.CompilerParams(dimension_semantics=("arbitrary",) * dims, vmem_limit_bytes=VMEM_LIMIT)


def cost(flops, mib):
    return pl.CostEstimate(flops=int(flops), bytes_accessed=int(mib * 2**20), transcendentals=0)


def shape(dims, dtype=BF16):
    return jax.ShapeDtypeStruct(dims, dtype)


def whole(dims):
    return pl.BlockSpec(dims, lambda *_: (0,) * len(dims))


def route(ids_row, tokens, wg_t, capacity, cap):
    n_experts = wg_t.shape[0]
    n_tok = tokens.shape[0]
    step = 256

    def body(ids_ref, x_ref, wg_ref, info_ref):
        ids = ids_ref[...]
        logits = nt(wg_ref[...], x_ref[...])
        raised = jnp.exp(logits - jnp.max(logits, axis=0, keepdims=True))
        prob = raised / jnp.sum(raised, axis=0, keepdims=True)
        hot = ids == lax.broadcasted_iota(jnp.int32, (n_experts, n_tok), 0)
        hot_f = jnp.where(hot, 1.0, 0.0)
        upper = lax.broadcasted_iota(jnp.int32, (step, step), 0) <= lax.broadcasted_iota(jnp.int32, (step, step), 1)
        upper = jnp.where(upper, 1.0, 0.0).astype(BF16)
        carry = jnp.zeros((n_experts, 1), F32)
        for b in range(n_tok // step):
            cols = slice(b * step, (b + 1) * step)
            seen = nn(hot_f[:, cols].astype(BF16), upper) + carry
            carry = seen[:, step - 1 : step]
            pos = jnp.sum(seen * hot_f[:, cols], axis=0, keepdims=True) - 1.0
            slot = ids[:, cols].astype(F32) * cap + pos
            info_ref[0:1, cols] = jnp.where(pos < capacity, slot, -1.0)
        info_ref[1:2, :] = jnp.sum(hot_f * prob, axis=0, keepdims=True)
        info_ref[2:3, :] = ids.astype(F32)
        info_ref[3:8, :] = jnp.zeros((5, n_tok), F32)
        info_ref[8:16, :] = prob

    return pl.pallas_call(
        body,
        grid=(1,),
        in_specs=[whole(ids_row.shape), whole(tokens.shape), whole(wg_t.shape)],
        out_specs=whole((INFO_ROWS, n_tok)),
        out_shape=shape((INFO_ROWS, n_tok), F32),
        compiler_params=params(1),
        cost_estimate=cost(2e9, 3),
        name="route",
    )(ids_row, tokens, wg_t)


def dispatch(meta, info, tokens, grad_out, groups, cap):
    n_tok, d_model = tokens.shape
    count = len(groups)

    def body(meta_ref, info_ref, x_ref, gy_ref, *outs):
        g = pl.program_id(0)
        first, flip = groups[0]
        for p in range(1, count):
            first = jnp.where(g == p, groups[p][0], first)
            flip = jnp.where(g == p, groups[p][1], flip)
        k = jnp.bitwise_xor(meta_ref[0], flip)
        row = lax.broadcasted_iota(jnp.int32, (2 * cap, 1), 0)
        low = row < cap
        base_a = (jnp.bitwise_xor(meta_ref[1], first) * 2 + k) * cap
        base_b = (jnp.bitwise_xor(meta_ref[1], first + 1) * 2 + k) * cap - cap
        codes = (row + jnp.where(low, base_a, base_b)).astype(F32)
        hit = info_ref[0:1, :] == codes
        pick = jnp.where(hit, 1.0, 0.0).astype(BF16)
        row_gate = jnp.sum(jnp.where(hit, info_ref[1:2, :], 0.0), axis=1, keepdims=True)
        x = nn(pick, x_ref[...]).astype(BF16)
        dy = (row_gate * nn(pick, gy_ref[...])).astype(BF16)
        for p in range(count):

            @pl.when(g == p)
            def _():
                outs[2 * p][0] = x[:cap]
                outs[2 * p][1] = dy[:cap]
                outs[2 * p + 1][0] = x[cap:]
                outs[2 * p + 1][1] = dy[cap:]

    return pl.pallas_call(
        body,
        grid_spec=pltpu.PrefetchScalarGridSpec(
            num_scalar_prefetch=1,
            grid=(count,),
            in_specs=[whole(info.shape), whole(tokens.shape), whole(tokens.shape)],
            out_specs=[whole((2, cap, d_model))] * (2 * count),
        ),
        out_shape=[shape((2, cap, d_model))] * (2 * count),
        compiler_params=params(1),
        cost_estimate=cost(8 * count * cap * n_tok * d_model, 8 + 4 * count),
        name="dispatch",
    )(meta, info, tokens, grad_out)


def own_half(meta, pair_a, pair_b, w_in, w_out, chunk, group, so_far):
    _, d_model, width = w_in.shape
    cap = pair_a.shape[1]
    rows = 2 * cap

    def body(meta_ref, pa, pb, wi, wo, *refs):
        h_ref, da_ref, y_ref, s_ref, x_ref, dy_ref = refs[-6:]
        c = pl.program_id(0)

        @pl.when(c == 0)
        def _():
            x_ref[:cap] = pa[0]
            x_ref[cap:] = pb[0]
            dy_ref[:cap] = pa[1]
            dy_ref[cap:] = pb[1]

        h, da = hidden_grads(x_ref[...], dy_ref[...], wi[0], wo[0])
        h_ref[...] = h
        da_ref[...] = da
        y = nn(h, wo[0])
        s = nt(da, wi[0])

        @pl.when(c == 0)
        def _():
            y_ref[...] = y
            s_ref[...] = s

        @pl.when(c > 0)
        def _():
            y_ref[...] += y
            s_ref[...] += s

    hid = pl.BlockSpec((rows, chunk), lambda c, m: (group, c))
    full = pl.BlockSpec((rows, d_model), lambda c, m: (group, 0))
    return pl.pallas_call(
        body,
        grid_spec=pltpu.PrefetchScalarGridSpec(
            num_scalar_prefetch=1,
            grid=(width // chunk,),
            in_specs=[
                whole(pair_a.shape),
                whole(pair_a.shape),
                pl.BlockSpec((1, d_model, chunk), lambda c, m: (m[0], 0, c)),
                pl.BlockSpec((1, chunk, d_model), lambda c, m: (m[0], c, 0)),
            ]
            + [pl.BlockSpec(memory_space=pl.ANY)] * len(so_far),
            out_specs=[hid, hid] + [full] * 4,
        ),
        out_shape=[shape((2 * rows, width))] * 2
        + [shape((2 * rows, d_model), F32)] * 2
        + [shape((2 * rows, d_model))] * 2,
        input_output_aliases={5 + i: i for i in range(len(so_far))},
        compiler_params=params(1),
        cost_estimate=cost(8 * rows * width * d_model, 20),
        name="own_half",
    )(meta, pair_a, pair_b, w_in, w_out, *so_far)


def far_half(x, dy, wi, wo, y_in, s_in, chunk, group):
    rows, d_model = x.shape
    width = wi.shape[1]
    steps = width // chunk
    if group is not None:
        rows //= 2
    half = rows // 2

    def body(x_ref, dy_ref, wi_ref, wo_ref, y0, s0, *outs):
        c = pl.program_id(0)
        h, da = hidden_grads(x_ref[...], dy_ref[...], wi_ref[...], wo_ref[...])
        y = nn(h, wo_ref[...])
        s = nt(da, wi_ref[...])
        if group is not None:
            for p in range(2):
                part = slice(p * half, (p + 1) * half)
                outs[p][...] = (y0[part] + y[part]).astype(BF16)
                outs[2 + p][...] = (s0[part] + s[part]).astype(BF16)
            return

        @pl.when(c == 0)
        def _():
            outs[0][...] = y0[...] + y
            outs[1][...] = s0[...] + s

        @pl.when(c > 0)
        def _():
            outs[0][...] += y
            outs[1][...] += s

    full = pl.BlockSpec((rows, d_model), lambda c: (group or 0, 0))
    if group is not None:
        out_specs, out_shape = [whole((half, d_model))] * 4, [shape((half, d_model))] * 4
    else:
        out_specs, out_shape = [full] * 2, [shape((rows, d_model), F32)] * 2
    return pl.pallas_call(
        body,
        grid=(steps,),
        in_specs=[
            full,
            full,
            pl.BlockSpec((d_model, chunk), lambda c: (0, c)),
            pl.BlockSpec((chunk, d_model), lambda c: (c, 0)),
            full,
            full,
        ],
        out_specs=out_specs,
        out_shape=out_shape,
        compiler_params=params(1),
        cost_estimate=cost(8 * rows * width * d_model, 10),
        name="far_half",
    )(x, dy, wi, wo, y_in, s_in)


def finished_grads(meta, x, dy, h, da, n_local, chunk):
    rows, d_model = x.shape
    width = h.shape[1]

    def body(meta_ref, x_ref, dy_ref, h_ref, da_ref, gi, go):
        gi[0] = tn(x_ref[...], da_ref[...])
        go[0] = tn(h_ref[...], dy_ref[...])

    hid = pl.BlockSpec((rows, chunk), lambda c, m: (0, c))
    return pl.pallas_call(
        body,
        grid_spec=pltpu.PrefetchScalarGridSpec(
            num_scalar_prefetch=1,
            grid=(width // chunk,),
            in_specs=[whole((rows, d_model))] * 2 + [hid] * 2,
            out_specs=[
                pl.BlockSpec((1, d_model, chunk), lambda c, m: (m[0], 0, c)),
                pl.BlockSpec((1, chunk, d_model), lambda c, m: (m[0], c, 0)),
            ],
        ),
        out_shape=[shape((n_local, d_model, width), F32), shape((n_local, width, d_model), F32)],
        compiler_params=params(1),
        cost_estimate=cost(4 * rows * width * d_model, 25),
        name="finished_grads",
    )(meta, x, dy, h, da)


def other_grads(meta, pairs, w_in, w_out, grad_w_in, grad_w_out, chunk):
    _, d_model, width = w_in.shape
    cap = pairs[0].shape[1]
    rows = len(pairs) * cap

    def body(meta_ref, *refs):
        parts = refs[: len(pairs)]
        wi, wo, _, _, gi, go, x, dy = refs[len(pairs) :]

        @pl.when(pl.program_id(0) == 0)
        def _():
            for p, part in enumerate(parts):
                x[p * cap : (p + 1) * cap, :] = part[0]
                dy[p * cap : (p + 1) * cap, :] = part[1]

        h, da = hidden_grads(x[...], dy[...], wi[0], wo[0])
        gi[0] = tn(x[...], da)
        go[0] = tn(h, dy[...])

    def other(m):
        return 1 - m[0]

    any_spec = pl.BlockSpec(memory_space=pl.ANY)
    wi_spec = pl.BlockSpec((1, d_model, chunk), lambda c, m: (other(m), 0, c))
    wo_spec = pl.BlockSpec((1, chunk, d_model), lambda c, m: (other(m), c, 0))
    return pl.pallas_call(
        body,
        grid_spec=pltpu.PrefetchScalarGridSpec(
            num_scalar_prefetch=1,
            grid=(width // chunk,),
            in_specs=[whole(pairs[0].shape)] * len(pairs) + [wi_spec, wo_spec, any_spec, any_spec],
            out_specs=[wi_spec, wo_spec],
            scratch_shapes=[pltpu.VMEM((rows, d_model), BF16)] * 2,
        ),
        out_shape=[shape(grad_w_in.shape, F32), shape(grad_w_out.shape, F32)],
        input_output_aliases={len(pairs) + 3: 0, len(pairs) + 4: 1},
        compiler_params=params(1),
        cost_estimate=cost(8 * rows * width * d_model, 25),
        name="other_grads",
    )(meta, *pairs, w_in, w_out, grad_w_in, grad_w_out)


def piece_pick(meta_ref, info_v, pieces, cap):
    lane = lax.broadcasted_iota(jnp.int32, (1, cap * len(pieces)), 1)
    codes = lane
    for p, (d, k) in enumerate(pieces):
        owner = jnp.bitwise_xor(meta_ref[1], d) * 2 + jnp.bitwise_xor(meta_ref[0], k)
        codes = jnp.where(lane >= p * cap, lane + (owner - p) * cap, codes)
    return jnp.where(info_v[:, 0:1] == codes.astype(F32), 1.0, 0.0).astype(BF16)


def start_all(copies):
    for copy in copies:
        copy.start()


def wait_all(copies):
    for copy in copies:
        copy.wait()


def combine_y(meta, pieces, info, tokens, grad_out, block):
    n_tok, d_model = tokens.shape
    keys, rows = list(pieces), list(pieces.values())
    count, cap = len(keys), rows[0].shape[0]
    n_experts = INFO_ROWS - 8
    blocks = n_tok // block

    def body(meta_ref, *refs):
        parts = refs[:count]
        info_ref, x_hbm, gy_hbm, out_hbm, dlog_ref, dwg_ref, all_rows, x, gy, out, row_sem, x_sem, gy_sem, out_sem = refs[count:]

        def tok(b):
            return pl.ds(pl.multiple_of(b * block, block), block)

        def row_copy(p):
            return pltpu.make_async_copy(parts[p], all_rows.at[pl.ds(p * cap, cap)], row_sem.at[p])

        def in_copies(b):
            return (
                pltpu.make_async_copy(gy_hbm.at[tok(b)], gy.at[tok(b)], gy_sem.at[b]),
                pltpu.make_async_copy(x_hbm.at[tok(b)], x.at[tok(b)], x_sem.at[b]),
            )

        def out_copy(b):
            return pltpu.make_async_copy(out.at[tok(b)], out_hbm.at[tok(b)], out_sem.at[b])

        start_all([row_copy(p) for p in range(count)])
        for b in range(blocks):
            start_all(in_copies(b))
        dwg_ref[...] = jnp.zeros_like(dwg_ref)
        wait_all([row_copy(p) for p in range(count)])

        @pl.loop(0, blocks)
        def _(b):
            info_v = info_ref[:, tok(b)].T
            y = nn(piece_pick(meta_ref, info_v, keys, cap), all_rows[...])
            gate = info_v[:, 1:2]
            prob = info_v[:, 8:16]
            hot = info_v[:, 2:3] == lax.broadcasted_iota(jnp.int32, prob.shape, 1).astype(F32)
            out[tok(b), :] = (gate * y).astype(BF16)
            wait_all(in_copies(b))
            out_copy(b).start()
            d_gate = jnp.sum(gy[tok(b), :].astype(F32) * y, axis=1, keepdims=True)
            dlog = d_gate * prob * (jnp.where(hot, 1.0, 0.0) - gate)
            dlog_ref[:, tok(b)] = dlog.T
            dwg_ref[...] += tn(dlog.astype(BF16), x[tok(b), :])

        wait_all([out_copy(b) for b in range(blocks)])

    any_spec = pl.BlockSpec(memory_space=pl.ANY)
    return pl.pallas_call(
        body,
        grid_spec=pltpu.PrefetchScalarGridSpec(
            num_scalar_prefetch=1,
            grid=(1,),
            in_specs=[any_spec] * count + [whole((INFO_ROWS, n_tok)), any_spec, any_spec],
            out_specs=[any_spec, whole((n_experts, n_tok)), whole((n_experts, d_model))],
            scratch_shapes=[pltpu.VMEM((cap * count, d_model), BF16)]
            + [pltpu.VMEM((n_tok, d_model), BF16)] * 3
            + [pltpu.SemaphoreType.DMA((count,))]
            + [pltpu.SemaphoreType.DMA((blocks,))] * 3,
        ),
        out_shape=[shape((n_tok, d_model)), shape((n_experts, n_tok), F32), shape((n_experts, d_model), F32)],
        compiler_params=params(1),
        cost_estimate=cost(2 * n_tok * cap * count * d_model, 16),
        name="combine_y",
    )(meta, *rows, info, tokens, grad_out)


def combine_s(meta, pieces, info, extra, block):
    n_tok = info.shape[1]
    keys, rows = list(pieces), list(pieces.values())
    count = len(keys)
    cap, d_model = rows[0].shape
    blocks = n_tok // block

    def body(meta_ref, *refs):
        parts, refs = refs[:count], refs[count:]
        if extra:
            info_ref, dlog_ref, wg_ref, so_hbm, out_hbm, all_rows, out, row_sem, out_sem, so_far, so_sem = refs
        else:
            info_ref, out_hbm, all_rows, out, row_sem, out_sem = refs

        def tok(b):
            return pl.ds(pl.multiple_of(b * block, block), block)

        def row_copy(p):
            return pltpu.make_async_copy(parts[p], all_rows.at[pl.ds(p * cap, cap)], row_sem.at[p])

        def so_copy(b):
            return pltpu.make_async_copy(so_hbm.at[tok(b)], so_far.at[tok(b)], so_sem.at[b])

        def out_copy(b):
            return pltpu.make_async_copy(out.at[tok(b)], out_hbm.at[tok(b)], out_sem.at[b])

        start_all([row_copy(p) for p in range(count)])
        if extra:
            start_all([so_copy(b) for b in range(blocks)])
        wait_all([row_copy(p) for p in range(count)])

        @pl.loop(0, blocks)
        def _(b):
            s = nn(piece_pick(meta_ref, info_ref[:, tok(b)].T, keys, cap), all_rows[...])
            if extra:
                dlog = dlog_ref[:, tok(b)].T.astype(BF16)
                s = s + nn(dlog, wg_ref[...])
                so_copy(b).wait()
                s = s + so_far[tok(b), :].astype(F32)
            out[tok(b), :] = s.astype(BF16)
            out_copy(b).start()

        wait_all([out_copy(b) for b in range(blocks)])

    any_spec = pl.BlockSpec(memory_space=pl.ANY)
    scratch = [pltpu.VMEM((cap * count, d_model), BF16), pltpu.VMEM((n_tok, d_model), BF16)]
    scratch += [pltpu.SemaphoreType.DMA((count,)), pltpu.SemaphoreType.DMA((blocks,))]
    in_specs = [any_spec] * count + [whole((INFO_ROWS, n_tok))]
    if extra:
        so_far, dlog_t, wg_t = extra
        in_specs += [whole(dlog_t.shape), whole(wg_t.shape), any_spec]
        extra = (dlog_t, wg_t, so_far)
        scratch += [pltpu.VMEM((n_tok, d_model), BF16), pltpu.SemaphoreType.DMA((blocks,))]
    return pl.pallas_call(
        body,
        grid_spec=pltpu.PrefetchScalarGridSpec(
            num_scalar_prefetch=1, grid=(1,), in_specs=in_specs, out_specs=any_spec, scratch_shapes=scratch
        ),
        out_shape=shape((n_tok, d_model)),
        compiler_params=params(1),
        cost_estimate=cost(2 * n_tok * cap * count * d_model, 10),
        name="combine_s",
    )(meta, *rows, info, *extra)


def solution(mesh):
    ep_size = mesh.shape["ep"]
    row_spec = P(("dp", "ep"), None)

    def to_ep(v, d):
        return lax.ppermute(v, "ep", [(i, i ^ d) for i in range(ep_size)])

    def to_twin(v):
        return lax.ppermute(v, "tp", [(0, 1), (1, 0)])

    def block(tokens, grad_out, w_router, w_in, w_out, expert_ids):
        n_tok, d_model = tokens.shape
        n_experts = w_router.shape[1]
        width = w_in.shape[2]
        capacity = (6 * n_tok + 5 * n_experts - 1) // (5 * n_experts)
        cap = (capacity + 15) // 16 * 16
        chunk = width // 3
        tp, ep = lax.axis_index("tp"), lax.axis_index("ep")
        meta = jnp.where(jnp.arange(2) == 0, tp, ep).astype(jnp.int32)

        far_w = {}
        for stage, lo, hi in (("a", 0, 2), ("b", 2, 3)):
            lo, size = lo * chunk, (hi - lo) * chunk
            part_in = lax.dynamic_slice(w_in, (1 - tp, 0, lo), (1, d_model, size))[0]
            part_out = lax.dynamic_slice(w_out, (1 - tp, lo, 0), (1, size, d_model))[0]
            far_w[stage] = to_twin(part_in), to_twin(part_out)

        info = route(expert_ids[None, :], tokens, w_router.T, capacity, cap)

        f2, f3 = dispatch(meta, info, tokens, grad_out, ((2, 0),), cap)
        f2, f3 = to_ep(f2, 2), to_ep(f3, 3)
        f0, f1, g2, g3, g0, g1 = dispatch(meta, info, tokens, grad_out, ((0, 0), (2, 1), (0, 1)), cap)
        f1 = to_ep(f1, 1)
        g2, g3 = to_ep(g2, 2), to_ep(g3, 3)
        g1 = to_ep(g1, 1)

        part = own_half(meta, f0, f1, w_in, w_out, chunk, 0, ())
        h, da, y, s, x, dy = own_half(meta, f2, f3, w_in, w_out, chunk, 1, part)
        y, s = far_half(x, dy, *far_w["a"], y, s, chunk, None)
        y0, y1, s0, s1 = far_half(x, dy, *far_w["b"], y, s, chunk, 0)
        y2, y3, s2, s3 = far_half(x, dy, *far_w["b"], y, s, chunk, 1)

        y1, s1 = to_ep(y1, 1), to_ep(s1, 1)
        y2, y3 = to_ep(y2, 2), to_ep(y3, 3)
        s2, s3 = to_ep(s2, 2), to_ep(s3, 3)
        y_mine, s_mine = [y0, y1, y2, y3], [s0, s1, s2, s3]
        y_twin = [to_twin(v) for v in y_mine]
        s_twin = [to_twin(v) for v in s_mine]

        grads = finished_grads(meta, x, dy, h, da, w_in.shape[0], chunk)
        grad_w_in, grad_w_out = other_grads(meta, (g0, g1, g2, g3), w_in, w_out, *grads, chunk)

        y_all = {(d, k): v for k, side in enumerate((y_mine, y_twin)) for d, v in enumerate(side)}
        s_all = {(d, k): v for k, side in enumerate((s_mine, s_twin)) for d, v in enumerate(side)}
        s_late = {key: s_all.pop(key) for key in ((2, 1), (3, 1))}
        moe_out, dlog, dwg = combine_y(meta, y_all, info, tokens, grad_out, n_tok // 4)
        dwg = dwg + to_ep(dwg, 1)
        dwg = dwg + to_ep(dwg, 2)
        so_far = combine_s(meta, s_all, info, (), n_tok // 4)
        grad_tokens = combine_s(meta, s_late, info, (so_far, dlog, w_router.T), n_tok // 4)
        return moe_out, grad_tokens, grad_w_in, grad_w_out, dwg.T

    in_specs = (row_spec, row_spec, P(None, None), P("ep", None, "tp"), P("ep", "tp", None), P(("dp", "ep")))
    out_specs = (row_spec, row_spec, P(("dp", "ep"), None, "tp"), P(("dp", "ep"), "tp", None), P("dp", None))
    return jax.shard_map(block, mesh=mesh, in_specs=in_specs, out_specs=out_specs, check_vma=False)
```

```python
import jax
import jax.numpy as jnp
from jax import lax
from jax.experimental import pallas as pl
from jax.experimental.pallas import tpu as pltpu
from jax.sharding import PartitionSpec as P


GELU_C = 0.7978845608028654
GELU_K = 0.044715
BF16 = jnp.bfloat16
F32 = jnp.float32
VMEM_LIMIT = 56 * 2**20
INFO_ROWS = 16


def nn(a, b):
    return jnp.dot(a, b, preferred_element_type=F32)


def nt(a, b):
    return lax.dot_general(a, b, (((1,), (1,)), ((), ())), preferred_element_type=F32)


def tn(a, b):
    return lax.dot_general(a, b, (((0,), (0,)), ((), ())), preferred_element_type=F32)


def gelu_and_slope(a):
    sq = a * a
    th = jnp.tanh(a * (GELU_C + (GELU_C * GELU_K) * sq))
    up = 1.0 + th
    act = (0.5 * a) * up
    return act, 0.5 * up + act * (1.0 - th) * (GELU_C + (3.0 * GELU_C * GELU_K) * sq)


def hidden_grads(x, dy, wi, wo):
    a = nn(x, wi)
    dh = nt(dy, wo)
    act, slope = gelu_and_slope(a)
    return act.astype(BF16), (dh * slope).astype(BF16)


def params(dims):
    return pltpu.CompilerParams(dimension_semantics=("arbitrary",) * dims, vmem_limit_bytes=VMEM_LIMIT)


def cost(flops, mib):
    return pl.CostEstimate(flops=int(flops), bytes_accessed=int(mib * 2**20), transcendentals=0)


def shape(dims, dtype=BF16):
    return jax.ShapeDtypeStruct(dims, dtype)


def whole(dims):
    return pl.BlockSpec(dims, lambda *_: (0,) * len(dims))


def route(ids_row, tokens, wg_t, capacity, cap):
    n_experts = wg_t.shape[0]
    n_tok = tokens.shape[0]
    step = 256

    def body(ids_ref, x_ref, wg_ref, info_ref):
        ids = ids_ref[...]
        logits = nt(wg_ref[...], x_ref[...])
        raised = jnp.exp(logits - jnp.max(logits, axis=0, keepdims=True))
        prob = raised / jnp.sum(raised, axis=0, keepdims=True)
        hot = ids == lax.broadcasted_iota(jnp.int32, (n_experts, n_tok), 0)
        hot_f = jnp.where(hot, 1.0, 0.0)
        upper = lax.broadcasted_iota(jnp.int32, (step, step), 0) <= lax.broadcasted_iota(jnp.int32, (step, step), 1)
        upper = jnp.where(upper, 1.0, 0.0).astype(BF16)
        carry = jnp.zeros((n_experts, 1), F32)
        for b in range(n_tok // step):
            cols = slice(b * step, (b + 1) * step)
            seen = nn(hot_f[:, cols].astype(BF16), upper) + carry
            carry = seen[:, step - 1 : step]
            pos = jnp.sum(seen * hot_f[:, cols], axis=0, keepdims=True) - 1.0
            slot = ids[:, cols].astype(F32) * cap + pos
            info_ref[0:1, cols] = jnp.where(pos < capacity, slot, -1.0)
        info_ref[1:2, :] = jnp.sum(hot_f * prob, axis=0, keepdims=True)
        info_ref[2:3, :] = ids.astype(F32)
        info_ref[3:8, :] = jnp.zeros((5, n_tok), F32)
        info_ref[8:16, :] = prob

    return pl.pallas_call(
        body,
        grid=(1,),
        in_specs=[whole(ids_row.shape), whole(tokens.shape), whole(wg_t.shape)],
        out_specs=whole((INFO_ROWS, n_tok)),
        out_shape=shape((INFO_ROWS, n_tok), F32),
        compiler_params=params(1),
        cost_estimate=cost(2e9, 3),
        name="route",
    )(ids_row, tokens, wg_t)


def dispatch(meta, info, tokens, grad_out, groups, cap):
    n_tok, d_model = tokens.shape
    count = len(groups)

    def body(meta_ref, info_ref, x_ref, gy_ref, *outs):
        g = pl.program_id(0)
        first, flip = groups[0]
        for p in range(1, count):
            first = jnp.where(g == p, groups[p][0], first)
            flip = jnp.where(g == p, groups[p][1], flip)
        k = jnp.bitwise_xor(meta_ref[0], flip)
        row = lax.broadcasted_iota(jnp.int32, (2 * cap, 1), 0)
        low = row < cap
        base_a = (jnp.bitwise_xor(meta_ref[1], first) * 2 + k) * cap
        base_b = (jnp.bitwise_xor(meta_ref[1], first + 1) * 2 + k) * cap - cap
        codes = (row + jnp.where(low, base_a, base_b)).astype(F32)
        hit = info_ref[0:1, :] == codes
        pick = jnp.where(hit, 1.0, 0.0).astype(BF16)
        row_gate = jnp.sum(jnp.where(hit, info_ref[1:2, :], 0.0), axis=1, keepdims=True)
        x = nn(pick, x_ref[...]).astype(BF16)
        dy = (row_gate * nn(pick, gy_ref[...])).astype(BF16)
        for p in range(count):

            @pl.when(g == p)
            def _():
                outs[2 * p][0] = x[:cap]
                outs[2 * p][1] = dy[:cap]
                outs[2 * p + 1][0] = x[cap:]
                outs[2 * p + 1][1] = dy[cap:]

    return pl.pallas_call(
        body,
        grid_spec=pltpu.PrefetchScalarGridSpec(
            num_scalar_prefetch=1,
            grid=(count,),
            in_specs=[whole(info.shape), whole(tokens.shape), whole(tokens.shape)],
            out_specs=[whole((2, cap, d_model))] * (2 * count),
        ),
        out_shape=[shape((2, cap, d_model))] * (2 * count),
        compiler_params=params(1),
        cost_estimate=cost(8 * count * cap * n_tok * d_model, 8 + 4 * count),
        name="dispatch",
    )(meta, info, tokens, grad_out)


def own_half(meta, pair_a, pair_b, w_in, w_out, chunk, group, so_far):
    _, d_model, width = w_in.shape
    cap = pair_a.shape[1]
    rows = 2 * cap

    def body(meta_ref, pa, pb, wi, wo, *refs):
        h_ref, da_ref, y_ref, s_ref, x_ref, dy_ref = refs[-6:]
        c = pl.program_id(0)

        @pl.when(c == 0)
        def _():
            x_ref[:cap] = pa[0]
            x_ref[cap:] = pb[0]
            dy_ref[:cap] = pa[1]
            dy_ref[cap:] = pb[1]

        h, da = hidden_grads(x_ref[...], dy_ref[...], wi[0], wo[0])
        h_ref[...] = h
        da_ref[...] = da
        y = nn(h, wo[0])
        s = nt(da, wi[0])

        @pl.when(c == 0)
        def _():
            y_ref[...] = y
            s_ref[...] = s

        @pl.when(c > 0)
        def _():
            y_ref[...] += y
            s_ref[...] += s

    hid = pl.BlockSpec((rows, chunk), lambda c, m: (group, c))
    full = pl.BlockSpec((rows, d_model), lambda c, m: (group, 0))
    return pl.pallas_call(
        body,
        grid_spec=pltpu.PrefetchScalarGridSpec(
            num_scalar_prefetch=1,
            grid=(width // chunk,),
            in_specs=[
                whole(pair_a.shape),
                whole(pair_a.shape),
                pl.BlockSpec((1, d_model, chunk), lambda c, m: (m[0], 0, c)),
                pl.BlockSpec((1, chunk, d_model), lambda c, m: (m[0], c, 0)),
            ]
            + [pl.BlockSpec(memory_space=pl.ANY)] * len(so_far),
            out_specs=[hid, hid] + [full] * 4,
        ),
        out_shape=[shape((2 * rows, width))] * 2
        + [shape((2 * rows, d_model), F32)] * 2
        + [shape((2 * rows, d_model))] * 2,
        input_output_aliases={5 + i: i for i in range(len(so_far))},
        compiler_params=params(1),
        cost_estimate=cost(8 * rows * width * d_model, 20),
        name="own_half",
    )(meta, pair_a, pair_b, w_in, w_out, *so_far)


def far_half(x, dy, wi, wo, y_in, s_in, chunk, group):
    rows, d_model = x.shape
    width = wi.shape[1]
    steps = width // chunk
    if group is not None:
        rows //= 2
    half = rows // 2

    def body(x_ref, dy_ref, wi_ref, wo_ref, y0, s0, *outs):
        c = pl.program_id(0)
        h, da = hidden_grads(x_ref[...], dy_ref[...], wi_ref[...], wo_ref[...])
        y = nn(h, wo_ref[...])
        s = nt(da, wi_ref[...])
        if group is not None:
            for p in range(2):
                part = slice(p * half, (p + 1) * half)
                outs[p][...] = (y0[part] + y[part]).astype(BF16)
                outs[2 + p][...] = (s0[part] + s[part]).astype(BF16)
            return

        @pl.when(c == 0)
        def _():
            outs[0][...] = y0[...] + y
            outs[1][...] = s0[...] + s

        @pl.when(c > 0)
        def _():
            outs[0][...] += y
            outs[1][...] += s

    full = pl.BlockSpec((rows, d_model), lambda c: (group or 0, 0))
    if group is not None:
        out_specs, out_shape = [whole((half, d_model))] * 4, [shape((half, d_model))] * 4
    else:
        out_specs, out_shape = [full] * 2, [shape((rows, d_model), F32)] * 2
    return pl.pallas_call(
        body,
        grid=(steps,),
        in_specs=[
            full,
            full,
            pl.BlockSpec((d_model, chunk), lambda c: (0, c)),
            pl.BlockSpec((chunk, d_model), lambda c: (c, 0)),
            full,
            full,
        ],
        out_specs=out_specs,
        out_shape=out_shape,
        compiler_params=params(1),
        cost_estimate=cost(8 * rows * width * d_model, 10),
        name="far_half",
    )(x, dy, wi, wo, y_in, s_in)


def finished_grads(meta, x, dy, h, da, n_local, chunk):
    rows, d_model = x.shape
    width = h.shape[1]

    def body(meta_ref, x_ref, dy_ref, h_ref, da_ref, gi, go):
        gi[0] = tn(x_ref[...], da_ref[...])
        go[0] = tn(h_ref[...], dy_ref[...])

    hid = pl.BlockSpec((rows, chunk), lambda c, m: (0, c))
    return pl.pallas_call(
        body,
        grid_spec=pltpu.PrefetchScalarGridSpec(
            num_scalar_prefetch=1,
            grid=(width // chunk,),
            in_specs=[whole((rows, d_model))] * 2 + [hid] * 2,
            out_specs=[
                pl.BlockSpec((1, d_model, chunk), lambda c, m: (m[0], 0, c)),
                pl.BlockSpec((1, chunk, d_model), lambda c, m: (m[0], c, 0)),
            ],
        ),
        out_shape=[shape((n_local, d_model, width), F32), shape((n_local, width, d_model), F32)],
        compiler_params=params(1),
        cost_estimate=cost(4 * rows * width * d_model, 25),
        name="finished_grads",
    )(meta, x, dy, h, da)


def other_grads(meta, pairs, w_in, w_out, grad_w_in, grad_w_out, chunk):
    _, d_model, width = w_in.shape
    cap = pairs[0].shape[1]
    rows = len(pairs) * cap

    def body(meta_ref, *refs):
        parts = refs[: len(pairs)]
        wi, wo, _, _, gi, go, x, dy = refs[len(pairs) :]

        @pl.when(pl.program_id(0) == 0)
        def _():
            for p, part in enumerate(parts):
                x[p * cap : (p + 1) * cap, :] = part[0]
                dy[p * cap : (p + 1) * cap, :] = part[1]

        h, da = hidden_grads(x[...], dy[...], wi[0], wo[0])
        gi[0] = tn(x[...], da)
        go[0] = tn(h, dy[...])

    def other(m):
        return 1 - m[0]

    any_spec = pl.BlockSpec(memory_space=pl.ANY)
    wi_spec = pl.BlockSpec((1, d_model, chunk), lambda c, m: (other(m), 0, c))
    wo_spec = pl.BlockSpec((1, chunk, d_model), lambda c, m: (other(m), c, 0))
    return pl.pallas_call(
        body,
        grid_spec=pltpu.PrefetchScalarGridSpec(
            num_scalar_prefetch=1,
            grid=(width // chunk,),
            in_specs=[whole(pairs[0].shape)] * len(pairs) + [wi_spec, wo_spec, any_spec, any_spec],
            out_specs=[wi_spec, wo_spec],
            scratch_shapes=[pltpu.VMEM((rows, d_model), BF16)] * 2,
        ),
        out_shape=[shape(grad_w_in.shape, F32), shape(grad_w_out.shape, F32)],
        input_output_aliases={len(pairs) + 3: 0, len(pairs) + 4: 1},
        compiler_params=params(1),
        cost_estimate=cost(8 * rows * width * d_model, 25),
        name="other_grads",
    )(meta, *pairs, w_in, w_out, grad_w_in, grad_w_out)


def stack_rows(parts, all_rows):
    @pl.when(pl.program_id(0) == 0)
    def _():
        cap = parts[0].shape[0]
        for p, part in enumerate(parts):
            all_rows[p * cap : (p + 1) * cap, :] = part[...]


def piece_pick(meta_ref, info_v, pieces, cap):
    lane = lax.broadcasted_iota(jnp.int32, (1, cap * len(pieces)), 1)
    codes = lane
    for p, (d, k) in enumerate(pieces):
        owner = jnp.bitwise_xor(meta_ref[1], d) * 2 + jnp.bitwise_xor(meta_ref[0], k)
        codes = jnp.where(lane >= p * cap, lane + (owner - p) * cap, codes)
    return jnp.where(info_v[:, 0:1] == codes.astype(F32), 1.0, 0.0).astype(BF16)


def combine_y(meta, pieces, info, tokens, grad_out, block):
    n_tok, d_model = tokens.shape
    keys, rows = list(pieces), list(pieces.values())
    cap = rows[0].shape[0]
    n_experts = INFO_ROWS - 8

    def body(meta_ref, *refs):
        parts = refs[: len(keys)]
        info_ref, x_ref, gy_ref, out_ref, dlog_ref, dwg_ref, all_rows = refs[len(keys) :]
        stack_rows(parts, all_rows)
        info_v = info_ref[...].T
        y = nn(piece_pick(meta_ref, info_v, keys, cap), all_rows[...])
        gate = info_v[:, 1:2]
        prob = info_v[:, 8:16]
        hot = info_v[:, 2:3] == lax.broadcasted_iota(jnp.int32, prob.shape, 1).astype(F32)
        out_ref[...] = (gate * y).astype(BF16)
        d_gate = jnp.sum(gy_ref[...].astype(F32) * y, axis=1, keepdims=True)
        dlog = (d_gate * prob * (jnp.where(hot, 1.0, 0.0) - gate)).astype(BF16)
        dlog_ref[...] = dlog
        dwg = tn(dlog, x_ref[...])

        @pl.when(pl.program_id(0) == 0)
        def _():
            dwg_ref[...] = dwg

        @pl.when(pl.program_id(0) > 0)
        def _():
            dwg_ref[...] += dwg

    tok = pl.BlockSpec((block, d_model), lambda b, m: (b, 0))
    return pl.pallas_call(
        body,
        grid_spec=pltpu.PrefetchScalarGridSpec(
            num_scalar_prefetch=1,
            grid=(n_tok // block,),
            in_specs=[whole((cap, d_model))] * len(keys)
            + [pl.BlockSpec((INFO_ROWS, block), lambda b, m: (0, b)), tok, tok],
            out_specs=[tok, pl.BlockSpec((block, n_experts), lambda b, m: (b, 0)), whole((n_experts, d_model))],
            scratch_shapes=[pltpu.VMEM((cap * len(keys), d_model), BF16)],
        ),
        out_shape=[shape((n_tok, d_model)), shape((n_tok, n_experts)), shape((n_experts, d_model), F32)],
        compiler_params=params(1),
        cost_estimate=cost(2 * n_tok * cap * len(keys) * d_model, 16),
        name="combine_y",
    )(meta, *rows, info, tokens, grad_out)


def combine_s(meta, pieces, info, extra, block):
    n_tok = info.shape[1]
    keys, rows = list(pieces), list(pieces.values())
    cap, d_model = rows[0].shape

    def body(meta_ref, *refs):
        parts = refs[: len(keys)]
        info_ref, *mid, out_ref, all_rows = refs[len(keys) :]
        stack_rows(parts, all_rows)
        s = nn(piece_pick(meta_ref, info_ref[...].T, keys, cap), all_rows[...])
        if extra:
            so_far, dlog_ref, wg_ref = mid
            s = s + so_far[...].astype(F32) + nn(dlog_ref[...], wg_ref[...])
        out_ref[...] = s.astype(BF16)

    tok = pl.BlockSpec((block, d_model), lambda b, m: (b, 0))
    extra_specs = []
    if extra:
        extra_specs = [tok, pl.BlockSpec((block, extra[1].shape[1]), lambda b, m: (b, 0)), whole(extra[2].shape)]
    return pl.pallas_call(
        body,
        grid_spec=pltpu.PrefetchScalarGridSpec(
            num_scalar_prefetch=1,
            grid=(n_tok // block,),
            in_specs=[whole((cap, d_model))] * len(keys)
            + [pl.BlockSpec((INFO_ROWS, block), lambda b, m: (0, b))]
            + extra_specs,
            out_specs=tok,
            scratch_shapes=[pltpu.VMEM((cap * len(keys), d_model), BF16)],
        ),
        out_shape=shape((n_tok, d_model)),
        compiler_params=params(1),
        cost_estimate=cost(2 * n_tok * cap * len(keys) * d_model, 10),
        name="combine_s",
    )(meta, *rows, info, *extra)


def solution(mesh):
    ep_size = mesh.shape["ep"]
    row_spec = P(("dp", "ep"), None)

    def to_ep(v, d):
        return lax.ppermute(v, "ep", [(i, i ^ d) for i in range(ep_size)])

    def to_twin(v):
        return lax.ppermute(v, "tp", [(0, 1), (1, 0)])

    def block(tokens, grad_out, w_router, w_in, w_out, expert_ids):
        n_tok, d_model = tokens.shape
        n_experts = w_router.shape[1]
        width = w_in.shape[2]
        capacity = (6 * n_tok + 5 * n_experts - 1) // (5 * n_experts)
        cap = (capacity + 15) // 16 * 16
        chunk = width // 3
        tp, ep = lax.axis_index("tp"), lax.axis_index("ep")
        meta = jnp.where(jnp.arange(2) == 0, tp, ep).astype(jnp.int32)

        far_w = {}
        for stage, lo, hi in (("a", 0, 2), ("b", 2, 3)):
            lo, size = lo * chunk, (hi - lo) * chunk
            part_in = lax.dynamic_slice(w_in, (1 - tp, 0, lo), (1, d_model, size))[0]
            part_out = lax.dynamic_slice(w_out, (1 - tp, lo, 0), (1, size, d_model))[0]
            far_w[stage] = to_twin(part_in), to_twin(part_out)

        info = route(expert_ids[None, :], tokens, w_router.T, capacity, cap)

        f2, f3 = dispatch(meta, info, tokens, grad_out, ((2, 0),), cap)
        f2, f3 = to_ep(f2, 2), to_ep(f3, 3)
        f0, f1, g2, g3, g0, g1 = dispatch(meta, info, tokens, grad_out, ((0, 0), (2, 1), (0, 1)), cap)
        f1 = to_ep(f1, 1)
        g2, g3 = to_ep(g2, 2), to_ep(g3, 3)
        g1 = to_ep(g1, 1)

        part = own_half(meta, f0, f1, w_in, w_out, chunk, 0, ())
        h, da, y, s, x, dy = own_half(meta, f2, f3, w_in, w_out, chunk, 1, part)
        y, s = far_half(x, dy, *far_w["a"], y, s, chunk, None)
        y0, y1, s0, s1 = far_half(x, dy, *far_w["b"], y, s, chunk, 0)
        y2, y3, s2, s3 = far_half(x, dy, *far_w["b"], y, s, chunk, 1)

        y1, s1 = to_ep(y1, 1), to_ep(s1, 1)
        y2, y3 = to_ep(y2, 2), to_ep(y3, 3)
        s2, s3 = to_ep(s2, 2), to_ep(s3, 3)
        y_mine, s_mine = [y0, y1, y2, y3], [s0, s1, s2, s3]
        y_twin = [to_twin(v) for v in y_mine]
        s_twin = [to_twin(v) for v in s_mine]

        grads = finished_grads(meta, x, dy, h, da, w_in.shape[0], chunk)
        grad_w_in, grad_w_out = other_grads(meta, (g0, g1, g2, g3), w_in, w_out, *grads, chunk)

        y_all = {(d, k): v for k, side in enumerate((y_mine, y_twin)) for d, v in enumerate(side)}
        s_all = {(d, k): v for k, side in enumerate((s_mine, s_twin)) for d, v in enumerate(side)}
        s_late = {key: s_all.pop(key) for key in ((2, 1), (3, 1))}
        moe_out, dlog, dwg = combine_y(meta, y_all, info, tokens, grad_out, n_tok // 4)
        dwg = dwg + to_ep(dwg, 1)
        dwg = dwg + to_ep(dwg, 2)
        so_far = combine_s(meta, s_all, info, (), n_tok // 4)
        grad_tokens = combine_s(meta, s_late, info, (so_far, dlog, w_router.T), n_tok // 4)
        return moe_out, grad_tokens, grad_w_in, grad_w_out, dwg.T

    in_specs = (row_spec, row_spec, P(None, None), P("ep", None, "tp"), P("ep", "tp", None), P(("dp", "ep")))
    out_specs = (row_spec, row_spec, P(("dp", "ep"), None, "tp"), P(("dp", "ep"), "tp", None), P("dp", None))
    return jax.shard_map(block, mesh=mesh, in_specs=in_specs, out_specs=out_specs, check_vma=False)
```

```python
import jax
import jax.numpy as jnp
from jax import lax
from jax.experimental import pallas as pl
from jax.experimental.pallas import tpu as pltpu
from jax.sharding import PartitionSpec as P


GELU_C = 0.7978845608028654
GELU_K = 0.044715
BF16 = jnp.bfloat16
F32 = jnp.float32
VMEM_LIMIT = 56 * 2**20
INFO_ROWS = 16


def nn(a, b):
    return jnp.dot(a, b, preferred_element_type=F32)


def nt(a, b):
    return lax.dot_general(a, b, (((1,), (1,)), ((), ())), preferred_element_type=F32)


def tn(a, b):
    return lax.dot_general(a, b, (((0,), (0,)), ((), ())), preferred_element_type=F32)


def gelu_and_slope(a):
    sq = a * a
    th = jnp.tanh(a * (GELU_C + (GELU_C * GELU_K) * sq))
    up = 1.0 + th
    act = (0.5 * a) * up
    return act, 0.5 * up + act * (1.0 - th) * (GELU_C + (3.0 * GELU_C * GELU_K) * sq)


def hidden_grads(x, dy, wi, wo):
    a = nn(x, wi)
    dh = nt(dy, wo)
    act, slope = gelu_and_slope(a)
    return act.astype(BF16), (dh * slope).astype(BF16)


def params(dims):
    return pltpu.CompilerParams(dimension_semantics=("arbitrary",) * dims, vmem_limit_bytes=VMEM_LIMIT)


def cost(flops, mib):
    return pl.CostEstimate(flops=int(flops), bytes_accessed=int(mib * 2**20), transcendentals=0)


def shape(dims, dtype=BF16):
    return jax.ShapeDtypeStruct(dims, dtype)


def whole(dims):
    return pl.BlockSpec(dims, lambda *_: (0,) * len(dims))


def route(ids_row, tokens, wg_t, capacity, cap):
    n_experts = wg_t.shape[0]
    n_tok = tokens.shape[0]
    step = 256

    def body(ids_ref, x_ref, wg_ref, info_ref):
        ids = ids_ref[...]
        logits = nt(wg_ref[...], x_ref[...])
        raised = jnp.exp(logits - jnp.max(logits, axis=0, keepdims=True))
        prob = raised / jnp.sum(raised, axis=0, keepdims=True)
        hot = ids == lax.broadcasted_iota(jnp.int32, (n_experts, n_tok), 0)
        hot_f = jnp.where(hot, 1.0, 0.0)
        upper = lax.broadcasted_iota(jnp.int32, (step, step), 0) <= lax.broadcasted_iota(jnp.int32, (step, step), 1)
        upper = jnp.where(upper, 1.0, 0.0).astype(BF16)
        carry = jnp.zeros((n_experts, 1), F32)
        for b in range(n_tok // step):
            cols = slice(b * step, (b + 1) * step)
            seen = nn(hot_f[:, cols].astype(BF16), upper) + carry
            carry = seen[:, step - 1 : step]
            pos = jnp.sum(seen * hot_f[:, cols], axis=0, keepdims=True) - 1.0
            slot = ids[:, cols].astype(F32) * cap + pos
            info_ref[0:1, cols] = jnp.where(pos < capacity, slot, -1.0)
        info_ref[1:2, :] = jnp.sum(hot_f * prob, axis=0, keepdims=True)
        info_ref[2:3, :] = ids.astype(F32)
        info_ref[3:8, :] = jnp.zeros((5, n_tok), F32)
        info_ref[8:16, :] = prob

    return pl.pallas_call(
        body,
        grid=(1,),
        in_specs=[whole(ids_row.shape), whole(tokens.shape), whole(wg_t.shape)],
        out_specs=whole((INFO_ROWS, n_tok)),
        out_shape=shape((INFO_ROWS, n_tok), F32),
        compiler_params=params(1),
        cost_estimate=cost(2e9, 3),
        name="route",
    )(ids_row, tokens, wg_t)


def dispatch(meta, info, tokens, grad_out, groups, cap):
    n_tok, d_model = tokens.shape
    count = len(groups)

    def body(meta_ref, info_ref, x_ref, gy_ref, *outs):
        g = pl.program_id(0)
        first, flip = groups[0]
        for p in range(1, count):
            first = jnp.where(g == p, groups[p][0], first)
            flip = jnp.where(g == p, groups[p][1], flip)
        k = jnp.bitwise_xor(meta_ref[0], flip)
        row = lax.broadcasted_iota(jnp.int32, (2 * cap, 1), 0)
        low = row < cap
        base_a = (jnp.bitwise_xor(meta_ref[1], first) * 2 + k) * cap
        base_b = (jnp.bitwise_xor(meta_ref[1], first + 1) * 2 + k) * cap - cap
        codes = (row + jnp.where(low, base_a, base_b)).astype(F32)
        hit = info_ref[0:1, :] == codes
        pick = jnp.where(hit, 1.0, 0.0).astype(BF16)
        row_gate = jnp.sum(jnp.where(hit, info_ref[1:2, :], 0.0), axis=1, keepdims=True)
        x = nn(pick, x_ref[...]).astype(BF16)
        dy = (row_gate * nn(pick, gy_ref[...])).astype(BF16)
        for p in range(count):

            @pl.when(g == p)
            def _():
                outs[2 * p][0] = x[:cap]
                outs[2 * p][1] = dy[:cap]
                outs[2 * p + 1][0] = x[cap:]
                outs[2 * p + 1][1] = dy[cap:]

    return pl.pallas_call(
        body,
        grid_spec=pltpu.PrefetchScalarGridSpec(
            num_scalar_prefetch=1,
            grid=(count,),
            in_specs=[whole(info.shape), whole(tokens.shape), whole(tokens.shape)],
            out_specs=[whole((2, cap, d_model))] * (2 * count),
        ),
        out_shape=[shape((2, cap, d_model))] * (2 * count),
        compiler_params=params(1),
        cost_estimate=cost(8 * count * cap * n_tok * d_model, 8 + 4 * count),
        name="dispatch",
    )(meta, info, tokens, grad_out)


def own_half(meta, pair_a, pair_b, w_in, w_out, chunk, group, so_far):
    _, d_model, width = w_in.shape
    cap = pair_a.shape[1]
    rows = 2 * cap

    def body(meta_ref, pa, pb, wi, wo, *refs):
        h_ref, da_ref, y_ref, s_ref, x_ref, dy_ref = refs[-6:]
        c = pl.program_id(0)

        @pl.when(c == 0)
        def _():
            x_ref[:cap] = pa[0]
            x_ref[cap:] = pb[0]
            dy_ref[:cap] = pa[1]
            dy_ref[cap:] = pb[1]

        h, da = hidden_grads(x_ref[...], dy_ref[...], wi[0], wo[0])
        h_ref[...] = h
        da_ref[...] = da
        y = nn(h, wo[0])
        s = nt(da, wi[0])

        @pl.when(c == 0)
        def _():
            y_ref[...] = y
            s_ref[...] = s

        @pl.when(c > 0)
        def _():
            y_ref[...] += y
            s_ref[...] += s

    hid = pl.BlockSpec((rows, chunk), lambda c, m: (group, c))
    full = pl.BlockSpec((rows, d_model), lambda c, m: (group, 0))
    return pl.pallas_call(
        body,
        grid_spec=pltpu.PrefetchScalarGridSpec(
            num_scalar_prefetch=1,
            grid=(width // chunk,),
            in_specs=[
                whole(pair_a.shape),
                whole(pair_a.shape),
                pl.BlockSpec((1, d_model, chunk), lambda c, m: (m[0], 0, c)),
                pl.BlockSpec((1, chunk, d_model), lambda c, m: (m[0], c, 0)),
            ]
            + [pl.BlockSpec(memory_space=pl.ANY)] * len(so_far),
            out_specs=[hid, hid] + [full] * 4,
        ),
        out_shape=[shape((2 * rows, width))] * 2
        + [shape((2 * rows, d_model), F32)] * 2
        + [shape((2 * rows, d_model))] * 2,
        input_output_aliases={5 + i: i for i in range(len(so_far))},
        compiler_params=params(1),
        cost_estimate=cost(8 * rows * width * d_model, 20),
        name="own_half",
    )(meta, pair_a, pair_b, w_in, w_out, *so_far)


def far_half(x, dy, wi, wo, y_in, s_in, chunk, group, joined):
    d_model = x.shape[1]
    rows = x.shape[0] // 2
    cap = rows // 2
    width = wi.shape[1]
    steps = width // chunk

    def body(x_ref, dy_ref, wi_ref, wo_ref, y0, s0, *outs):
        h, da = hidden_grads(x_ref[...], dy_ref[...], wi_ref[...], wo_ref[...])
        y = nn(h, wo_ref[...])
        s = nt(da, wi_ref[...])
        if group is not None:
            for p in range(2):
                part = slice(p * cap, (p + 1) * cap)
                y_out, s_out = (outs[p].at[0], outs[p].at[1]) if joined else (outs[p], outs[2 + p])
                y_out[...] = (y0[part] + y[part]).astype(BF16)
                s_out[...] = (s0[part] + s[part]).astype(BF16)
            return
        c = pl.program_id(1)

        @pl.when(c == 0)
        def _():
            outs[0][...] = y0[...] + y
            outs[1][...] = s0[...] + s

        @pl.when(c > 0)
        def _():
            outs[0][...] += y
            outs[1][...] += s

    if group is None:
        grid = (2, steps)
        full = pl.BlockSpec((rows, d_model), lambda g, c: (g, 0))
        out_specs, out_shape = [full] * 2, [shape(x.shape, F32)] * 2
    else:
        grid = (1, steps)
        full = pl.BlockSpec((rows, d_model), lambda g, c: (group, 0))
        dims, count = ((2, cap, d_model), 2) if joined else ((cap, d_model), 4)
        out_specs, out_shape = [whole(dims)] * count, [shape(dims)] * count
    return pl.pallas_call(
        body,
        grid=grid,
        in_specs=[
            full,
            full,
            pl.BlockSpec((d_model, chunk), lambda g, c: (0, c)),
            pl.BlockSpec((chunk, d_model), lambda g, c: (c, 0)),
            full,
            full,
        ],
        out_specs=out_specs,
        out_shape=out_shape,
        compiler_params=params(2),
        cost_estimate=cost(8 * rows * grid[0] * width * d_model, 10),
        name="far_half",
    )(x, dy, wi, wo, y_in, s_in)


def finished_grads(meta, x, dy, h, da, n_local, chunk, lo, hi, so_far):
    rows, d_model = x.shape
    width = h.shape[1]

    def body(meta_ref, x_ref, dy_ref, h_ref, da_ref, *refs):
        gi, go = refs[-2:]
        gi[0] = tn(x_ref[...], da_ref[...])
        go[0] = tn(h_ref[...], dy_ref[...])

    hid = pl.BlockSpec((rows, chunk), lambda c, m: (0, c + lo))
    return pl.pallas_call(
        body,
        grid_spec=pltpu.PrefetchScalarGridSpec(
            num_scalar_prefetch=1,
            grid=(hi - lo,),
            in_specs=[whole((rows, d_model))] * 2 + [hid] * 2 + [pl.BlockSpec(memory_space=pl.ANY)] * len(so_far),
            out_specs=[
                pl.BlockSpec((1, d_model, chunk), lambda c, m: (m[0], 0, c + lo)),
                pl.BlockSpec((1, chunk, d_model), lambda c, m: (m[0], c + lo, 0)),
            ],
        ),
        out_shape=[shape((n_local, d_model, width), F32), shape((n_local, width, d_model), F32)],
        input_output_aliases={5 + i: i for i in range(len(so_far))},
        compiler_params=params(1),
        cost_estimate=cost(4 * rows * (hi - lo) * chunk * d_model, 8 * (hi - lo)),
        name="finished_grads",
    )(meta, x, dy, h, da, *so_far)


def other_grads(meta, pairs, w_in, w_out, grad_w_in, grad_w_out, chunk):
    _, d_model, width = w_in.shape
    cap = pairs[0].shape[1]
    rows = len(pairs) * cap

    def body(meta_ref, *refs):
        parts = refs[: len(pairs)]
        wi, wo, _, _, gi, go, x, dy = refs[len(pairs) :]

        @pl.when(pl.program_id(0) == 0)
        def _():
            for p, part in enumerate(parts):
                x[p * cap : (p + 1) * cap, :] = part[0]
                dy[p * cap : (p + 1) * cap, :] = part[1]

        h, da = hidden_grads(x[...], dy[...], wi[0], wo[0])
        gi[0] = tn(x[...], da)
        go[0] = tn(h, dy[...])

    def other(m):
        return 1 - m[0]

    any_spec = pl.BlockSpec(memory_space=pl.ANY)
    wi_spec = pl.BlockSpec((1, d_model, chunk), lambda c, m: (other(m), 0, c))
    wo_spec = pl.BlockSpec((1, chunk, d_model), lambda c, m: (other(m), c, 0))
    return pl.pallas_call(
        body,
        grid_spec=pltpu.PrefetchScalarGridSpec(
            num_scalar_prefetch=1,
            grid=(width // chunk,),
            in_specs=[whole(pairs[0].shape)] * len(pairs) + [wi_spec, wo_spec, any_spec, any_spec],
            out_specs=[wi_spec, wo_spec],
            scratch_shapes=[pltpu.VMEM((rows, d_model), BF16)] * 2,
        ),
        out_shape=[shape(grad_w_in.shape, F32), shape(grad_w_out.shape, F32)],
        input_output_aliases={len(pairs) + 3: 0, len(pairs) + 4: 1},
        compiler_params=params(1),
        cost_estimate=cost(8 * rows * width * d_model, 25),
        name="other_grads",
    )(meta, *pairs, w_in, w_out, grad_w_in, grad_w_out)


def stack_rows(parts, all_rows):
    @pl.when(pl.program_id(0) == 0)
    def _():
        cap = parts[0].shape[0]
        for p, part in enumerate(parts):
            all_rows[p * cap : (p + 1) * cap, :] = part[...]


def piece_pick(meta_ref, info_v, pieces, cap):
    lane = lax.broadcasted_iota(jnp.int32, (1, cap * len(pieces)), 1)
    codes = lane
    for p, (d, k) in enumerate(pieces):
        owner = jnp.bitwise_xor(meta_ref[1], d) * 2 + jnp.bitwise_xor(meta_ref[0], k)
        codes = jnp.where(lane >= p * cap, lane + (owner - p) * cap, codes)
    return jnp.where(info_v[:, 0:1] == codes.astype(F32), 1.0, 0.0).astype(BF16)


def piece_specs(rows):
    specs, arrays = [], []
    for piece in rows:
        if isinstance(piece, tuple):
            array, which = piece
            specs.append(pl.BlockSpec((None,) + array.shape[1:], lambda *_, w=which: (w, 0, 0)))
        else:
            array = piece
            specs.append(whole(array.shape))
        arrays.append(array)
    return specs, arrays, arrays[0].shape[-2]


def combine_y(meta, pieces, info, tokens, grad_out, block):
    n_tok, d_model = tokens.shape
    keys = list(pieces)
    specs, rows, cap = piece_specs(pieces.values())
    n_experts = INFO_ROWS - 8

    def body(meta_ref, *refs):
        parts = refs[: len(keys)]
        info_ref, x_ref, gy_ref, out_ref, dlog_ref, dwg_ref, all_rows = refs[len(keys) :]
        stack_rows(parts, all_rows)
        info_v = info_ref[...].T
        y = nn(piece_pick(meta_ref, info_v, keys, cap), all_rows[...])
        gate = info_v[:, 1:2]
        prob = info_v[:, 8:16]
        hot = info_v[:, 2:3] == lax.broadcasted_iota(jnp.int32, prob.shape, 1).astype(F32)
        out_ref[...] = (gate * y).astype(BF16)
        d_gate = jnp.sum(gy_ref[...].astype(F32) * y, axis=1, keepdims=True)
        dlog = (d_gate * prob * (jnp.where(hot, 1.0, 0.0) - gate)).astype(BF16)
        dlog_ref[...] = dlog
        dwg = tn(dlog, x_ref[...])

        @pl.when(pl.program_id(0) == 0)
        def _():
            dwg_ref[...] = dwg

        @pl.when(pl.program_id(0) > 0)
        def _():
            dwg_ref[...] += dwg

    tok = pl.BlockSpec((block, d_model), lambda b, m: (b, 0))
    return pl.pallas_call(
        body,
        grid_spec=pltpu.PrefetchScalarGridSpec(
            num_scalar_prefetch=1,
            grid=(n_tok // block,),
            in_specs=specs
            + [pl.BlockSpec((INFO_ROWS, block), lambda b, m: (0, b)), tok, tok],
            out_specs=[tok, pl.BlockSpec((block, n_experts), lambda b, m: (b, 0)), whole((n_experts, d_model))],
            scratch_shapes=[pltpu.VMEM((cap * len(keys), d_model), BF16)],
        ),
        out_shape=[shape((n_tok, d_model)), shape((n_tok, n_experts)), shape((n_experts, d_model), F32)],
        compiler_params=params(1),
        cost_estimate=cost(2 * n_tok * cap * len(keys) * d_model, 16),
        name="combine_y",
    )(meta, *rows, info, tokens, grad_out)


def combine_s(meta, pieces, info, extra, block):
    n_tok = info.shape[1]
    keys = list(pieces)
    specs, rows, cap = piece_specs(pieces.values())
    d_model = rows[0].shape[-1]

    def body(meta_ref, *refs):
        parts = refs[: len(keys)]
        info_ref, *mid, out_ref, all_rows = refs[len(keys) :]
        stack_rows(parts, all_rows)
        s = nn(piece_pick(meta_ref, info_ref[...].T, keys, cap), all_rows[...])
        if extra:
            so_far, dlog_ref, wg_ref = mid
            s = s + so_far[...].astype(F32) + nn(dlog_ref[...], wg_ref[...])
        out_ref[...] = s.astype(BF16)

    tok = pl.BlockSpec((block, d_model), lambda b, m: (b, 0))
    extra_specs = []
    if extra:
        extra_specs = [tok, pl.BlockSpec((block, extra[1].shape[1]), lambda b, m: (b, 0)), whole(extra[2].shape)]
    return pl.pallas_call(
        body,
        grid_spec=pltpu.PrefetchScalarGridSpec(
            num_scalar_prefetch=1,
            grid=(n_tok // block,),
            in_specs=specs
            + [pl.BlockSpec((INFO_ROWS, block), lambda b, m: (0, b))]
            + extra_specs,
            out_specs=tok,
            scratch_shapes=[pltpu.VMEM((cap * len(keys), d_model), BF16)],
        ),
        out_shape=shape((n_tok, d_model)),
        compiler_params=params(1),
        cost_estimate=cost(2 * n_tok * cap * len(keys) * d_model, 10),
        name="combine_s",
    )(meta, *rows, info, *extra)


def solution(mesh):
    ep_size = mesh.shape["ep"]
    row_spec = P(("dp", "ep"), None)

    def to_ep(v, d):
        return lax.ppermute(v, "ep", [(i, i ^ d) for i in range(ep_size)])

    def to_twin(v):
        return lax.ppermute(v, "tp", [(0, 1), (1, 0)])

    def block(tokens, grad_out, w_router, w_in, w_out, expert_ids):
        n_tok, d_model = tokens.shape
        n_experts = w_router.shape[1]
        width = w_in.shape[2]
        capacity = (6 * n_tok + 5 * n_experts - 1) // (5 * n_experts)
        cap = (capacity + 7) // 8 * 8
        chunk = width // 3
        tp, ep = lax.axis_index("tp"), lax.axis_index("ep")
        meta = jnp.where(jnp.arange(2) == 0, tp, ep).astype(jnp.int32)

        far_w = {}
        for stage, lo, hi in (("a", 0, 2), ("b", 2, 3)):
            lo, size = lo * chunk, (hi - lo) * chunk
            part_in = lax.dynamic_slice(w_in, (1 - tp, 0, lo), (1, d_model, size))[0]
            part_out = lax.dynamic_slice(w_out, (1 - tp, lo, 0), (1, size, d_model))[0]
            far_w[stage] = to_twin(part_in), to_twin(part_out)

        info = route(expert_ids[None, :], tokens, w_router.T, capacity, cap)

        f2, f3 = dispatch(meta, info, tokens, grad_out, ((2, 0),), cap)
        f2, f3 = to_ep(f2, 2), to_ep(f3, 3)
        f0, f1, g2, g3, g0, g1 = dispatch(meta, info, tokens, grad_out, ((0, 0), (2, 1), (0, 1)), cap)
        f1 = to_ep(f1, 1)
        g2, g3 = to_ep(g2, 2), to_ep(g3, 3)
        g1 = to_ep(g1, 1)

        part = own_half(meta, f0, f1, w_in, w_out, chunk, 0, ())
        h, da, y, s, x, dy = own_half(meta, f2, f3, w_in, w_out, chunk, 1, part)
        y, s = far_half(x, dy, *far_w["a"], y, s, chunk, None, False)
        grads = finished_grads(meta, x, dy, h, da, w_in.shape[0], chunk, 0, 1, ())
        ys0, ys1 = far_half(x, dy, *far_w["b"], y, s, chunk, 0, True)
        y2, y3, s2, s3 = far_half(x, dy, *far_w["b"], y, s, chunk, 1, False)

        ys1 = to_ep(ys1, 1)
        y2, y3 = to_ep(y2, 2), to_ep(y3, 3)
        s2, s3 = to_ep(s2, 2), to_ep(s3, 3)
        twin0, twin1 = to_twin(ys0), to_twin(ys1)
        y_mine, s_mine = [(ys0, 0), (ys1, 0), y2, y3], [(ys0, 1), (ys1, 1), s2, s3]
        y_twin = [(twin0, 0), (twin1, 0), to_twin(y2), to_twin(y3)]
        s_twin = [(twin0, 1), (twin1, 1), to_twin(s2), to_twin(s3)]

        grads = finished_grads(meta, x, dy, h, da, w_in.shape[0], chunk, 1, 3, grads)
        grad_w_in, grad_w_out = other_grads(meta, (g0, g1, g2, g3), w_in, w_out, *grads, chunk)

        y_all = {(d, k): v for k, side in enumerate((y_mine, y_twin)) for d, v in enumerate(side)}
        s_all = {(d, k): v for k, side in enumerate((s_mine, s_twin)) for d, v in enumerate(side)}
        s_late = {key: s_all.pop(key) for key in ((2, 1), (3, 1))}
        moe_out, dlog, dwg = combine_y(meta, y_all, info, tokens, grad_out, n_tok // 4)
        dwg = dwg + to_ep(dwg, 1)
        dwg = dwg + to_ep(dwg, 2)
        so_far = combine_s(meta, s_all, info, (), n_tok // 2)
        grad_tokens = combine_s(meta, s_late, info, (so_far, dlog, w_router.T), n_tok // 2)
        return moe_out, grad_tokens, grad_w_in, grad_w_out, dwg.T

    in_specs = (row_spec, row_spec, P(None, None), P("ep", None, "tp"), P("ep", "tp", None), P(("dp", "ep")))
    out_specs = (row_spec, row_spec, P(("dp", "ep"), None, "tp"), P(("dp", "ep"), "tp", None), P("dp", None))
    return jax.shard_map(block, mesh=mesh, in_specs=in_specs, out_specs=out_specs, check_vma=False)
```

```python
import jax
import jax.numpy as jnp
from jax import lax
from jax.experimental import pallas as pl
from jax.experimental.pallas import tpu as pltpu
from jax.sharding import PartitionSpec as P


GELU_C = 0.7978845608028654
GELU_K = 0.044715
BF16 = jnp.bfloat16
F32 = jnp.float32
VMEM_LIMIT = 56 * 2**20
INFO_ROWS = 16


def nn(a, b):
    return jnp.dot(a, b, preferred_element_type=F32)


def nt(a, b):
    return lax.dot_general(a, b, (((1,), (1,)), ((), ())), preferred_element_type=F32)


def tn(a, b):
    return lax.dot_general(a, b, (((0,), (0,)), ((), ())), preferred_element_type=F32)


def gelu_and_slope(a):
    sq = a * a
    th = jnp.tanh(a * (GELU_C + (GELU_C * GELU_K) * sq))
    up = 1.0 + th
    act = (0.5 * a) * up
    return act, 0.5 * up + act * (1.0 - th) * (GELU_C + (3.0 * GELU_C * GELU_K) * sq)


def hidden_grads(x, dy, wi, wo):
    a = nn(x, wi)
    dh = nt(dy, wo)
    act, slope = gelu_and_slope(a)
    return act.astype(BF16), (dh * slope).astype(BF16)


def params(dims):
    return pltpu.CompilerParams(dimension_semantics=("arbitrary",) * dims, vmem_limit_bytes=VMEM_LIMIT)


def cost(flops, mib):
    return pl.CostEstimate(flops=int(flops), bytes_accessed=int(mib * 2**20), transcendentals=0)


def shape(dims, dtype=BF16):
    return jax.ShapeDtypeStruct(dims, dtype)


def whole(dims):
    return pl.BlockSpec(dims, lambda *_: (0,) * len(dims))


def route(ids_row, tokens, wg_t, capacity, cap):
    n_experts = wg_t.shape[0]
    n_tok = tokens.shape[0]
    step = 256

    def body(ids_ref, x_ref, wg_ref, info_ref):
        ids = ids_ref[...]
        logits = nt(wg_ref[...], x_ref[...])
        raised = jnp.exp(logits - jnp.max(logits, axis=0, keepdims=True))
        prob = raised / jnp.sum(raised, axis=0, keepdims=True)
        hot = ids == lax.broadcasted_iota(jnp.int32, (n_experts, n_tok), 0)
        hot_f = jnp.where(hot, 1.0, 0.0)
        upper = lax.broadcasted_iota(jnp.int32, (step, step), 0) <= lax.broadcasted_iota(jnp.int32, (step, step), 1)
        upper = jnp.where(upper, 1.0, 0.0).astype(BF16)
        carry = jnp.zeros((n_experts, 1), F32)
        for b in range(n_tok // step):
            cols = slice(b * step, (b + 1) * step)
            seen = nn(hot_f[:, cols].astype(BF16), upper) + carry
            carry = seen[:, step - 1 : step]
            pos = jnp.sum(seen * hot_f[:, cols], axis=0, keepdims=True) - 1.0
            slot = ids[:, cols].astype(F32) * cap + pos
            info_ref[0:1, cols] = jnp.where(pos < capacity, slot, -1.0)
        info_ref[1:2, :] = jnp.sum(hot_f * prob, axis=0, keepdims=True)
        info_ref[2:3, :] = ids.astype(F32)
        info_ref[3:8, :] = jnp.zeros((5, n_tok), F32)
        info_ref[8:16, :] = prob

    return pl.pallas_call(
        body,
        grid=(1,),
        in_specs=[whole(ids_row.shape), whole(tokens.shape), whole(wg_t.shape)],
        out_specs=whole((INFO_ROWS, n_tok)),
        out_shape=shape((INFO_ROWS, n_tok), F32),
        compiler_params=params(1),
        cost_estimate=cost(2e9, 3),
        name="route",
    )(ids_row, tokens, wg_t)


def dispatch(meta, info, tokens, grad_out, groups, cap):
    n_tok, d_model = tokens.shape
    count = len(groups)

    def body(meta_ref, info_ref, x_ref, gy_ref, *outs):
        g = pl.program_id(0)
        first, flip = groups[0]
        for p in range(1, count):
            first = jnp.where(g == p, groups[p][0], first)
            flip = jnp.where(g == p, groups[p][1], flip)
        k = jnp.bitwise_xor(meta_ref[0], flip)
        row = lax.broadcasted_iota(jnp.int32, (2 * cap, 1), 0)
        low = row < cap
        base_a = (jnp.bitwise_xor(meta_ref[1], first) * 2 + k) * cap
        base_b = (jnp.bitwise_xor(meta_ref[1], first + 1) * 2 + k) * cap - cap
        codes = (row + jnp.where(low, base_a, base_b)).astype(F32)
        hit = info_ref[0:1, :] == codes
        pick = jnp.where(hit, 1.0, 0.0).astype(BF16)
        row_gate = jnp.sum(jnp.where(hit, info_ref[1:2, :], 0.0), axis=1, keepdims=True)
        x = nn(pick, x_ref[...]).astype(BF16)
        dy = (row_gate * nn(pick, gy_ref[...])).astype(BF16)
        for p in range(count):

            @pl.when(g == p)
            def _():
                outs[2 * p][0] = x[:cap]
                outs[2 * p][1] = dy[:cap]
                outs[2 * p + 1][0] = x[cap:]
                outs[2 * p + 1][1] = dy[cap:]

    return pl.pallas_call(
        body,
        grid_spec=pltpu.PrefetchScalarGridSpec(
            num_scalar_prefetch=1,
            grid=(count,),
            in_specs=[whole(info.shape), whole(tokens.shape), whole(tokens.shape)],
            out_specs=[whole((2, cap, d_model))] * (2 * count),
        ),
        out_shape=[shape((2, cap, d_model))] * (2 * count),
        compiler_params=params(1),
        cost_estimate=cost(8 * count * cap * n_tok * d_model, 8 + 4 * count),
        name="dispatch",
    )(meta, info, tokens, grad_out)


def own_half(meta, pair_a, pair_b, w_in, w_out, chunk, group, so_far):
    _, d_model, width = w_in.shape
    cap = pair_a.shape[1]
    rows = 2 * cap

    def body(meta_ref, pa, pb, wi, wo, *refs):
        h_ref, da_ref, y_ref, s_ref, x_ref, dy_ref = refs[-6:]
        c = pl.program_id(0)

        @pl.when(c == 0)
        def _():
            x_ref[:cap] = pa[0]
            x_ref[cap:] = pb[0]
            dy_ref[:cap] = pa[1]
            dy_ref[cap:] = pb[1]

        h, da = hidden_grads(x_ref[...], dy_ref[...], wi[0], wo[0])
        h_ref[...] = h
        da_ref[...] = da
        y = nn(h, wo[0])
        s = nt(da, wi[0])

        @pl.when(c == 0)
        def _():
            y_ref[...] = y
            s_ref[...] = s

        @pl.when(c > 0)
        def _():
            y_ref[...] += y
            s_ref[...] += s

    hid = pl.BlockSpec((rows, chunk), lambda c, m: (group, c))
    full = pl.BlockSpec((rows, d_model), lambda c, m: (group, 0))
    return pl.pallas_call(
        body,
        grid_spec=pltpu.PrefetchScalarGridSpec(
            num_scalar_prefetch=1,
            grid=(width // chunk,),
            in_specs=[
                whole(pair_a.shape),
                whole(pair_a.shape),
                pl.BlockSpec((1, d_model, chunk), lambda c, m: (m[0], 0, c)),
                pl.BlockSpec((1, chunk, d_model), lambda c, m: (m[0], c, 0)),
            ]
            + [pl.BlockSpec(memory_space=pl.ANY)] * len(so_far),
            out_specs=[hid, hid] + [full] * 4,
        ),
        out_shape=[shape((2 * rows, width))] * 2
        + [shape((2 * rows, d_model), F32)] * 2
        + [shape((2 * rows, d_model))] * 2,
        input_output_aliases={5 + i: i for i in range(len(so_far))},
        compiler_params=params(1),
        cost_estimate=cost(8 * rows * width * d_model, 20),
        name="own_half",
    )(meta, pair_a, pair_b, w_in, w_out, *so_far)


def far_half(x, dy, wi, wo, y_in, s_in, chunk, group, joined):
    d_model = x.shape[1]
    rows = x.shape[0] // 2
    cap = rows // 2
    width = wi.shape[1]
    steps = width // chunk

    def body(x_ref, dy_ref, wi_ref, wo_ref, y0, s0, *outs):
        h, da = hidden_grads(x_ref[...], dy_ref[...], wi_ref[...], wo_ref[...])
        y = nn(h, wo_ref[...])
        s = nt(da, wi_ref[...])
        if group is not None:
            for p in range(2):
                part = slice(p * cap, (p + 1) * cap)
                y_out, s_out = (outs[p].at[0], outs[p].at[1]) if joined else (outs[p], outs[2 + p])
                y_out[...] = (y0[part] + y[part]).astype(BF16)
                s_out[...] = (s0[part] + s[part]).astype(BF16)
            return
        c = pl.program_id(1)

        @pl.when(c == 0)
        def _():
            outs[0][...] = y0[...] + y
            outs[1][...] = s0[...] + s

        @pl.when(c > 0)
        def _():
            outs[0][...] += y
            outs[1][...] += s

    if group is None:
        grid = (2, steps)
        full = pl.BlockSpec((rows, d_model), lambda g, c: (g, 0))
        out_specs, out_shape = [full] * 2, [shape(x.shape, F32)] * 2
    else:
        grid = (1, steps)
        full = pl.BlockSpec((rows, d_model), lambda g, c: (group, 0))
        dims, count = ((2, cap, d_model), 2) if joined else ((cap, d_model), 4)
        out_specs, out_shape = [whole(dims)] * count, [shape(dims)] * count
    return pl.pallas_call(
        body,
        grid=grid,
        in_specs=[
            full,
            full,
            pl.BlockSpec((d_model, chunk), lambda g, c: (0, c)),
            pl.BlockSpec((chunk, d_model), lambda g, c: (c, 0)),
            full,
            full,
        ],
        out_specs=out_specs,
        out_shape=out_shape,
        compiler_params=params(2),
        cost_estimate=cost(8 * rows * grid[0] * width * d_model, 10),
        name="far_half",
    )(x, dy, wi, wo, y_in, s_in)


def finished_grads(meta, x, dy, h, da, n_local, chunk):
    rows, d_model = x.shape
    width = h.shape[1]

    def body(meta_ref, x_ref, dy_ref, h_ref, da_ref, gi, go):
        gi[0] = tn(x_ref[...], da_ref[...])
        go[0] = tn(h_ref[...], dy_ref[...])

    hid = pl.BlockSpec((rows, chunk), lambda c, m: (0, c))
    return pl.pallas_call(
        body,
        grid_spec=pltpu.PrefetchScalarGridSpec(
            num_scalar_prefetch=1,
            grid=(width // chunk,),
            in_specs=[whole((rows, d_model))] * 2 + [hid] * 2,
            out_specs=[
                pl.BlockSpec((1, d_model, chunk), lambda c, m: (m[0], 0, c)),
                pl.BlockSpec((1, chunk, d_model), lambda c, m: (m[0], c, 0)),
            ],
        ),
        out_shape=[shape((n_local, d_model, width), F32), shape((n_local, width, d_model), F32)],
        compiler_params=params(1),
        cost_estimate=cost(4 * rows * width * d_model, 25),
        name="finished_grads",
    )(meta, x, dy, h, da)


def other_grads(meta, pairs, w_in, w_out, grad_w_in, grad_w_out, chunk):
    _, d_model, width = w_in.shape
    cap = pairs[0].shape[1]
    rows = len(pairs) * cap

    def body(meta_ref, *refs):
        parts = refs[: len(pairs)]
        wi, wo, _, _, gi, go, x, dy = refs[len(pairs) :]

        @pl.when(pl.program_id(0) == 0)
        def _():
            for p, part in enumerate(parts):
                x[p * cap : (p + 1) * cap, :] = part[0]
                dy[p * cap : (p + 1) * cap, :] = part[1]

        h, da = hidden_grads(x[...], dy[...], wi[0], wo[0])
        gi[0] = tn(x[...], da)
        go[0] = tn(h, dy[...])

    def other(m):
        return 1 - m[0]

    any_spec = pl.BlockSpec(memory_space=pl.ANY)
    wi_spec = pl.BlockSpec((1, d_model, chunk), lambda c, m: (other(m), 0, c))
    wo_spec = pl.BlockSpec((1, chunk, d_model), lambda c, m: (other(m), c, 0))
    return pl.pallas_call(
        body,
        grid_spec=pltpu.PrefetchScalarGridSpec(
            num_scalar_prefetch=1,
            grid=(width // chunk,),
            in_specs=[whole(pairs[0].shape)] * len(pairs) + [wi_spec, wo_spec, any_spec, any_spec],
            out_specs=[wi_spec, wo_spec],
            scratch_shapes=[pltpu.VMEM((rows, d_model), BF16)] * 2,
        ),
        out_shape=[shape(grad_w_in.shape, F32), shape(grad_w_out.shape, F32)],
        input_output_aliases={len(pairs) + 3: 0, len(pairs) + 4: 1},
        compiler_params=params(1),
        cost_estimate=cost(8 * rows * width * d_model, 25),
        name="other_grads",
    )(meta, *pairs, w_in, w_out, grad_w_in, grad_w_out)


def stack_rows(parts, all_rows):
    @pl.when(pl.program_id(0) == 0)
    def _():
        cap = parts[0].shape[0]
        for p, part in enumerate(parts):
            all_rows[p * cap : (p + 1) * cap, :] = part[...]


def piece_pick(meta_ref, info_v, pieces, cap):
    lane = lax.broadcasted_iota(jnp.int32, (1, cap * len(pieces)), 1)
    codes = lane
    for p, (d, k) in enumerate(pieces):
        owner = jnp.bitwise_xor(meta_ref[1], d) * 2 + jnp.bitwise_xor(meta_ref[0], k)
        codes = jnp.where(lane >= p * cap, lane + (owner - p) * cap, codes)
    return jnp.where(info_v[:, 0:1] == codes.astype(F32), 1.0, 0.0).astype(BF16)


def piece_specs(rows):
    specs, arrays = [], []
    for piece in rows:
        if isinstance(piece, tuple):
            array, which = piece
            specs.append(pl.BlockSpec((None,) + array.shape[1:], lambda *_, w=which: (w, 0, 0)))
        else:
            array = piece
            specs.append(whole(array.shape))
        arrays.append(array)
    return specs, arrays, arrays[0].shape[-2]


def combine_y(meta, pieces, info, tokens, grad_out, block):
    n_tok, d_model = tokens.shape
    keys = list(pieces)
    specs, rows, cap = piece_specs(pieces.values())
    n_experts = INFO_ROWS - 8

    def body(meta_ref, *refs):
        parts = refs[: len(keys)]
        info_ref, x_ref, gy_ref, out_ref, dlog_ref, dwg_ref, all_rows = refs[len(keys) :]
        stack_rows(parts, all_rows)
        info_v = info_ref[...].T
        y = nn(piece_pick(meta_ref, info_v, keys, cap), all_rows[...])
        gate = info_v[:, 1:2]
        prob = info_v[:, 8:16]
        hot = info_v[:, 2:3] == lax.broadcasted_iota(jnp.int32, prob.shape, 1).astype(F32)
        out_ref[...] = (gate * y).astype(BF16)
        d_gate = jnp.sum(gy_ref[...].astype(F32) * y, axis=1, keepdims=True)
        dlog = (d_gate * prob * (jnp.where(hot, 1.0, 0.0) - gate)).astype(BF16)
        dlog_ref[...] = dlog
        dwg = tn(dlog, x_ref[...])

        @pl.when(pl.program_id(0) == 0)
        def _():
            dwg_ref[...] = dwg

        @pl.when(pl.program_id(0) > 0)
        def _():
            dwg_ref[...] += dwg

    tok = pl.BlockSpec((block, d_model), lambda b, m: (b, 0))
    return pl.pallas_call(
        body,
        grid_spec=pltpu.PrefetchScalarGridSpec(
            num_scalar_prefetch=1,
            grid=(n_tok // block,),
            in_specs=specs
            + [pl.BlockSpec((INFO_ROWS, block), lambda b, m: (0, b)), tok, tok],
            out_specs=[tok, pl.BlockSpec((block, n_experts), lambda b, m: (b, 0)), whole((n_experts, d_model))],
            scratch_shapes=[pltpu.VMEM((cap * len(keys), d_model), BF16)],
        ),
        out_shape=[shape((n_tok, d_model)), shape((n_tok, n_experts)), shape((n_experts, d_model), F32)],
        compiler_params=params(1),
        cost_estimate=cost(2 * n_tok * cap * len(keys) * d_model, 16),
        name="combine_y",
    )(meta, *rows, info, tokens, grad_out)


def combine_s(meta, pieces, info, extra, block):
    n_tok = info.shape[1]
    keys = list(pieces)
    specs, rows, cap = piece_specs(pieces.values())
    d_model = rows[0].shape[-1]

    def body(meta_ref, *refs):
        parts = refs[: len(keys)]
        info_ref, *mid, out_ref, all_rows = refs[len(keys) :]
        stack_rows(parts, all_rows)
        s = nn(piece_pick(meta_ref, info_ref[...].T, keys, cap), all_rows[...])
        if extra:
            so_far, dlog_ref, wg_ref = mid
            s = s + so_far[...].astype(F32) + nn(dlog_ref[...], wg_ref[...])
        out_ref[...] = s.astype(BF16)

    tok = pl.BlockSpec((block, d_model), lambda b, m: (b, 0))
    extra_specs = []
    if extra:
        extra_specs = [tok, pl.BlockSpec((block, extra[1].shape[1]), lambda b, m: (b, 0)), whole(extra[2].shape)]
    return pl.pallas_call(
        body,
        grid_spec=pltpu.PrefetchScalarGridSpec(
            num_scalar_prefetch=1,
            grid=(n_tok // block,),
            in_specs=specs
            + [pl.BlockSpec((INFO_ROWS, block), lambda b, m: (0, b))]
            + extra_specs,
            out_specs=tok,
            scratch_shapes=[pltpu.VMEM((cap * len(keys), d_model), BF16)],
        ),
        out_shape=shape((n_tok, d_model)),
        compiler_params=params(1),
        cost_estimate=cost(2 * n_tok * cap * len(keys) * d_model, 10),
        name="combine_s",
    )(meta, *rows, info, *extra)


def solution(mesh):
    ep_size = mesh.shape["ep"]
    row_spec = P(("dp", "ep"), None)

    def to_ep(v, d):
        return lax.ppermute(v, "ep", [(i, i ^ d) for i in range(ep_size)])

    def to_twin(v):
        return lax.ppermute(v, "tp", [(0, 1), (1, 0)])

    def block(tokens, grad_out, w_router, w_in, w_out, expert_ids):
        n_tok, d_model = tokens.shape
        n_experts = w_router.shape[1]
        width = w_in.shape[2]
        capacity = (6 * n_tok + 5 * n_experts - 1) // (5 * n_experts)
        cap = (capacity + 7) // 8 * 8
        chunk = width // 3
        tp, ep = lax.axis_index("tp"), lax.axis_index("ep")
        meta = jnp.where(jnp.arange(2) == 0, tp, ep).astype(jnp.int32)

        far_w = {}
        for stage, lo, hi in (("a", 0, 2), ("b", 2, 3)):
            lo, size = lo * chunk, (hi - lo) * chunk
            part_in = lax.dynamic_slice(w_in, (1 - tp, 0, lo), (1, d_model, size))[0]
            part_out = lax.dynamic_slice(w_out, (1 - tp, lo, 0), (1, size, d_model))[0]
            far_w[stage] = to_twin(part_in), to_twin(part_out)

        info = route(expert_ids[None, :], tokens, w_router.T, capacity, cap)

        f2, f3 = dispatch(meta, info, tokens, grad_out, ((2, 0),), cap)
        f2, f3 = to_ep(f2, 2), to_ep(f3, 3)
        f0, f1, g2, g3, g0, g1 = dispatch(meta, info, tokens, grad_out, ((0, 0), (2, 1), (0, 1)), cap)
        f1 = to_ep(f1, 1)
        g2, g3 = to_ep(g2, 2), to_ep(g3, 3)
        g1 = to_ep(g1, 1)

        part = own_half(meta, f0, f1, w_in, w_out, chunk, 0, ())
        h, da, y, s, x, dy = own_half(meta, f2, f3, w_in, w_out, chunk, 1, part)
        y, s = far_half(x, dy, *far_w["a"], y, s, chunk, None, False)
        grads = finished_grads(meta, x, dy, h, da, w_in.shape[0], chunk)
        ys0, ys1 = far_half(x, dy, *far_w["b"], y, s, chunk, 0, True)
        y2, y3, s2, s3 = far_half(x, dy, *far_w["b"], y, s, chunk, 1, False)

        ys1 = to_ep(ys1, 1)
        y2, y3 = to_ep(y2, 2), to_ep(y3, 3)
        s2, s3 = to_ep(s2, 2), to_ep(s3, 3)
        twin0, twin1 = to_twin(ys0), to_twin(ys1)
        y_mine, s_mine = [(ys0, 0), (ys1, 0), y2, y3], [(ys0, 1), (ys1, 1), s2, s3]
        y_twin = [(twin0, 0), (twin1, 0), to_twin(y2), to_twin(y3)]
        s_twin = [(twin0, 1), (twin1, 1), to_twin(s2), to_twin(s3)]

        grad_w_in, grad_w_out = other_grads(meta, (g0, g1, g2, g3), w_in, w_out, *grads, chunk)

        y_all = {(d, k): v for k, side in enumerate((y_mine, y_twin)) for d, v in enumerate(side)}
        s_all = {(d, k): v for k, side in enumerate((s_mine, s_twin)) for d, v in enumerate(side)}
        s_late = {key: s_all.pop(key) for key in ((2, 1), (3, 1))}
        moe_out, dlog, dwg = combine_y(meta, y_all, info, tokens, grad_out, n_tok // 2)
        dwg = dwg + to_ep(dwg, 1)
        dwg = dwg + to_ep(dwg, 2)
        so_far = combine_s(meta, s_all, info, (), n_tok // 2)
        grad_tokens = combine_s(meta, s_late, info, (so_far, dlog, w_router.T), n_tok // 2)
        return moe_out, grad_tokens, grad_w_in, grad_w_out, dwg.T

    in_specs = (row_spec, row_spec, P(None, None), P("ep", None, "tp"), P("ep", "tp", None), P(("dp", "ep")))
    out_specs = (row_spec, row_spec, P(("dp", "ep"), None, "tp"), P(("dp", "ep"), "tp", None), P("dp", None))
    return jax.shard_map(block, mesh=mesh, in_specs=in_specs, out_specs=out_specs, check_vma=False)
```

```python
import jax
import jax.numpy as jnp
from jax import lax
from jax.experimental import pallas as pl
from jax.experimental.pallas import tpu as pltpu
from jax.sharding import PartitionSpec as P


GELU_C = 0.7978845608028654
GELU_K = 0.044715
BF16 = jnp.bfloat16
F32 = jnp.float32
VMEM_LIMIT = 67043328
INFO_ROWS = 16


def nn(a, b):
    return jnp.dot(a, b, preferred_element_type=F32)


def nt(a, b):
    return lax.dot_general(a, b, (((1,), (1,)), ((), ())), preferred_element_type=F32)


def tn(a, b):
    return lax.dot_general(a, b, (((0,), (0,)), ((), ())), preferred_element_type=F32)


def gelu_and_slope(a):
    sq = a * a
    th = jnp.tanh(a * (GELU_C + (GELU_C * GELU_K) * sq))
    up = 1.0 + th
    act = (0.5 * a) * up
    return act, 0.5 * up + act * (1.0 - th) * (GELU_C + (3.0 * GELU_C * GELU_K) * sq)


def hidden_grads(x, dy, wi, wo):
    a = nn(x, wi)
    dh = nt(dy, wo)
    act, slope = gelu_and_slope(a)
    return act.astype(BF16), (dh * slope).astype(BF16)


def params(dims):
    return pltpu.CompilerParams(dimension_semantics=("arbitrary",) * dims, vmem_limit_bytes=VMEM_LIMIT)


def cost(flops, mib):
    return pl.CostEstimate(flops=int(flops), bytes_accessed=int(mib * 2**20), transcendentals=0)


def shape(dims, dtype=BF16):
    return jax.ShapeDtypeStruct(dims, dtype)


def whole(dims):
    return pl.BlockSpec(dims, lambda *_: (0,) * len(dims))


def route(ids_row, tokens, wg_t, capacity, cap):
    n_experts = wg_t.shape[0]
    n_tok = tokens.shape[0]
    step = 256

    def body(ids_ref, x_ref, wg_ref, info_ref):
        ids = ids_ref[...]
        logits = nt(wg_ref[...], x_ref[...])
        raised = jnp.exp(logits - jnp.max(logits, axis=0, keepdims=True))
        prob = raised / jnp.sum(raised, axis=0, keepdims=True)
        hot = ids == lax.broadcasted_iota(jnp.int32, (n_experts, n_tok), 0)
        hot_f = jnp.where(hot, 1.0, 0.0)
        upper = lax.broadcasted_iota(jnp.int32, (step, step), 0) <= lax.broadcasted_iota(jnp.int32, (step, step), 1)
        upper = jnp.where(upper, 1.0, 0.0).astype(BF16)
        carry = jnp.zeros((n_experts, 1), F32)
        for b in range(n_tok // step):
            cols = slice(b * step, (b + 1) * step)
            seen = nn(hot_f[:, cols].astype(BF16), upper) + carry
            carry = seen[:, step - 1 : step]
            pos = jnp.sum(seen * hot_f[:, cols], axis=0, keepdims=True) - 1.0
            slot = ids[:, cols].astype(F32) * cap + pos
            info_ref[0:1, cols] = jnp.where(pos < capacity, slot, -1.0)
        info_ref[1:2, :] = jnp.sum(hot_f * prob, axis=0, keepdims=True)
        info_ref[2:3, :] = ids.astype(F32)
        info_ref[3:8, :] = jnp.zeros((5, n_tok), F32)
        info_ref[8:16, :] = prob

    return pl.pallas_call(
        body,
        grid=(1,),
        in_specs=[whole(ids_row.shape), whole(tokens.shape), whole(wg_t.shape)],
        out_specs=whole((INFO_ROWS, n_tok)),
        out_shape=shape((INFO_ROWS, n_tok), F32),
        compiler_params=params(1),
        cost_estimate=cost(2e9, 3),
        name="route",
    )(ids_row, tokens, wg_t)


def dispatch(meta, info, tokens, grad_out, groups, cap):
    n_tok, d_model = tokens.shape
    count = len(groups)

    def body(meta_ref, info_ref, x_ref, gy_ref, *outs):
        g = pl.program_id(0)
        first, flip = groups[0]
        for p in range(1, count):
            first = jnp.where(g == p, groups[p][0], first)
            flip = jnp.where(g == p, groups[p][1], flip)
        k = jnp.bitwise_xor(meta_ref[0], flip)
        row = lax.broadcasted_iota(jnp.int32, (2 * cap, 1), 0)
        low = row < cap
        base_a = (jnp.bitwise_xor(meta_ref[1], first) * 2 + k) * cap
        base_b = (jnp.bitwise_xor(meta_ref[1], first + 1) * 2 + k) * cap - cap
        codes = (row + jnp.where(low, base_a, base_b)).astype(F32)
        hit = info_ref[0:1, :] == codes
        pick = jnp.where(hit, 1.0, 0.0).astype(BF16)
        row_gate = jnp.sum(jnp.where(hit, info_ref[1:2, :], 0.0), axis=1, keepdims=True)
        x = nn(pick, x_ref[...]).astype(BF16)
        dy = (row_gate * nn(pick, gy_ref[...])).astype(BF16)
        for p in range(count):

            @pl.when(g == p)
            def _():
                outs[2 * p][0] = x[:cap]
                outs[2 * p][1] = dy[:cap]
                outs[2 * p + 1][0] = x[cap:]
                outs[2 * p + 1][1] = dy[cap:]

    return pl.pallas_call(
        body,
        grid_spec=pltpu.PrefetchScalarGridSpec(
            num_scalar_prefetch=1,
            grid=(count,),
            in_specs=[whole(info.shape), whole(tokens.shape), whole(tokens.shape)],
            out_specs=[whole((2, cap, d_model))] * (2 * count),
        ),
        out_shape=[shape((2, cap, d_model))] * (2 * count),
        compiler_params=params(1),
        cost_estimate=cost(8 * count * cap * n_tok * d_model, 8 + 4 * count),
        name="dispatch",
    )(meta, info, tokens, grad_out)


def own_half(meta, pair_a, pair_b, w_in, w_out, chunk, group, so_far):
    _, d_model, width = w_in.shape
    cap = pair_a.shape[1]

    def body(meta_ref, pa, pb, wi, wo, *refs):
        h_ref, da_ref, y_ref, s_ref, x_ref, dy_ref = refs[-6:]
        p, c = pl.program_id(0), pl.program_id(1)

        for source, pair in enumerate((pa, pb)):

            @pl.when(jnp.logical_and(c == 0, p == source))
            def _():
                x_ref[...] = pair[0]
                dy_ref[...] = pair[1]

        h, da = hidden_grads(x_ref[...], dy_ref[...], wi[0], wo[0])
        h_ref[...] = h
        da_ref[...] = da
        y = nn(h, wo[0])
        s = nt(da, wi[0])

        @pl.when(c == 0)
        def _():
            y_ref[...] = y
            s_ref[...] = s

        @pl.when(c > 0)
        def _():
            y_ref[...] += y
            s_ref[...] += s

    hid = pl.BlockSpec((cap, chunk), lambda p, c, m: (2 * group + p, c))
    full = pl.BlockSpec((cap, d_model), lambda p, c, m: (2 * group + p, 0))
    return pl.pallas_call(
        body,
        grid_spec=pltpu.PrefetchScalarGridSpec(
            num_scalar_prefetch=1,
            grid=(2, width // chunk),
            in_specs=[
                whole(pair_a.shape),
                whole(pair_a.shape),
                pl.BlockSpec((1, d_model, chunk), lambda p, c, m: (m[0], 0, c)),
                pl.BlockSpec((1, chunk, d_model), lambda p, c, m: (m[0], c, 0)),
            ]
            + [pl.BlockSpec(memory_space=pl.ANY)] * len(so_far),
            out_specs=[hid, hid] + [full] * 4,
        ),
        out_shape=[shape((4 * cap, width))] * 2
        + [shape((4 * cap, d_model), F32)] * 2
        + [shape((4 * cap, d_model))] * 2,
        input_output_aliases={5 + i: i for i in range(len(so_far))},
        compiler_params=params(2),
        cost_estimate=cost(16 * cap * width * d_model, 20),
        name="own_half",
    )(meta, pair_a, pair_b, w_in, w_out, *so_far)


def far_half(x, dy, wi, wo, y_in, s_in, chunk, group, joined):
    d_model = x.shape[1]
    cap = x.shape[0] // 4
    width = wi.shape[1]
    steps = width // chunk

    def body(x_ref, dy_ref, wi_ref, wo_ref, y0, s0, *outs):
        h, da = hidden_grads(x_ref[...], dy_ref[...], wi_ref[...], wo_ref[...])
        y = nn(h, wo_ref[...])
        s = nt(da, wi_ref[...])
        c = pl.program_id(1)
        if group is not None:
            y = (y0[...] + y).astype(BF16)
            s = (s0[...] + s).astype(BF16)
            for p in range(2):

                @pl.when(pl.program_id(0) == p)
                def _():
                    y_out, s_out = (outs[p].at[0], outs[p].at[1]) if joined else (outs[p], outs[2 + p])
                    y_out[...] = y
                    s_out[...] = s

            return

        @pl.when(c == 0)
        def _():
            outs[0][...] = y0[...] + y
            outs[1][...] = s0[...] + s

        @pl.when(c > 0)
        def _():
            outs[0][...] += y
            outs[1][...] += s

    blocks, base = (4, 0) if group is None else (2, 2 * group)
    full = pl.BlockSpec((cap, d_model), lambda p, c: (base + p, 0))
    if group is None:
        out_specs, out_shape = [full] * 2, [shape(x.shape, F32)] * 2
    else:
        dims, count = ((2, cap, d_model), 2) if joined else ((cap, d_model), 4)
        out_specs, out_shape = [whole(dims)] * count, [shape(dims)] * count
    return pl.pallas_call(
        body,
        grid=(blocks, steps),
        in_specs=[
            full,
            full,
            pl.BlockSpec((d_model, chunk), lambda p, c: (0, c)),
            pl.BlockSpec((chunk, d_model), lambda p, c: (c, 0)),
            full,
            full,
        ],
        out_specs=out_specs,
        out_shape=out_shape,
        compiler_params=params(2),
        cost_estimate=cost(8 * cap * blocks * width * d_model, 10),
        name="far_half",
    )(x, dy, wi, wo, y_in, s_in)


def finished_grads(meta, x, dy, h, da, n_local, chunk):
    rows, d_model = x.shape
    width = h.shape[1]

    def body(meta_ref, x_ref, dy_ref, h_ref, da_ref, gi, go):
        gi[0] = tn(x_ref[...], da_ref[...])
        go[0] = tn(h_ref[...], dy_ref[...])

    hid = pl.BlockSpec((rows, chunk), lambda c, m: (0, c))
    return pl.pallas_call(
        body,
        grid_spec=pltpu.PrefetchScalarGridSpec(
            num_scalar_prefetch=1,
            grid=(width // chunk,),
            in_specs=[whole((rows, d_model))] * 2 + [hid] * 2,
            out_specs=[
                pl.BlockSpec((1, d_model, chunk), lambda c, m: (m[0], 0, c)),
                pl.BlockSpec((1, chunk, d_model), lambda c, m: (m[0], c, 0)),
            ],
        ),
        out_shape=[shape((n_local, d_model, width), F32), shape((n_local, width, d_model), F32)],
        compiler_params=params(1),
        cost_estimate=cost(4 * rows * width * d_model, 25),
        name="finished_grads",
    )(meta, x, dy, h, da)


def other_grads(meta, pairs, w_in, w_out, grad_w_in, grad_w_out, chunk):
    _, d_model, width = w_in.shape
    cap = pairs[0].shape[1]
    rows = len(pairs) * cap

    def body(meta_ref, *refs):
        parts = refs[: len(pairs)]
        wi, wo, _, _, gi, go, x, dy = refs[len(pairs) :]

        @pl.when(pl.program_id(0) == 0)
        def _():
            for p, part in enumerate(parts):
                x[p * cap : (p + 1) * cap, :] = part[0]
                dy[p * cap : (p + 1) * cap, :] = part[1]

        h, da = hidden_grads(x[...], dy[...], wi[0], wo[0])
        gi[0] = tn(x[...], da)
        go[0] = tn(h, dy[...])

    def other(m):
        return 1 - m[0]

    any_spec = pl.BlockSpec(memory_space=pl.ANY)
    wi_spec = pl.BlockSpec((1, d_model, chunk), lambda c, m: (other(m), 0, c))
    wo_spec = pl.BlockSpec((1, chunk, d_model), lambda c, m: (other(m), c, 0))
    return pl.pallas_call(
        body,
        grid_spec=pltpu.PrefetchScalarGridSpec(
            num_scalar_prefetch=1,
            grid=(width // chunk,),
            in_specs=[whole(pairs[0].shape)] * len(pairs) + [wi_spec, wo_spec, any_spec, any_spec],
            out_specs=[wi_spec, wo_spec],
            scratch_shapes=[pltpu.VMEM((rows, d_model), BF16)] * 2,
        ),
        out_shape=[shape(grad_w_in.shape, F32), shape(grad_w_out.shape, F32)],
        input_output_aliases={len(pairs) + 3: 0, len(pairs) + 4: 1},
        compiler_params=params(1),
        cost_estimate=cost(8 * rows * width * d_model, 25),
        name="other_grads",
    )(meta, *pairs, w_in, w_out, grad_w_in, grad_w_out)


def stack_rows(parts, all_rows):
    @pl.when(pl.program_id(0) == 0)
    def _():
        cap = parts[0].shape[0]
        for p, part in enumerate(parts):
            all_rows[p * cap : (p + 1) * cap, :] = part[...]


def piece_pick(meta_ref, info_v, pieces, cap):
    lane = lax.broadcasted_iota(jnp.int32, (1, cap * len(pieces)), 1)
    codes = lane
    for p, (d, k) in enumerate(pieces):
        owner = jnp.bitwise_xor(meta_ref[1], d) * 2 + jnp.bitwise_xor(meta_ref[0], k)
        codes = jnp.where(lane >= p * cap, lane + (owner - p) * cap, codes)
    return jnp.where(info_v[:, 0:1] == codes.astype(F32), 1.0, 0.0).astype(BF16)


def piece_specs(rows):
    specs, arrays = [], []
    for piece in rows:
        if isinstance(piece, tuple):
            array, which = piece
            specs.append(pl.BlockSpec((None,) + array.shape[1:], lambda *_, w=which: (w, 0, 0)))
        else:
            array = piece
            specs.append(whole(array.shape))
        arrays.append(array)
    return specs, arrays, arrays[0].shape[-2]


def combine_y(meta, pieces, info, so_far, tokens, grad_out, block):
    n_tok, d_model = tokens.shape
    keys = list(pieces)
    specs, rows, cap = piece_specs(pieces.values())
    n_experts = INFO_ROWS - 8

    def body(meta_ref, *refs):
        parts = refs[: len(keys)]
        info_ref, so_ref, x_ref, gy_ref, out_ref, dlog_ref, dwg_ref, all_rows = refs[len(keys) :]
        stack_rows(parts, all_rows)
        info_v = info_ref[...].T
        y = nn(piece_pick(meta_ref, info_v, keys, cap), all_rows[...]) + so_ref[...].astype(F32)
        gate = info_v[:, 1:2]
        prob = info_v[:, 8:16]
        hot = info_v[:, 2:3] == lax.broadcasted_iota(jnp.int32, prob.shape, 1).astype(F32)
        out_ref[...] = (gate * y).astype(BF16)
        d_gate = jnp.sum(gy_ref[...].astype(F32) * y, axis=1, keepdims=True)
        dlog = (d_gate * prob * (jnp.where(hot, 1.0, 0.0) - gate)).astype(BF16)
        dlog_ref[...] = dlog
        dwg = tn(dlog, x_ref[...])

        @pl.when(pl.program_id(0) == 0)
        def _():
            dwg_ref[...] = dwg

        @pl.when(pl.program_id(0) > 0)
        def _():
            dwg_ref[...] += dwg

    tok = pl.BlockSpec((block, d_model), lambda b, m: (b, 0))
    return pl.pallas_call(
        body,
        grid_spec=pltpu.PrefetchScalarGridSpec(
            num_scalar_prefetch=1,
            grid=(n_tok // block,),
            in_specs=specs
            + [pl.BlockSpec((INFO_ROWS, block), lambda b, m: (0, b)), tok, tok, tok],
            out_specs=[tok, pl.BlockSpec((block, n_experts), lambda b, m: (b, 0)), whole((n_experts, d_model))],
            scratch_shapes=[pltpu.VMEM((cap * len(keys), d_model), BF16)],
        ),
        out_shape=[shape((n_tok, d_model)), shape((n_tok, n_experts)), shape((n_experts, d_model), F32)],
        compiler_params=params(1),
        cost_estimate=cost(2 * n_tok * cap * len(keys) * d_model, 16),
        name="combine_y",
    )(meta, *rows, info, so_far, tokens, grad_out)


def combine_s(meta, pieces, info, extra, block):
    n_tok = info.shape[1]
    keys = list(pieces)
    specs, rows, cap = piece_specs(pieces.values())
    d_model = rows[0].shape[-1]

    def body(meta_ref, *refs):
        parts = refs[: len(keys)]
        info_ref, *mid, out_ref, all_rows = refs[len(keys) :]
        stack_rows(parts, all_rows)
        s = nn(piece_pick(meta_ref, info_ref[...].T, keys, cap), all_rows[...])
        if extra:
            so_far, dlog_ref, wg_ref = mid
            s = s + so_far[...].astype(F32) + nn(dlog_ref[...], wg_ref[...])
        out_ref[...] = s.astype(BF16)

    tok = pl.BlockSpec((block, d_model), lambda b, m: (b, 0))
    extra_specs = []
    if extra:
        extra_specs = [tok, pl.BlockSpec((block, extra[1].shape[1]), lambda b, m: (b, 0)), whole(extra[2].shape)]
    return pl.pallas_call(
        body,
        grid_spec=pltpu.PrefetchScalarGridSpec(
            num_scalar_prefetch=1,
            grid=(n_tok // block,),
            in_specs=specs
            + [pl.BlockSpec((INFO_ROWS, block), lambda b, m: (0, b))]
            + extra_specs,
            out_specs=tok,
            scratch_shapes=[pltpu.VMEM((cap * len(keys), d_model), BF16)],
        ),
        out_shape=shape((n_tok, d_model)),
        compiler_params=params(1),
        cost_estimate=cost(2 * n_tok * cap * len(keys) * d_model, 10),
        name="combine_s",
    )(meta, *rows, info, *extra)


def solution(mesh):
    ep_size = mesh.shape["ep"]
    row_spec = P(("dp", "ep"), None)

    def to_ep(v, d):
        return lax.ppermute(v, "ep", [(i, i ^ d) for i in range(ep_size)])

    def to_twin(v):
        return lax.ppermute(v, "tp", [(0, 1), (1, 0)])

    def block(tokens, grad_out, w_router, w_in, w_out, expert_ids):
        n_tok, d_model = tokens.shape
        n_experts = w_router.shape[1]
        width = w_in.shape[2]
        capacity = (6 * n_tok + 5 * n_experts - 1) // (5 * n_experts)
        cap = (capacity + 7) // 8 * 8
        chunk = width // 3
        tp, ep = lax.axis_index("tp"), lax.axis_index("ep")
        meta = jnp.where(jnp.arange(2) == 0, tp, ep).astype(jnp.int32)

        far_w = {}
        for stage, lo, hi in (("a", 0, 2), ("b", 2, 3)):
            lo, size = lo * chunk, (hi - lo) * chunk
            part_in = lax.dynamic_slice(w_in, (1 - tp, 0, lo), (1, d_model, size))[0]
            part_out = lax.dynamic_slice(w_out, (1 - tp, lo, 0), (1, size, d_model))[0]
            far_w[stage] = to_twin(part_in), to_twin(part_out)

        info = route(expert_ids[None, :], tokens, w_router.T, capacity, cap)

        f2, f3 = dispatch(meta, info, tokens, grad_out, ((2, 0),), cap)
        f2, f3 = to_ep(f2, 2), to_ep(f3, 3)
        f0, f1, g2, g3, g0, g1 = dispatch(meta, info, tokens, grad_out, ((0, 0), (2, 1), (0, 1)), cap)
        f1 = to_ep(f1, 1)
        g2, g3 = to_ep(g2, 2), to_ep(g3, 3)
        g1 = to_ep(g1, 1)

        part = own_half(meta, f0, f1, w_in, w_out, chunk, 0, ())
        h, da, y, s, x, dy = own_half(meta, f2, f3, w_in, w_out, chunk, 1, part)
        y, s = far_half(x, dy, *far_w["a"], y, s, chunk, None, False)
        grads = finished_grads(meta, x, dy, h, da, w_in.shape[0], chunk)
        ys0, ys1 = far_half(x, dy, *far_w["b"], y, s, chunk, 0, True)
        y2, y3, s2, s3 = far_half(x, dy, *far_w["b"], y, s, chunk, 1, False)

        ys1 = to_ep(ys1, 1)
        y2, y3 = to_ep(y2, 2), to_ep(y3, 3)
        s2, s3 = to_ep(s2, 2), to_ep(s3, 3)
        twin0, twin1 = to_twin(ys0), to_twin(ys1)
        y_mine, s_mine = [(ys0, 0), (ys1, 0), y2, y3], [(ys0, 1), (ys1, 1), s2, s3]
        y_twin = [(twin0, 0), (twin1, 0), to_twin(y2), to_twin(y3)]
        s_twin = [(twin0, 1), (twin1, 1), to_twin(s2), to_twin(s3)]

        grad_w_in, grad_w_out = other_grads(meta, (g0, g1, g2, g3), w_in, w_out, *grads, chunk)

        y_all = {(d, k): v for k, side in enumerate((y_mine, y_twin)) for d, v in enumerate(side)}
        s_all = {(d, k): v for k, side in enumerate((s_mine, s_twin)) for d, v in enumerate(side)}
        s_late = {key: s_all.pop(key) for key in ((2, 1), (3, 1))}
        y_late = {key: y_all.pop(key) for key in ((1, 1), (2, 1), (3, 1))}
        y_first = combine_s(meta, y_all, info, (), n_tok // 2)
        moe_out, dlog, dwg = combine_y(meta, y_late, info, y_first, tokens, grad_out, n_tok // 2)
        dwg = dwg + to_ep(dwg, 1)
        dwg = dwg + to_ep(dwg, 2)
        so_far = combine_s(meta, s_all, info, (), n_tok // 2)
        grad_tokens = combine_s(meta, s_late, info, (so_far, dlog, w_router.T), n_tok // 2)
        return moe_out, grad_tokens, grad_w_in, grad_w_out, dwg.T

    in_specs = (row_spec, row_spec, P(None, None), P("ep", None, "tp"), P("ep", "tp", None), P(("dp", "ep")))
    out_specs = (row_spec, row_spec, P(("dp", "ep"), None, "tp"), P(("dp", "ep"), "tp", None), P("dp", None))
    return jax.shard_map(block, mesh=mesh, in_specs=in_specs, out_specs=out_specs, check_vma=False)
```

```python
import jax
import jax.numpy as jnp
from jax import lax
from jax.experimental import pallas as pl
from jax.experimental.pallas import tpu as pltpu
from jax.sharding import PartitionSpec as P


GELU_C = 0.7978845608028654
GELU_K = 0.044715
BF16 = jnp.bfloat16
F32 = jnp.float32
VMEM_LIMIT = 67043328
SMALL_VMEM = 56 * 2**20
INFO_ROWS = 16


def nn(a, b):
    return jnp.dot(a, b, preferred_element_type=F32)


def nt(a, b):
    return lax.dot_general(a, b, (((1,), (1,)), ((), ())), preferred_element_type=F32)


def tn(a, b):
    return lax.dot_general(a, b, (((0,), (0,)), ((), ())), preferred_element_type=F32)


def gelu_and_slope(a):
    sq = a * a
    th = jnp.tanh(a * (GELU_C + (GELU_C * GELU_K) * sq))
    up = 1.0 + th
    act = (0.5 * a) * up
    return act, 0.5 * up + act * (1.0 - th) * (GELU_C + (3.0 * GELU_C * GELU_K) * sq)


def hidden_grads(x, dy, wi, wo):
    a = nn(x, wi)
    dh = nt(dy, wo)
    act, slope = gelu_and_slope(a)
    return act.astype(BF16), (dh * slope).astype(BF16)


def params(dims, vmem=VMEM_LIMIT):
    return pltpu.CompilerParams(dimension_semantics=("arbitrary",) * dims, vmem_limit_bytes=vmem)


def cost(flops, mib):
    return pl.CostEstimate(flops=int(flops), bytes_accessed=int(mib * 2**20), transcendentals=0)


def shape(dims, dtype=BF16):
    return jax.ShapeDtypeStruct(dims, dtype)


def whole(dims):
    return pl.BlockSpec(dims, lambda *_: (0,) * len(dims))


def route_tokens(ids, x, wg_t, info_ref, capacity, cap):
    n_experts, n_tok = wg_t.shape[0], x.shape[0]
    step = 256
    logits = nt(wg_t, x)
    raised = jnp.exp(logits - jnp.max(logits, axis=0, keepdims=True))
    prob = raised / jnp.sum(raised, axis=0, keepdims=True)
    hot = ids == lax.broadcasted_iota(jnp.int32, (n_experts, n_tok), 0)
    hot_f = jnp.where(hot, 1.0, 0.0)
    upper = lax.broadcasted_iota(jnp.int32, (step, step), 0) <= lax.broadcasted_iota(jnp.int32, (step, step), 1)
    upper = jnp.where(upper, 1.0, 0.0).astype(BF16)
    carry = jnp.zeros((n_experts, 1), F32)
    for b in range(n_tok // step):
        cols = slice(b * step, (b + 1) * step)
        seen = nn(hot_f[:, cols].astype(BF16), upper) + carry
        carry = seen[:, step - 1 : step]
        pos = jnp.sum(seen * hot_f[:, cols], axis=0, keepdims=True) - 1.0
        slot = ids[:, cols].astype(F32) * cap + pos
        info_ref[0:1, cols] = jnp.where(pos < capacity, slot, -1.0)
    info_ref[1:2, :] = jnp.sum(hot_f * prob, axis=0, keepdims=True)
    info_ref[2:3, :] = ids.astype(F32)
    info_ref[3:8, :] = jnp.zeros((5, n_tok), F32)
    info_ref[8:16, :] = prob


def pick_rows(meta_ref, info_ref, x_ref, gy_ref, first, flip, cap):
    k = jnp.bitwise_xor(meta_ref[0], flip)
    row = lax.broadcasted_iota(jnp.int32, (2 * cap, 1), 0)
    base_a = (jnp.bitwise_xor(meta_ref[1], first) * 2 + k) * cap
    base_b = (jnp.bitwise_xor(meta_ref[1], first + 1) * 2 + k) * cap - cap
    codes = (row + jnp.where(row < cap, base_a, base_b)).astype(F32)
    hit = info_ref[0:1, :] == codes
    pick = jnp.where(hit, 1.0, 0.0).astype(BF16)
    row_gate = jnp.sum(jnp.where(hit, info_ref[1:2, :], 0.0), axis=1, keepdims=True)
    x = nn(pick, x_ref[...]).astype(BF16)
    return x, (row_gate * nn(pick, gy_ref[...])).astype(BF16)


def route_and_dispatch(meta, ids_row, tokens, grad_out, wg_t, first, flip, capacity, cap):
    n_tok, d_model = tokens.shape

    def body(meta_ref, ids_ref, x_ref, wg_ref, gy_hbm, info_ref, out_a, out_b, gy_ref, sem):
        load = pltpu.make_async_copy(gy_hbm, gy_ref, sem)
        load.start()
        route_tokens(ids_ref[...], x_ref[...], wg_ref[...], info_ref, capacity, cap)
        load.wait()
        x, dy = pick_rows(meta_ref, info_ref, x_ref, gy_ref, first, flip, cap)
        out_a[0], out_a[1], out_b[0], out_b[1] = x[:cap], dy[:cap], x[cap:], dy[cap:]

    return pl.pallas_call(
        body,
        grid_spec=pltpu.PrefetchScalarGridSpec(
            num_scalar_prefetch=1,
            grid=(1,),
            in_specs=[whole(ids_row.shape), whole(tokens.shape), whole(wg_t.shape), pl.BlockSpec(memory_space=pl.ANY)],
            out_specs=[whole((INFO_ROWS, n_tok))] + [whole((2, cap, d_model))] * 2,
            scratch_shapes=[pltpu.VMEM((n_tok, d_model), BF16), pltpu.SemaphoreType.DMA],
        ),
        out_shape=[shape((INFO_ROWS, n_tok), F32)] + [shape((2, cap, d_model))] * 2,
        compiler_params=params(1, SMALL_VMEM),
        cost_estimate=cost(8 * cap * n_tok * d_model, 10),
        name="route",
    )(meta, ids_row, tokens, wg_t, grad_out)


def dispatch(meta, info, tokens, grad_out, groups, cap):
    n_tok, d_model = tokens.shape
    count = len(groups)

    def body(meta_ref, info_ref, x_ref, gy_ref, *refs):
        outs, (stage, sems) = refs[: 2 * count], refs[2 * count :]
        g = pl.program_id(0)
        first, flip = groups[0]
        for p in range(1, count):
            first = jnp.where(g == p, groups[p][0], first)
            flip = jnp.where(g == p, groups[p][1], flip)
        x, dy = pick_rows(meta_ref, info_ref, x_ref, gy_ref, first, flip, cap)
        for half in range(2):
            part = slice(half * cap, (half + 1) * cap)
            stage[2 * g + half, 0] = x[part]
            stage[2 * g + half, 1] = dy[part]

        def store(i):
            return pltpu.make_async_copy(stage.at[i], outs[i], sems.at[i])

        for p in range(count):

            @pl.when(g == p)
            def _():
                store(2 * p).start()
                store(2 * p + 1).start()

        @pl.when(g == count - 1)
        def _():
            for i in range(2 * count):
                store(i).wait()

    return pl.pallas_call(
        body,
        grid_spec=pltpu.PrefetchScalarGridSpec(
            num_scalar_prefetch=1,
            grid=(count,),
            in_specs=[whole(info.shape), whole(tokens.shape), whole(tokens.shape)],
            out_specs=[pl.BlockSpec(memory_space=pl.ANY)] * (2 * count),
            scratch_shapes=[
                pltpu.VMEM((2 * count, 2, cap, d_model), BF16),
                pltpu.SemaphoreType.DMA((2 * count,)),
            ],
        ),
        out_shape=[shape((2, cap, d_model))] * (2 * count),
        compiler_params=params(1, SMALL_VMEM),
        cost_estimate=cost(8 * count * cap * n_tok * d_model, 8 + 4 * count),
        name="dispatch",
    )(meta, info, tokens, grad_out)


def own_half(meta, pair_a, pair_b, w_in, w_out, chunk, group, so_far):
    _, d_model, width = w_in.shape
    cap = pair_a.shape[1]
    rows = 2 * cap

    def body(meta_ref, pa, pb, wi, wo, *refs):
        h_ref, da_ref, y_ref, s_ref, x_ref, dy_ref = refs[-6:]
        c = pl.program_id(0)

        @pl.when(c == 0)
        def _():
            x_ref[:cap] = pa[0]
            x_ref[cap:] = pb[0]
            dy_ref[:cap] = pa[1]
            dy_ref[cap:] = pb[1]

        h, da = hidden_grads(x_ref[...], dy_ref[...], wi[0], wo[0])
        h_ref[...] = h
        da_ref[...] = da
        y = nn(h, wo[0])
        s = nt(da, wi[0])

        @pl.when(c == 0)
        def _():
            y_ref[...] = y
            s_ref[...] = s

        @pl.when(c > 0)
        def _():
            y_ref[...] += y
            s_ref[...] += s

    hid = pl.BlockSpec((rows, chunk), lambda c, m: (group, c))
    full = pl.BlockSpec((rows, d_model), lambda c, m: (group, 0))
    return pl.pallas_call(
        body,
        grid_spec=pltpu.PrefetchScalarGridSpec(
            num_scalar_prefetch=1,
            grid=(width // chunk,),
            in_specs=[
                whole(pair_a.shape),
                whole(pair_a.shape),
                pl.BlockSpec((1, d_model, chunk), lambda c, m: (m[0], 0, c)),
                pl.BlockSpec((1, chunk, d_model), lambda c, m: (m[0], c, 0)),
            ]
            + [pl.BlockSpec(memory_space=pl.ANY)] * len(so_far),
            out_specs=[hid, hid] + [full] * 4,
        ),
        out_shape=[shape((2 * rows, width))] * 2
        + [shape((2 * rows, d_model), F32)] * 2
        + [shape((2 * rows, d_model))] * 2,
        input_output_aliases={5 + i: i for i in range(len(so_far))},
        compiler_params=params(1, SMALL_VMEM),
        cost_estimate=cost(8 * rows * width * d_model, 20),
        name="own_half",
    )(meta, pair_a, pair_b, w_in, w_out, *so_far)


def far_half(x, dy, wi, wo, y_in, s_in, chunk, group, joined):
    d_model = x.shape[1]
    cap = x.shape[0] // 4
    width = wi.shape[1]
    steps = width // chunk

    def body(x_ref, dy_ref, wi_ref, wo_ref, y0, s0, *outs):
        h, da = hidden_grads(x_ref[...], dy_ref[...], wi_ref[...], wo_ref[...])
        y = nn(h, wo_ref[...])
        s = nt(da, wi_ref[...])
        c = pl.program_id(1)
        if group is not None:
            y = (y0[...] + y).astype(BF16)
            s = (s0[...] + s).astype(BF16)
            for p in range(2):

                @pl.when(pl.program_id(0) == p)
                def _():
                    y_out, s_out = (outs[p].at[0], outs[p].at[1]) if joined else (outs[p], outs[2 + p])
                    y_out[...] = y
                    s_out[...] = s

            return

        @pl.when(c == 0)
        def _():
            outs[0][...] = y0[...] + y
            outs[1][...] = s0[...] + s

        @pl.when(c > 0)
        def _():
            outs[0][...] += y
            outs[1][...] += s

    blocks, base, rows = (2, 0, 2 * cap) if group is None else (2, 2 * group, cap)
    full = pl.BlockSpec((rows, d_model), lambda p, c: (base + p, 0))
    if group is None:
        out_specs, out_shape = [full] * 2, [shape(x.shape, F32)] * 2
    else:
        dims, count = ((2, cap, d_model), 2) if joined else ((cap, d_model), 4)
        out_specs, out_shape = [whole(dims)] * count, [shape(dims)] * count
    return pl.pallas_call(
        body,
        grid=(blocks, steps),
        in_specs=[
            full,
            full,
            pl.BlockSpec((d_model, chunk), lambda p, c: (0, c)),
            pl.BlockSpec((chunk, d_model), lambda p, c: (c, 0)),
            full,
            full,
        ],
        out_specs=out_specs,
        out_shape=out_shape,
        compiler_params=params(2, SMALL_VMEM if group is None else VMEM_LIMIT),
        cost_estimate=cost(8 * rows * blocks * width * d_model, 10),
        name="far_half",
    )(x, dy, wi, wo, y_in, s_in)


def finished_grads(meta, x, dy, h, da, n_local, chunk):
    rows, d_model = x.shape
    width = h.shape[1]

    def body(meta_ref, x_ref, dy_ref, h_ref, da_ref, gi, go):
        gi[0] = tn(x_ref[...], da_ref[...])
        go[0] = tn(h_ref[...], dy_ref[...])

    hid = pl.BlockSpec((rows, chunk), lambda c, m: (0, c))
    return pl.pallas_call(
        body,
        grid_spec=pltpu.PrefetchScalarGridSpec(
            num_scalar_prefetch=1,
            grid=(width // chunk,),
            in_specs=[whole((rows, d_model))] * 2 + [hid] * 2,
            out_specs=[
                pl.BlockSpec((1, d_model, chunk), lambda c, m: (m[0], 0, c)),
                pl.BlockSpec((1, chunk, d_model), lambda c, m: (m[0], c, 0)),
            ],
        ),
        out_shape=[shape((n_local, d_model, width), F32), shape((n_local, width, d_model), F32)],
        compiler_params=params(1),
        cost_estimate=cost(4 * rows * width * d_model, 25),
        name="finished_grads",
    )(meta, x, dy, h, da)


def other_grads(meta, pairs, w_in, w_out, grad_w_in, grad_w_out, chunk):
    _, d_model, width = w_in.shape
    cap = pairs[0].shape[1]
    rows = len(pairs) * cap

    def body(meta_ref, *refs):
        parts = refs[: len(pairs)]
        wi, wo, _, _, gi, go, x, dy = refs[len(pairs) :]

        @pl.when(pl.program_id(0) == 0)
        def _():
            for p, part in enumerate(parts):
                x[p * cap : (p + 1) * cap, :] = part[0]
                dy[p * cap : (p + 1) * cap, :] = part[1]

        h, da = hidden_grads(x[...], dy[...], wi[0], wo[0])
        gi[0] = tn(x[...], da)
        go[0] = tn(h, dy[...])

    def other(m):
        return 1 - m[0]

    any_spec = pl.BlockSpec(memory_space=pl.ANY)
    wi_spec = pl.BlockSpec((1, d_model, chunk), lambda c, m: (other(m), 0, c))
    wo_spec = pl.BlockSpec((1, chunk, d_model), lambda c, m: (other(m), c, 0))
    return pl.pallas_call(
        body,
        grid_spec=pltpu.PrefetchScalarGridSpec(
            num_scalar_prefetch=1,
            grid=(width // chunk,),
            in_specs=[whole(pairs[0].shape)] * len(pairs) + [wi_spec, wo_spec, any_spec, any_spec],
            out_specs=[wi_spec, wo_spec],
            scratch_shapes=[pltpu.VMEM((rows, d_model), BF16)] * 2,
        ),
        out_shape=[shape(grad_w_in.shape, F32), shape(grad_w_out.shape, F32)],
        input_output_aliases={len(pairs) + 3: 0, len(pairs) + 4: 1},
        compiler_params=params(1),
        cost_estimate=cost(8 * rows * width * d_model, 25),
        name="other_grads",
    )(meta, *pairs, w_in, w_out, grad_w_in, grad_w_out)


def stack_rows(parts, all_rows):
    @pl.when(pl.program_id(0) == 0)
    def _():
        cap = parts[0].shape[0]
        for p, part in enumerate(parts):
            all_rows[p * cap : (p + 1) * cap, :] = part[...]


def piece_pick(meta_ref, info_v, pieces, cap):
    lane = lax.broadcasted_iota(jnp.int32, (1, cap * len(pieces)), 1)
    codes = lane
    for p, (d, k) in enumerate(pieces):
        owner = jnp.bitwise_xor(meta_ref[1], d) * 2 + jnp.bitwise_xor(meta_ref[0], k)
        codes = jnp.where(lane >= p * cap, lane + (owner - p) * cap, codes)
    return jnp.where(info_v[:, 0:1] == codes.astype(F32), 1.0, 0.0).astype(BF16)


def piece_specs(rows):
    specs, arrays = [], []
    for piece in rows:
        if isinstance(piece, tuple):
            array, which = piece
            specs.append(pl.BlockSpec((None,) + array.shape[1:], lambda *_, w=which: (w, 0, 0)))
        else:
            array = piece
            specs.append(whole(array.shape))
        arrays.append(array)
    return specs, arrays, arrays[0].shape[-2]


def combine_y(meta, pieces, info, so_far, tokens, grad_out, block):
    n_tok, d_model = tokens.shape
    keys = list(pieces)
    specs, rows, cap = piece_specs(pieces.values())
    n_experts = INFO_ROWS - 8

    def body(meta_ref, *refs):
        parts = refs[: len(keys)]
        info_ref, so_ref, x_ref, gy_ref, out_ref, dlog_ref, dwg_ref, all_rows = refs[len(keys) :]
        stack_rows(parts, all_rows)
        info_v = info_ref[...].T
        y = nn(piece_pick(meta_ref, info_v, keys, cap), all_rows[...]) + so_ref[...].astype(F32)
        gate = info_v[:, 1:2]
        prob = info_v[:, 8:16]
        hot = info_v[:, 2:3] == lax.broadcasted_iota(jnp.int32, prob.shape, 1).astype(F32)
        out_ref[...] = (gate * y).astype(BF16)
        d_gate = jnp.sum(gy_ref[...].astype(F32) * y, axis=1, keepdims=True)
        dlog = (d_gate * prob * (jnp.where(hot, 1.0, 0.0) - gate)).astype(BF16)
        dlog_ref[...] = dlog
        dwg = tn(dlog, x_ref[...])

        @pl.when(pl.program_id(0) == 0)
        def _():
            dwg_ref[...] = dwg

        @pl.when(pl.program_id(0) > 0)
        def _():
            dwg_ref[...] += dwg

    tok = pl.BlockSpec((block, d_model), lambda b, m: (b, 0))
    return pl.pallas_call(
        body,
        grid_spec=pltpu.PrefetchScalarGridSpec(
            num_scalar_prefetch=1,
            grid=(n_tok // block,),
            in_specs=specs
            + [pl.BlockSpec((INFO_ROWS, block), lambda b, m: (0, b)), tok, tok, tok],
            out_specs=[tok, pl.BlockSpec((block, n_experts), lambda b, m: (b, 0)), whole((n_experts, d_model))],
            scratch_shapes=[pltpu.VMEM((cap * len(keys), d_model), BF16)],
        ),
        out_shape=[shape((n_tok, d_model)), shape((n_tok, n_experts)), shape((n_experts, d_model), F32)],
        compiler_params=params(1),
        cost_estimate=cost(2 * n_tok * cap * len(keys) * d_model, 16),
        name="combine_y",
    )(meta, *rows, info, so_far, tokens, grad_out)


def combine_s(meta, pieces, info, extra, block):
    n_tok = info.shape[1]
    keys = list(pieces)
    specs, rows, cap = piece_specs(pieces.values())
    d_model = rows[0].shape[-1]

    def body(meta_ref, *refs):
        parts = refs[: len(keys)]
        info_ref, *mid, out_ref, all_rows = refs[len(keys) :]
        stack_rows(parts, all_rows)
        s = nn(piece_pick(meta_ref, info_ref[...].T, keys, cap), all_rows[...])
        if extra:
            so_far, dlog_ref, wg_ref = mid
            s = s + so_far[...].astype(F32) + nn(dlog_ref[...], wg_ref[...])
        out_ref[...] = s.astype(BF16)

    tok = pl.BlockSpec((block, d_model), lambda b, m: (b, 0))
    extra_specs = []
    if extra:
        extra_specs = [tok, pl.BlockSpec((block, extra[1].shape[1]), lambda b, m: (b, 0)), whole(extra[2].shape)]
    return pl.pallas_call(
        body,
        grid_spec=pltpu.PrefetchScalarGridSpec(
            num_scalar_prefetch=1,
            grid=(n_tok // block,),
            in_specs=specs
            + [pl.BlockSpec((INFO_ROWS, block), lambda b, m: (0, b))]
            + extra_specs,
            out_specs=tok,
            scratch_shapes=[pltpu.VMEM((cap * len(keys), d_model), BF16)],
        ),
        out_shape=shape((n_tok, d_model)),
        compiler_params=params(1),
        cost_estimate=cost(2 * n_tok * cap * len(keys) * d_model, 10),
        name="combine_s",
    )(meta, *rows, info, *extra)


def solution(mesh):
    ep_size = mesh.shape["ep"]
    row_spec = P(("dp", "ep"), None)

    def to_ep(v, d):
        return lax.ppermute(v, "ep", [(i, i ^ d) for i in range(ep_size)])

    def to_twin(v):
        return lax.ppermute(v, "tp", [(0, 1), (1, 0)])

    def block(tokens, grad_out, w_router, w_in, w_out, expert_ids):
        n_tok, d_model = tokens.shape
        n_experts = w_router.shape[1]
        width = w_in.shape[2]
        capacity = (6 * n_tok + 5 * n_experts - 1) // (5 * n_experts)
        cap = (capacity + 7) // 8 * 8
        chunk = width // 3
        tp, ep = lax.axis_index("tp"), lax.axis_index("ep")
        meta = jnp.where(jnp.arange(2) == 0, tp, ep).astype(jnp.int32)

        far_w = {}
        for stage, lo, hi in (("a", 0, 2), ("b", 2, 3)):
            lo, size = lo * chunk, (hi - lo) * chunk
            part_in = lax.dynamic_slice(w_in, (1 - tp, 0, lo), (1, d_model, size))[0]
            part_out = lax.dynamic_slice(w_out, (1 - tp, lo, 0), (1, size, d_model))[0]
            far_w[stage] = to_twin(part_in), to_twin(part_out)

        wg_t = w_router.T
        info, f2, f3 = route_and_dispatch(
            meta, expert_ids[None, :], tokens, grad_out, wg_t, 2, 0, capacity, cap
        )
        f2, f3 = to_ep(f2, 2), to_ep(f3, 3)
        f0, f1, g2, g3, g0, g1 = dispatch(meta, info, tokens, grad_out, ((0, 0), (2, 1), (0, 1)), cap)
        f1 = to_ep(f1, 1)
        g2, g3 = to_ep(g2, 2), to_ep(g3, 3)
        g1 = to_ep(g1, 1)

        part = own_half(meta, f0, f1, w_in, w_out, chunk, 0, ())
        h, da, y, s, x, dy = own_half(meta, f2, f3, w_in, w_out, chunk, 1, part)
        y, s = far_half(x, dy, *far_w["a"], y, s, chunk, None, False)
        grads = finished_grads(meta, x, dy, h, da, w_in.shape[0], chunk)
        ys0, ys1 = far_half(x, dy, *far_w["b"], y, s, chunk, 0, True)
        y2, y3, s2, s3 = far_half(x, dy, *far_w["b"], y, s, chunk, 1, False)

        ys1 = to_ep(ys1, 1)
        y2, y3 = to_ep(y2, 2), to_ep(y3, 3)
        s2, s3 = to_ep(s2, 2), to_ep(s3, 3)
        twin0, twin1 = to_twin(ys0), to_twin(ys1)
        y_mine, s_mine = [(ys0, 0), (ys1, 0), y2, y3], [(ys0, 1), (ys1, 1), s2, s3]
        y_twin = [(twin0, 0), (twin1, 0), to_twin(y2), to_twin(y3)]
        s_twin = [(twin0, 1), (twin1, 1), to_twin(s2), to_twin(s3)]

        grad_w_in, grad_w_out = other_grads(meta, (g0, g1, g2, g3), w_in, w_out, *grads, chunk)

        y_all = {(d, k): v for k, side in enumerate((y_mine, y_twin)) for d, v in enumerate(side)}
        s_all = {(d, k): v for k, side in enumerate((s_mine, s_twin)) for d, v in enumerate(side)}
        s_late = {key: s_all.pop(key) for key in ((2, 1), (3, 1))}
        y_late = {key: y_all.pop(key) for key in ((1, 1), (2, 1), (3, 1))}
        y_first = combine_s(meta, y_all, info, (), n_tok // 2)
        moe_out, dlog, dwg = combine_y(meta, y_late, info, y_first, tokens, grad_out, n_tok // 4)
        dwg = dwg + to_ep(dwg, 1)
        dwg_far = to_ep(dwg, 2)
        dwg = (dwg + dwg_far).T
        so_far = combine_s(meta, s_all, info, (), n_tok // 2)
        grad_tokens = combine_s(meta, s_late, info, (so_far, dlog, wg_t), n_tok // 2)
        return moe_out, grad_tokens, grad_w_in, grad_w_out, dwg

    in_specs = (row_spec, row_spec, P(None, None), P("ep", None, "tp"), P("ep", "tp", None), P(("dp", "ep")))
    out_specs = (row_spec, row_spec, P(("dp", "ep"), None, "tp"), P(("dp", "ep"), "tp", None), P("dp", None))
    return jax.shard_map(block, mesh=mesh, in_specs=in_specs, out_specs=out_specs, check_vma=False)
```

```python
import jax
import jax.numpy as jnp
from jax import lax
from jax.experimental import pallas as pl
from jax.experimental.pallas import tpu as pltpu
from jax.sharding import PartitionSpec as P


GELU_C = 0.7978845608028654
GELU_K = 0.044715
BF16 = jnp.bfloat16
F32 = jnp.float32
VMEM_LIMIT = 67043328
SMALL_VMEM = 56 * 2**20
INFO_ROWS = 16


def nn(a, b):
    return jnp.dot(a, b, preferred_element_type=F32)


def nt(a, b):
    return lax.dot_general(a, b, (((1,), (1,)), ((), ())), preferred_element_type=F32)


def tn(a, b):
    return lax.dot_general(a, b, (((0,), (0,)), ((), ())), preferred_element_type=F32)


def gelu_and_slope(a):
    sq = a * a
    th = jnp.tanh(a * (GELU_C + (GELU_C * GELU_K) * sq))
    up = 1.0 + th
    act = (0.5 * a) * up
    return act, 0.5 * up + act * (1.0 - th) * (GELU_C + (3.0 * GELU_C * GELU_K) * sq)


def hidden_grads(x, dy, wi, wo):
    a = nn(x, wi)
    dh = nt(dy, wo)
    act, slope = gelu_and_slope(a)
    return act.astype(BF16), (dh * slope).astype(BF16)


def params(dims, vmem=VMEM_LIMIT):
    return pltpu.CompilerParams(dimension_semantics=("arbitrary",) * dims, vmem_limit_bytes=vmem)


def cost(flops, mib):
    return pl.CostEstimate(flops=int(flops), bytes_accessed=int(mib * 2**20), transcendentals=0)


def shape(dims, dtype=BF16):
    return jax.ShapeDtypeStruct(dims, dtype)


def whole(dims):
    return pl.BlockSpec(dims, lambda *_: (0,) * len(dims))


def route_tokens(ids, x, wg_t, info_ref, capacity, cap):
    n_experts, n_tok = wg_t.shape[0], x.shape[0]
    step = 256
    logits = nt(wg_t, x)
    raised = jnp.exp(logits - jnp.max(logits, axis=0, keepdims=True))
    prob = raised / jnp.sum(raised, axis=0, keepdims=True)
    hot = ids == lax.broadcasted_iota(jnp.int32, (n_experts, n_tok), 0)
    hot_f = jnp.where(hot, 1.0, 0.0)
    upper = lax.broadcasted_iota(jnp.int32, (step, step), 0) <= lax.broadcasted_iota(jnp.int32, (step, step), 1)
    upper = jnp.where(upper, 1.0, 0.0).astype(BF16)
    carry = jnp.zeros((n_experts, 1), F32)
    for b in range(n_tok // step):
        cols = slice(b * step, (b + 1) * step)
        seen = nn(hot_f[:, cols].astype(BF16), upper) + carry
        carry = seen[:, step - 1 : step]
        pos = jnp.sum(seen * hot_f[:, cols], axis=0, keepdims=True) - 1.0
        slot = ids[:, cols].astype(F32) * cap + pos
        info_ref[0:1, cols] = jnp.where(pos < capacity, slot, -1.0)
    info_ref[1:2, :] = jnp.sum(hot_f * prob, axis=0, keepdims=True)
    info_ref[2:3, :] = ids.astype(F32)
    info_ref[3:8, :] = jnp.zeros((5, n_tok), F32)
    info_ref[8:16, :] = prob


def pick_rows(meta_ref, info_ref, x_ref, gy_ref, first, flip, cap):
    k = jnp.bitwise_xor(meta_ref[0], flip)
    row = lax.broadcasted_iota(jnp.int32, (2 * cap, 1), 0)
    base_a = (jnp.bitwise_xor(meta_ref[1], first) * 2 + k) * cap
    base_b = (jnp.bitwise_xor(meta_ref[1], first + 1) * 2 + k) * cap - cap
    codes = (row + jnp.where(row < cap, base_a, base_b)).astype(F32)
    hit = info_ref[0:1, :] == codes
    pick = jnp.where(hit, 1.0, 0.0).astype(BF16)
    row_gate = jnp.sum(jnp.where(hit, info_ref[1:2, :], 0.0), axis=1, keepdims=True)
    x = nn(pick, x_ref[...]).astype(BF16)
    return x, (row_gate * nn(pick, gy_ref[...])).astype(BF16)


def route_and_dispatch(meta, ids_row, tokens, grad_out, wg_t, first, flip, capacity, cap):
    n_tok, d_model = tokens.shape

    def body(meta_ref, ids_ref, x_ref, wg_ref, gy_hbm, info_ref, out_a, out_b, gy_ref, sem):
        load = pltpu.make_async_copy(gy_hbm, gy_ref, sem)
        load.start()
        route_tokens(ids_ref[...], x_ref[...], wg_ref[...], info_ref, capacity, cap)
        load.wait()
        x, dy = pick_rows(meta_ref, info_ref, x_ref, gy_ref, first, flip, cap)
        out_a[0], out_a[1], out_b[0], out_b[1] = x[:cap], dy[:cap], x[cap:], dy[cap:]

    return pl.pallas_call(
        body,
        grid_spec=pltpu.PrefetchScalarGridSpec(
            num_scalar_prefetch=1,
            grid=(1,),
            in_specs=[whole(ids_row.shape), whole(tokens.shape), whole(wg_t.shape), pl.BlockSpec(memory_space=pl.ANY)],
            out_specs=[whole((INFO_ROWS, n_tok))] + [whole((2, cap, d_model))] * 2,
            scratch_shapes=[pltpu.VMEM((n_tok, d_model), BF16), pltpu.SemaphoreType.DMA],
        ),
        out_shape=[shape((INFO_ROWS, n_tok), F32)] + [shape((2, cap, d_model))] * 2,
        compiler_params=params(1, SMALL_VMEM),
        cost_estimate=cost(8 * cap * n_tok * d_model, 10),
        name="route",
    )(meta, ids_row, tokens, wg_t, grad_out)


def dispatch(meta, info, tokens, grad_out, groups, cap):
    n_tok, d_model = tokens.shape
    count = len(groups)

    def body(meta_ref, info_ref, x_ref, gy_ref, *refs):
        outs, (stage, sems) = refs[: 2 * count], refs[2 * count :]
        g = pl.program_id(0)
        first, flip = groups[0]
        for p in range(1, count):
            first = jnp.where(g == p, groups[p][0], first)
            flip = jnp.where(g == p, groups[p][1], flip)
        x, dy = pick_rows(meta_ref, info_ref, x_ref, gy_ref, first, flip, cap)
        for half in range(2):
            part = slice(half * cap, (half + 1) * cap)
            stage[2 * g + half, 0] = x[part]
            stage[2 * g + half, 1] = dy[part]

        def store(i):
            return pltpu.make_async_copy(stage.at[i], outs[i], sems.at[i])

        for p in range(count):

            @pl.when(g == p)
            def _():
                store(2 * p).start()
                store(2 * p + 1).start()

        @pl.when(g == count - 1)
        def _():
            for i in range(2 * count):
                store(i).wait()

    return pl.pallas_call(
        body,
        grid_spec=pltpu.PrefetchScalarGridSpec(
            num_scalar_prefetch=1,
            grid=(count,),
            in_specs=[whole(info.shape), whole(tokens.shape), whole(tokens.shape)],
            out_specs=[pl.BlockSpec(memory_space=pl.ANY)] * (2 * count),
            scratch_shapes=[
                pltpu.VMEM((2 * count, 2, cap, d_model), BF16),
                pltpu.SemaphoreType.DMA((2 * count,)),
            ],
        ),
        out_shape=[shape((2, cap, d_model))] * (2 * count),
        compiler_params=params(1, SMALL_VMEM),
        cost_estimate=cost(8 * count * cap * n_tok * d_model, 8 + 4 * count),
        name="dispatch",
    )(meta, info, tokens, grad_out)


def own_half(meta, pair_a, pair_b, w_in, w_out, chunk, group, so_far):
    _, d_model, width = w_in.shape
    cap = pair_a.shape[1]
    rows = 2 * cap

    def body(meta_ref, pa, pb, wi, wo, *refs):
        h_ref, da_ref, y_ref, s_ref, x_ref, dy_ref = refs[-6:]
        c = pl.program_id(0)

        @pl.when(c == 0)
        def _():
            x_ref[:cap] = pa[0]
            x_ref[cap:] = pb[0]
            dy_ref[:cap] = pa[1]
            dy_ref[cap:] = pb[1]

        h, da = hidden_grads(x_ref[...], dy_ref[...], wi[0], wo[0])
        h_ref[...] = h
        da_ref[...] = da
        y = nn(h, wo[0])
        s = nt(da, wi[0])

        @pl.when(c == 0)
        def _():
            y_ref[...] = y
            s_ref[...] = s

        @pl.when(c > 0)
        def _():
            y_ref[...] += y
            s_ref[...] += s

    hid = pl.BlockSpec((rows, chunk), lambda c, m: (group, c))
    full = pl.BlockSpec((rows, d_model), lambda c, m: (group, 0))
    return pl.pallas_call(
        body,
        grid_spec=pltpu.PrefetchScalarGridSpec(
            num_scalar_prefetch=1,
            grid=(width // chunk,),
            in_specs=[
                whole(pair_a.shape),
                whole(pair_a.shape),
                pl.BlockSpec((1, d_model, chunk), lambda c, m: (m[0], 0, c)),
                pl.BlockSpec((1, chunk, d_model), lambda c, m: (m[0], c, 0)),
            ]
            + [pl.BlockSpec(memory_space=pl.ANY)] * len(so_far),
            out_specs=[hid, hid] + [full] * 4,
        ),
        out_shape=[shape((2 * rows, width))] * 2
        + [shape((2 * rows, d_model), F32)] * 2
        + [shape((2 * rows, d_model))] * 2,
        input_output_aliases={5 + i: i for i in range(len(so_far))},
        compiler_params=params(1, SMALL_VMEM),
        cost_estimate=cost(8 * rows * width * d_model, 20),
        name="own_half",
    )(meta, pair_a, pair_b, w_in, w_out, *so_far)


def far_half(x, dy, wi, wo, y_in, s_in, chunk, group, joined):
    d_model = x.shape[1]
    cap = x.shape[0] // 4
    width = wi.shape[1]
    steps = width // chunk

    def body(x_ref, dy_ref, wi_ref, wo_ref, y0, s0, *outs):
        h, da = hidden_grads(x_ref[...], dy_ref[...], wi_ref[...], wo_ref[...])
        y = nn(h, wo_ref[...])
        s = nt(da, wi_ref[...])
        c = pl.program_id(1)
        if group is not None:
            y = (y0[...] + y).astype(BF16)
            s = (s0[...] + s).astype(BF16)
            for p in range(2):

                @pl.when(pl.program_id(0) == p)
                def _():
                    y_out, s_out = (outs[p].at[0], outs[p].at[1]) if joined else (outs[p], outs[2 + p])
                    y_out[...] = y
                    s_out[...] = s

            return

        @pl.when(c == 0)
        def _():
            outs[0][...] = y0[...] + y
            outs[1][...] = s0[...] + s

        @pl.when(c > 0)
        def _():
            outs[0][...] += y
            outs[1][...] += s

    blocks, base, rows = (2, 0, 2 * cap) if group is None else (2, 2 * group, cap)
    full = pl.BlockSpec((rows, d_model), lambda p, c: (base + p, 0))
    if group is None:
        out_specs, out_shape = [full] * 2, [shape(x.shape, F32)] * 2
    else:
        dims, count = ((2, cap, d_model), 2) if joined else ((cap, d_model), 4)
        out_specs, out_shape = [whole(dims)] * count, [shape(dims)] * count
    return pl.pallas_call(
        body,
        grid=(blocks, steps),
        in_specs=[
            full,
            full,
            pl.BlockSpec((d_model, chunk), lambda p, c: (0, c)),
            pl.BlockSpec((chunk, d_model), lambda p, c: (c, 0)),
            full,
            full,
        ],
        out_specs=out_specs,
        out_shape=out_shape,
        compiler_params=params(2, SMALL_VMEM if group is None else VMEM_LIMIT),
        cost_estimate=cost(8 * rows * blocks * width * d_model, 10),
        name="far_half",
    )(x, dy, wi, wo, y_in, s_in)


def finished_grads(meta, x, dy, h, da, n_local, chunk):
    rows, d_model = x.shape
    width = h.shape[1]

    def body(meta_ref, x_ref, dy_ref, h_ref, da_ref, gi, go):
        gi[0] = tn(x_ref[...], da_ref[...])
        go[0] = tn(h_ref[...], dy_ref[...])

    hid = pl.BlockSpec((rows, chunk), lambda c, m: (0, c))
    return pl.pallas_call(
        body,
        grid_spec=pltpu.PrefetchScalarGridSpec(
            num_scalar_prefetch=1,
            grid=(width // chunk,),
            in_specs=[whole((rows, d_model))] * 2 + [hid] * 2,
            out_specs=[
                pl.BlockSpec((1, d_model, chunk), lambda c, m: (m[0], 0, c)),
                pl.BlockSpec((1, chunk, d_model), lambda c, m: (m[0], c, 0)),
            ],
        ),
        out_shape=[shape((n_local, d_model, width), F32), shape((n_local, width, d_model), F32)],
        compiler_params=params(1),
        cost_estimate=cost(4 * rows * width * d_model, 25),
        name="finished_grads",
    )(meta, x, dy, h, da)


def other_grads(meta, pairs, w_in, w_out, grad_w_in, grad_w_out, chunk):
    _, d_model, width = w_in.shape
    cap = pairs[0].shape[1]
    rows = len(pairs) * cap

    def body(meta_ref, *refs):
        parts = refs[: len(pairs)]
        wi, wo, _, _, gi, go, x, dy = refs[len(pairs) :]

        @pl.when(pl.program_id(0) == 0)
        def _():
            for p, part in enumerate(parts):
                x[p * cap : (p + 1) * cap, :] = part[0]
                dy[p * cap : (p + 1) * cap, :] = part[1]

        h, da = hidden_grads(x[...], dy[...], wi[0], wo[0])
        gi[0] = tn(x[...], da)
        go[0] = tn(h, dy[...])

    def other(m):
        return 1 - m[0]

    any_spec = pl.BlockSpec(memory_space=pl.ANY)
    wi_spec = pl.BlockSpec((1, d_model, chunk), lambda c, m: (other(m), 0, c))
    wo_spec = pl.BlockSpec((1, chunk, d_model), lambda c, m: (other(m), c, 0))
    return pl.pallas_call(
        body,
        grid_spec=pltpu.PrefetchScalarGridSpec(
            num_scalar_prefetch=1,
            grid=(width // chunk,),
            in_specs=[whole(pairs[0].shape)] * len(pairs) + [wi_spec, wo_spec, any_spec, any_spec],
            out_specs=[wi_spec, wo_spec],
            scratch_shapes=[pltpu.VMEM((rows, d_model), BF16)] * 2,
        ),
        out_shape=[shape(grad_w_in.shape, F32), shape(grad_w_out.shape, F32)],
        input_output_aliases={len(pairs) + 3: 0, len(pairs) + 4: 1},
        compiler_params=params(1),
        cost_estimate=cost(8 * rows * width * d_model, 25),
        name="other_grads",
    )(meta, *pairs, w_in, w_out, grad_w_in, grad_w_out)


def stack_rows(parts, all_rows):
    @pl.when(pl.program_id(0) == 0)
    def _():
        cap = parts[0].shape[0]
        for p, part in enumerate(parts):
            all_rows[p * cap : (p + 1) * cap, :] = part[...]


def piece_pick(meta_ref, info_v, pieces, cap):
    lane = lax.broadcasted_iota(jnp.int32, (1, cap * len(pieces)), 1)
    codes = lane
    for p, (d, k) in enumerate(pieces):
        owner = jnp.bitwise_xor(meta_ref[1], d) * 2 + jnp.bitwise_xor(meta_ref[0], k)
        codes = jnp.where(lane >= p * cap, lane + (owner - p) * cap, codes)
    return jnp.where(info_v[:, 0:1] == codes.astype(F32), 1.0, 0.0).astype(BF16)


def piece_specs(rows):
    specs, arrays = [], []
    for piece in rows:
        if isinstance(piece, tuple):
            array, which = piece
            specs.append(pl.BlockSpec((None,) + array.shape[1:], lambda *_, w=which: (w, 0, 0)))
        else:
            array = piece
            specs.append(whole(array.shape))
        arrays.append(array)
    return specs, arrays, arrays[0].shape[-2]


def combine_y(meta, pieces, info, so_far, tokens, grad_out, block):
    n_tok, d_model = tokens.shape
    keys = list(pieces)
    specs, rows, cap = piece_specs(pieces.values())
    n_experts = INFO_ROWS - 8

    def body(meta_ref, *refs):
        parts = refs[: len(keys)]
        info_ref, so_ref, x_ref, gy_ref, out_ref, dlog_ref, dwg_ref, all_rows = refs[len(keys) :]
        stack_rows(parts, all_rows)
        info_v = info_ref[...].T
        y = nn(piece_pick(meta_ref, info_v, keys, cap), all_rows[...]) + so_ref[...].astype(F32)
        gate = info_v[:, 1:2]
        prob = info_v[:, 8:16]
        hot = info_v[:, 2:3] == lax.broadcasted_iota(jnp.int32, prob.shape, 1).astype(F32)
        out_ref[...] = (gate * y).astype(BF16)
        d_gate = jnp.sum(gy_ref[...].astype(F32) * y, axis=1, keepdims=True)
        dlog = (d_gate * prob * (jnp.where(hot, 1.0, 0.0) - gate)).astype(BF16)
        dlog_ref[...] = dlog
        dwg = tn(dlog, x_ref[...])

        @pl.when(pl.program_id(0) == 0)
        def _():
            dwg_ref[...] = dwg

        @pl.when(pl.program_id(0) > 0)
        def _():
            dwg_ref[...] += dwg

    tok = pl.BlockSpec((block, d_model), lambda b, m: (b, 0))
    return pl.pallas_call(
        body,
        grid_spec=pltpu.PrefetchScalarGridSpec(
            num_scalar_prefetch=1,
            grid=(n_tok // block,),
            in_specs=specs
            + [pl.BlockSpec((INFO_ROWS, block), lambda b, m: (0, b)), tok, tok, tok],
            out_specs=[tok, pl.BlockSpec((block, n_experts), lambda b, m: (b, 0)), whole((n_experts, d_model))],
            scratch_shapes=[pltpu.VMEM((cap * len(keys), d_model), BF16)],
        ),
        out_shape=[shape((n_tok, d_model)), shape((n_tok, n_experts)), shape((n_experts, d_model), F32)],
        compiler_params=params(1),
        cost_estimate=cost(2 * n_tok * cap * len(keys) * d_model, 16),
        name="combine_y",
    )(meta, *rows, info, so_far, tokens, grad_out)


def combine_s(meta, pieces, info, block):
    n_tok = info.shape[1]
    keys = list(pieces)
    specs, rows, cap = piece_specs(pieces.values())
    d_model = rows[0].shape[-1]

    def body(meta_ref, *refs):
        parts = refs[: len(keys)]
        info_ref, out_ref, all_rows = refs[len(keys) :]
        stack_rows(parts, all_rows)
        out_ref[...] = nn(piece_pick(meta_ref, info_ref[...].T, keys, cap), all_rows[...]).astype(BF16)

    return pl.pallas_call(
        body,
        grid_spec=pltpu.PrefetchScalarGridSpec(
            num_scalar_prefetch=1,
            grid=(n_tok // block,),
            in_specs=specs + [pl.BlockSpec((INFO_ROWS, block), lambda b, m: (0, b))],
            out_specs=pl.BlockSpec((block, d_model), lambda b, m: (b, 0)),
            scratch_shapes=[pltpu.VMEM((cap * len(keys), d_model), BF16)],
        ),
        out_shape=shape((n_tok, d_model)),
        compiler_params=params(1),
        cost_estimate=cost(2 * n_tok * cap * len(keys) * d_model, 10),
        name="combine_s",
    )(meta, *rows, info)


def solution(mesh):
    ep_size = mesh.shape["ep"]
    row_spec = P(("dp", "ep"), None)

    def to_ep(v, d):
        return lax.ppermute(v, "ep", [(i, i ^ d) for i in range(ep_size)])

    def to_twin(v):
        return lax.ppermute(v, "tp", [(0, 1), (1, 0)])

    def block(tokens, grad_out, w_router, w_in, w_out, expert_ids):
        n_tok, d_model = tokens.shape
        n_experts = w_router.shape[1]
        width = w_in.shape[2]
        capacity = (6 * n_tok + 5 * n_experts - 1) // (5 * n_experts)
        cap = (capacity + 7) // 8 * 8
        chunk = width // 3
        tp, ep = lax.axis_index("tp"), lax.axis_index("ep")
        meta = jnp.where(jnp.arange(2) == 0, tp, ep).astype(jnp.int32)

        far_w = {}
        for stage, lo, hi in (("a", 0, 2), ("b", 2, 3)):
            lo, size = lo * chunk, (hi - lo) * chunk
            part_in = lax.dynamic_slice(w_in, (1 - tp, 0, lo), (1, d_model, size))[0]
            part_out = lax.dynamic_slice(w_out, (1 - tp, lo, 0), (1, size, d_model))[0]
            far_w[stage] = to_twin(part_in), to_twin(part_out)

        wg_t = w_router.T
        info, f2, f3 = route_and_dispatch(
            meta, expert_ids[None, :], tokens, grad_out, wg_t, 2, 0, capacity, cap
        )
        f2, f3 = to_ep(f2, 2), to_ep(f3, 3)
        f0, f1, g2, g3, g0, g1 = dispatch(meta, info, tokens, grad_out, ((0, 0), (2, 1), (0, 1)), cap)
        f1 = to_ep(f1, 1)
        g2, g3 = to_ep(g2, 2), to_ep(g3, 3)
        g1 = to_ep(g1, 1)

        part = own_half(meta, f0, f1, w_in, w_out, chunk, 0, ())
        h, da, y, s, x, dy = own_half(meta, f2, f3, w_in, w_out, chunk, 1, part)
        y, s = far_half(x, dy, *far_w["a"], y, s, chunk, None, False)
        grads = finished_grads(meta, x, dy, h, da, w_in.shape[0], chunk)
        ys0, ys1 = far_half(x, dy, *far_w["b"], y, s, chunk, 0, True)
        y2, y3, s2, s3 = far_half(x, dy, *far_w["b"], y, s, chunk, 1, False)

        ys1 = to_ep(ys1, 1)
        y2, y3 = to_ep(y2, 2), to_ep(y3, 3)
        s2, s3 = to_ep(s2, 2), to_ep(s3, 3)
        twin0, twin1 = to_twin(ys0), to_twin(ys1)
        y_mine, s_mine = [(ys0, 0), (ys1, 0), y2, y3], [(ys0, 1), (ys1, 1), s2, s3]
        y_twin = [(twin0, 0), (twin1, 0), to_twin(y2), to_twin(y3)]
        s_twin = [(twin0, 1), (twin1, 1), to_twin(s2), to_twin(s3)]

        grad_w_in, grad_w_out = other_grads(meta, (g0, g1, g2, g3), w_in, w_out, *grads, chunk)

        y_all = {(d, k): v for k, side in enumerate((y_mine, y_twin)) for d, v in enumerate(side)}
        s_all = {(d, k): v for k, side in enumerate((s_mine, s_twin)) for d, v in enumerate(side)}
        s_late = {key: s_all.pop(key) for key in ((2, 1), (3, 1))}
        y_late = {key: y_all.pop(key) for key in ((1, 1), (2, 1), (3, 1))}
        y_first = combine_s(meta, y_all, info, n_tok // 2)
        moe_out, dlog, dwg = combine_y(meta, y_late, info, y_first, tokens, grad_out, n_tok // 4)
        dwg_of = [to_ep(dwg, d) for d in (1, 2, 3)]
        dwg = ((dwg + dwg_of[0]) + (dwg_of[1] + dwg_of[2])).T
        so_far = combine_s(meta, s_all, info, n_tok // 2)
        slot = info[0].astype(jnp.int32)
        dx = so_far.astype(F32) + nn(dlog, wg_t)
        for key in ((2, 1), (3, 1)):
            owner = jnp.bitwise_xor(ep, key[0]) * 2 + jnp.bitwise_xor(tp, key[1])
            pick = slot[:, None] - owner * cap == jnp.arange(cap)[None, :]
            dx = dx + nn(pick.astype(BF16), s_late[key])
        grad_tokens = dx.astype(BF16)
        return moe_out, grad_tokens, grad_w_in, grad_w_out, dwg

    in_specs = (row_spec, row_spec, P(None, None), P("ep", None, "tp"), P("ep", "tp", None), P(("dp", "ep")))
    out_specs = (row_spec, row_spec, P(("dp", "ep"), None, "tp"), P(("dp", "ep"), "tp", None), P("dp", None))
    return jax.shard_map(block, mesh=mesh, in_specs=in_specs, out_specs=out_specs, check_vma=False)
```

```python
import jax
import jax.numpy as jnp
from jax import lax
from jax.experimental import pallas as pl
from jax.experimental.pallas import tpu as pltpu
from jax.sharding import PartitionSpec as P


GELU_C = 0.7978845608028654
GELU_K = 0.044715
BF16 = jnp.bfloat16
F32 = jnp.float32
VMEM_LIMIT = 67043328
SMALL_VMEM = 56 * 2**20
INFO_ROWS = 16


def nn(a, b):
    return jnp.dot(a, b, preferred_element_type=F32)


def nt(a, b):
    return lax.dot_general(a, b, (((1,), (1,)), ((), ())), preferred_element_type=F32)


def tn(a, b):
    return lax.dot_general(a, b, (((0,), (0,)), ((), ())), preferred_element_type=F32)


def gelu_and_slope(a):
    sq = a * a
    th = jnp.tanh(a * (GELU_C + (GELU_C * GELU_K) * sq))
    up = 1.0 + th
    act = (0.5 * a) * up
    return act, 0.5 * up + act * (1.0 - th) * (GELU_C + (3.0 * GELU_C * GELU_K) * sq)


def hidden_grads(x, dy, wi, wo):
    a = nn(x, wi)
    dh = nt(dy, wo)
    act, slope = gelu_and_slope(a)
    return act.astype(BF16), (dh * slope).astype(BF16)


def params(dims, vmem=VMEM_LIMIT):
    return pltpu.CompilerParams(dimension_semantics=("arbitrary",) * dims, vmem_limit_bytes=vmem)


def cost(flops, mib):
    return pl.CostEstimate(flops=int(flops), bytes_accessed=int(mib * 2**20), transcendentals=0)


def shape(dims, dtype=BF16):
    return jax.ShapeDtypeStruct(dims, dtype)


def whole(dims):
    return pl.BlockSpec(dims, lambda *_: (0,) * len(dims))


def route_tokens(ids, x, wg_t, info_ref, capacity, cap):
    n_experts, n_tok = wg_t.shape[0], x.shape[0]
    step = 256
    logits = nt(wg_t, x)
    raised = jnp.exp(logits - jnp.max(logits, axis=0, keepdims=True))
    prob = raised / jnp.sum(raised, axis=0, keepdims=True)
    hot = ids == lax.broadcasted_iota(jnp.int32, (n_experts, n_tok), 0)
    hot_f = jnp.where(hot, 1.0, 0.0)
    upper = lax.broadcasted_iota(jnp.int32, (step, step), 0) <= lax.broadcasted_iota(jnp.int32, (step, step), 1)
    upper = jnp.where(upper, 1.0, 0.0).astype(BF16)
    carry = jnp.zeros((n_experts, 1), F32)
    for b in range(n_tok // step):
        cols = slice(b * step, (b + 1) * step)
        seen = nn(hot_f[:, cols].astype(BF16), upper) + carry
        carry = seen[:, step - 1 : step]
        pos = jnp.sum(seen * hot_f[:, cols], axis=0, keepdims=True) - 1.0
        slot = ids[:, cols].astype(F32) * cap + pos
        info_ref[0:1, cols] = jnp.where(pos < capacity, slot, -1.0)
    info_ref[1:2, :] = jnp.sum(hot_f * prob, axis=0, keepdims=True)
    info_ref[2:3, :] = ids.astype(F32)
    info_ref[3:8, :] = jnp.zeros((5, n_tok), F32)
    info_ref[8:16, :] = prob


def pick_rows(meta_ref, info_ref, x_ref, gy_ref, first, flip, cap):
    k = jnp.bitwise_xor(meta_ref[0], flip)
    row = lax.broadcasted_iota(jnp.int32, (2 * cap, 1), 0)
    base_a = (jnp.bitwise_xor(meta_ref[1], first) * 2 + k) * cap
    base_b = (jnp.bitwise_xor(meta_ref[1], first + 1) * 2 + k) * cap - cap
    codes = (row + jnp.where(row < cap, base_a, base_b)).astype(F32)
    hit = info_ref[0:1, :] == codes
    pick = jnp.where(hit, 1.0, 0.0).astype(BF16)
    row_gate = jnp.sum(jnp.where(hit, info_ref[1:2, :], 0.0), axis=1, keepdims=True)
    x = nn(pick, x_ref[...]).astype(BF16)
    return x, (row_gate * nn(pick, gy_ref[...])).astype(BF16)


def route_and_dispatch(meta, ids_row, tokens, grad_out, wg_t, first, flip, capacity, cap):
    n_tok, d_model = tokens.shape

    def body(meta_ref, ids_ref, x_ref, wg_ref, gy_hbm, info_ref, out_a, out_b, gy_ref, sem):
        load = pltpu.make_async_copy(gy_hbm, gy_ref, sem)
        load.start()
        route_tokens(ids_ref[...], x_ref[...], wg_ref[...], info_ref, capacity, cap)
        load.wait()
        x, dy = pick_rows(meta_ref, info_ref, x_ref, gy_ref, first, flip, cap)
        out_a[0], out_a[1], out_b[0], out_b[1] = x[:cap], dy[:cap], x[cap:], dy[cap:]

    return pl.pallas_call(
        body,
        grid_spec=pltpu.PrefetchScalarGridSpec(
            num_scalar_prefetch=1,
            grid=(1,),
            in_specs=[whole(ids_row.shape), whole(tokens.shape), whole(wg_t.shape), pl.BlockSpec(memory_space=pl.ANY)],
            out_specs=[whole((INFO_ROWS, n_tok))] + [whole((2, cap, d_model))] * 2,
            scratch_shapes=[pltpu.VMEM((n_tok, d_model), BF16), pltpu.SemaphoreType.DMA],
        ),
        out_shape=[shape((INFO_ROWS, n_tok), F32)] + [shape((2, cap, d_model))] * 2,
        compiler_params=params(1, SMALL_VMEM),
        cost_estimate=cost(8 * cap * n_tok * d_model, 10),
        name="route",
    )(meta, ids_row, tokens, wg_t, grad_out)


def dispatch(meta, info, tokens, grad_out, groups, cap):
    n_tok, d_model = tokens.shape
    count = len(groups)

    def body(meta_ref, info_ref, x_ref, gy_ref, *refs):
        outs, (stage, sems) = refs[: 2 * count], refs[2 * count :]
        g = pl.program_id(0)
        first, flip = groups[0]
        for p in range(1, count):
            first = jnp.where(g == p, groups[p][0], first)
            flip = jnp.where(g == p, groups[p][1], flip)
        x, dy = pick_rows(meta_ref, info_ref, x_ref, gy_ref, first, flip, cap)
        for half in range(2):
            part = slice(half * cap, (half + 1) * cap)
            stage[2 * g + half, 0] = x[part]
            stage[2 * g + half, 1] = dy[part]

        def store(i):
            return pltpu.make_async_copy(stage.at[i], outs[i], sems.at[i])

        for p in range(count):

            @pl.when(g == p)
            def _():
                store(2 * p).start()
                store(2 * p + 1).start()

        @pl.when(g == count - 1)
        def _():
            for i in range(2 * count):
                store(i).wait()

    return pl.pallas_call(
        body,
        grid_spec=pltpu.PrefetchScalarGridSpec(
            num_scalar_prefetch=1,
            grid=(count,),
            in_specs=[whole(info.shape), whole(tokens.shape), whole(tokens.shape)],
            out_specs=[pl.BlockSpec(memory_space=pl.ANY)] * (2 * count),
            scratch_shapes=[
                pltpu.VMEM((2 * count, 2, cap, d_model), BF16),
                pltpu.SemaphoreType.DMA((2 * count,)),
            ],
        ),
        out_shape=[shape((2, cap, d_model))] * (2 * count),
        compiler_params=params(1, SMALL_VMEM),
        cost_estimate=cost(8 * count * cap * n_tok * d_model, 8 + 4 * count),
        name="disp",
    )(meta, info, tokens, grad_out)


def own_half(meta, pair_a, pair_b, w_in, w_out, chunk, group, so_far):
    _, d_model, width = w_in.shape
    cap = pair_a.shape[1]
    rows = 2 * cap

    def body(meta_ref, pa, pb, wi, wo, *refs):
        h_ref, da_ref, y_ref, s_ref, x_ref, dy_ref = refs[-6:]
        c = pl.program_id(0)

        @pl.when(c == 0)
        def _():
            x_ref[:cap] = pa[0]
            x_ref[cap:] = pb[0]
            dy_ref[:cap] = pa[1]
            dy_ref[cap:] = pb[1]

        h, da = hidden_grads(x_ref[...], dy_ref[...], wi[0], wo[0])
        h_ref[...] = h
        da_ref[...] = da
        y = nn(h, wo[0])
        s = nt(da, wi[0])

        @pl.when(c == 0)
        def _():
            y_ref[...] = y
            s_ref[...] = s

        @pl.when(c > 0)
        def _():
            y_ref[...] += y
            s_ref[...] += s

    hid = pl.BlockSpec((rows, chunk), lambda c, m: (group, c))
    full = pl.BlockSpec((rows, d_model), lambda c, m: (group, 0))
    return pl.pallas_call(
        body,
        grid_spec=pltpu.PrefetchScalarGridSpec(
            num_scalar_prefetch=1,
            grid=(width // chunk,),
            in_specs=[
                whole(pair_a.shape),
                whole(pair_a.shape),
                pl.BlockSpec((1, d_model, chunk), lambda c, m: (m[0], 0, c)),
                pl.BlockSpec((1, chunk, d_model), lambda c, m: (m[0], c, 0)),
            ]
            + [pl.BlockSpec(memory_space=pl.ANY)] * len(so_far),
            out_specs=[hid, hid] + [full] * 4,
        ),
        out_shape=[shape((2 * rows, width))] * 2
        + [shape((2 * rows, d_model), F32)] * 2
        + [shape((2 * rows, d_model))] * 2,
        input_output_aliases={5 + i: i for i in range(len(so_far))},
        compiler_params=params(1, SMALL_VMEM),
        cost_estimate=cost(8 * rows * width * d_model, 20),
        name="own",
    )(meta, pair_a, pair_b, w_in, w_out, *so_far)


def far_half(x, dy, wi, wo, y_in, s_in, chunk, group, joined):
    d_model = x.shape[1]
    cap = x.shape[0] // 4
    width = wi.shape[1]
    steps = width // chunk

    def body(x_ref, dy_ref, wi_ref, wo_ref, y0, s0, *outs):
        h, da = hidden_grads(x_ref[...], dy_ref[...], wi_ref[...], wo_ref[...])
        y = nn(h, wo_ref[...])
        s = nt(da, wi_ref[...])
        c = pl.program_id(1)
        if group is not None:
            y = (y0[...] + y).astype(BF16)
            s = (s0[...] + s).astype(BF16)
            for p in range(2):

                @pl.when(pl.program_id(0) == p)
                def _():
                    y_out, s_out = (outs[p].at[0], outs[p].at[1]) if joined else (outs[p], outs[2 + p])
                    y_out[...] = y
                    s_out[...] = s

            return

        @pl.when(c == 0)
        def _():
            outs[0][...] = y0[...] + y
            outs[1][...] = s0[...] + s

        @pl.when(c > 0)
        def _():
            outs[0][...] += y
            outs[1][...] += s

    blocks, base, rows = (2, 0, 2 * cap) if group is None else (2, 2 * group, cap)
    full = pl.BlockSpec((rows, d_model), lambda p, c: (base + p, 0))
    if group is None:
        out_specs, out_shape = [full] * 2, [shape(x.shape, F32)] * 2
    else:
        dims, count = ((2, cap, d_model), 2) if joined else ((cap, d_model), 4)
        out_specs, out_shape = [whole(dims)] * count, [shape(dims)] * count
    return pl.pallas_call(
        body,
        grid=(blocks, steps),
        in_specs=[
            full,
            full,
            pl.BlockSpec((d_model, chunk), lambda p, c: (0, c)),
            pl.BlockSpec((chunk, d_model), lambda p, c: (c, 0)),
            full,
            full,
        ],
        out_specs=out_specs,
        out_shape=out_shape,
        compiler_params=params(2, SMALL_VMEM if group is None else VMEM_LIMIT),
        cost_estimate=cost(8 * rows * blocks * width * d_model, 10),
        name="far",
    )(x, dy, wi, wo, y_in, s_in)


def finished_grads(meta, x, dy, h, da, n_local, chunk):
    rows, d_model = x.shape
    width = h.shape[1]

    def body(meta_ref, x_ref, dy_ref, h_ref, da_ref, gi, go):
        gi[0] = tn(x_ref[...], da_ref[...])
        go[0] = tn(h_ref[...], dy_ref[...])

    hid = pl.BlockSpec((rows, chunk), lambda c, m: (0, c))
    return pl.pallas_call(
        body,
        grid_spec=pltpu.PrefetchScalarGridSpec(
            num_scalar_prefetch=1,
            grid=(width // chunk,),
            in_specs=[whole((rows, d_model))] * 2 + [hid] * 2,
            out_specs=[
                pl.BlockSpec((1, d_model, chunk), lambda c, m: (m[0], 0, c)),
                pl.BlockSpec((1, chunk, d_model), lambda c, m: (m[0], c, 0)),
            ],
        ),
        out_shape=[shape((n_local, d_model, width), F32), shape((n_local, width, d_model), F32)],
        compiler_params=params(1),
        cost_estimate=cost(4 * rows * width * d_model, 25),
        name="grads_a",
    )(meta, x, dy, h, da)


def other_grads(meta, pairs, w_in, w_out, grad_w_in, grad_w_out, chunk):
    _, d_model, width = w_in.shape
    cap = pairs[0].shape[1]
    rows = len(pairs) * cap

    def body(meta_ref, *refs):
        parts = refs[: len(pairs)]
        wi, wo, _, _, gi, go, x, dy = refs[len(pairs) :]

        @pl.when(pl.program_id(0) == 0)
        def _():
            for p, part in enumerate(parts):
                x[p * cap : (p + 1) * cap, :] = part[0]
                dy[p * cap : (p + 1) * cap, :] = part[1]

        h, da = hidden_grads(x[...], dy[...], wi[0], wo[0])
        gi[0] = tn(x[...], da)
        go[0] = tn(h, dy[...])

    def other(m):
        return 1 - m[0]

    any_spec = pl.BlockSpec(memory_space=pl.ANY)
    wi_spec = pl.BlockSpec((1, d_model, chunk), lambda c, m: (other(m), 0, c))
    wo_spec = pl.BlockSpec((1, chunk, d_model), lambda c, m: (other(m), c, 0))
    return pl.pallas_call(
        body,
        grid_spec=pltpu.PrefetchScalarGridSpec(
            num_scalar_prefetch=1,
            grid=(width // chunk,),
            in_specs=[whole(pairs[0].shape)] * len(pairs) + [wi_spec, wo_spec, any_spec, any_spec],
            out_specs=[wi_spec, wo_spec],
            scratch_shapes=[pltpu.VMEM((rows, d_model), BF16)] * 2,
        ),
        out_shape=[shape(grad_w_in.shape, F32), shape(grad_w_out.shape, F32)],
        input_output_aliases={len(pairs) + 3: 0, len(pairs) + 4: 1},
        compiler_params=params(1),
        cost_estimate=cost(8 * rows * width * d_model, 25),
        name="grads_b",
    )(meta, *pairs, w_in, w_out, grad_w_in, grad_w_out)


def stack_rows(parts, all_rows):
    @pl.when(pl.program_id(0) == 0)
    def _():
        cap = parts[0].shape[0]
        for p, part in enumerate(parts):
            all_rows[p * cap : (p + 1) * cap, :] = part[...]


def piece_pick(meta_ref, info_v, pieces, cap):
    lane = lax.broadcasted_iota(jnp.int32, (1, cap * len(pieces)), 1)
    codes = lane
    for p, (d, k) in enumerate(pieces):
        owner = jnp.bitwise_xor(meta_ref[1], d) * 2 + jnp.bitwise_xor(meta_ref[0], k)
        codes = jnp.where(lane >= p * cap, lane + (owner - p) * cap, codes)
    return jnp.where(info_v[:, 0:1] == codes.astype(F32), 1.0, 0.0).astype(BF16)


def piece_specs(rows):
    specs, arrays = [], []
    for piece in rows:
        if isinstance(piece, tuple):
            array, which = piece
            specs.append(pl.BlockSpec((None,) + array.shape[1:], lambda *_, w=which: (w, 0, 0)))
        else:
            array = piece
            specs.append(whole(array.shape))
        arrays.append(array)
    return specs, arrays, arrays[0].shape[-2]


def combine_y(meta, pieces, info, so_far, tokens, grad_out, block):
    n_tok, d_model = tokens.shape
    keys = list(pieces)
    specs, rows, cap = piece_specs(pieces.values())
    n_experts = INFO_ROWS - 8

    def body(meta_ref, *refs):
        parts = refs[: len(keys)]
        info_ref, so_ref, x_ref, gy_ref, out_ref, dlog_ref, dwg_ref, all_rows = refs[len(keys) :]
        stack_rows(parts, all_rows)
        info_v = info_ref[...].T
        y = nn(piece_pick(meta_ref, info_v, keys, cap), all_rows[...]) + so_ref[...].astype(F32)
        gate = info_v[:, 1:2]
        prob = info_v[:, 8:16]
        hot = info_v[:, 2:3] == lax.broadcasted_iota(jnp.int32, prob.shape, 1).astype(F32)
        out_ref[...] = (gate * y).astype(BF16)
        d_gate = jnp.sum(gy_ref[...].astype(F32) * y, axis=1, keepdims=True)
        dlog = (d_gate * prob * (jnp.where(hot, 1.0, 0.0) - gate)).astype(BF16)
        dlog_ref[...] = dlog
        dwg = tn(dlog, x_ref[...])

        @pl.when(pl.program_id(0) == 0)
        def _():
            dwg_ref[...] = dwg

        @pl.when(pl.program_id(0) > 0)
        def _():
            dwg_ref[...] += dwg

    tok = pl.BlockSpec((block, d_model), lambda b, m: (b, 0))
    return pl.pallas_call(
        body,
        grid_spec=pltpu.PrefetchScalarGridSpec(
            num_scalar_prefetch=1,
            grid=(n_tok // block,),
            in_specs=specs
            + [pl.BlockSpec((INFO_ROWS, block), lambda b, m: (0, b)), tok, tok, tok],
            out_specs=[tok, pl.BlockSpec((block, n_experts), lambda b, m: (b, 0)), whole((n_experts, d_model))],
            scratch_shapes=[pltpu.VMEM((cap * len(keys), d_model), BF16)],
        ),
        out_shape=[shape((n_tok, d_model)), shape((n_tok, n_experts)), shape((n_experts, d_model), F32)],
        compiler_params=params(1),
        cost_estimate=cost(2 * n_tok * cap * len(keys) * d_model, 16),
        name="comb_y",
    )(meta, *rows, info, so_far, tokens, grad_out)


def combine_s(meta, pieces, info, block):
    n_tok = info.shape[1]
    keys = list(pieces)
    specs, rows, cap = piece_specs(pieces.values())
    d_model = rows[0].shape[-1]

    def body(meta_ref, *refs):
        parts = refs[: len(keys)]
        info_ref, out_ref, all_rows = refs[len(keys) :]
        stack_rows(parts, all_rows)
        out_ref[...] = nn(piece_pick(meta_ref, info_ref[...].T, keys, cap), all_rows[...]).astype(BF16)

    return pl.pallas_call(
        body,
        grid_spec=pltpu.PrefetchScalarGridSpec(
            num_scalar_prefetch=1,
            grid=(n_tok // block,),
            in_specs=specs + [pl.BlockSpec((INFO_ROWS, block), lambda b, m: (0, b))],
            out_specs=pl.BlockSpec((block, d_model), lambda b, m: (b, 0)),
            scratch_shapes=[pltpu.VMEM((cap * len(keys), d_model), BF16)],
        ),
        out_shape=shape((n_tok, d_model)),
        compiler_params=params(1),
        cost_estimate=cost(2 * n_tok * cap * len(keys) * d_model, 10),
        name="comb_s",
    )(meta, *rows, info)


def solution(mesh):
    ep_size = mesh.shape["ep"]
    row_spec = P(("dp", "ep"), None)

    def to_ep(v, d):
        return lax.ppermute(v, "ep", [(i, i ^ d) for i in range(ep_size)])

    def to_twin(v):
        return lax.ppermute(v, "tp", [(0, 1), (1, 0)])

    def block(tokens, grad_out, w_router, w_in, w_out, expert_ids):
        n_tok, d_model = tokens.shape
        n_experts = w_router.shape[1]
        width = w_in.shape[2]
        capacity = (6 * n_tok + 5 * n_experts - 1) // (5 * n_experts)
        cap = (capacity + 7) // 8 * 8
        chunk = width // 3
        tp, ep = lax.axis_index("tp"), lax.axis_index("ep")
        meta = jnp.where(jnp.arange(2) == 0, tp, ep).astype(jnp.int32)

        far_w = {}
        for stage, lo, hi in (("a", 0, 2), ("b", 2, 3)):
            lo, size = lo * chunk, (hi - lo) * chunk
            part_in = lax.dynamic_slice(w_in, (1 - tp, 0, lo), (1, d_model, size))[0]
            part_out = lax.dynamic_slice(w_out, (1 - tp, lo, 0), (1, size, d_model))[0]
            far_w[stage] = to_twin(part_in), to_twin(part_out)

        wg_t = w_router.T
        info, f2, f3 = route_and_dispatch(
            meta, expert_ids[None, :], tokens, grad_out, wg_t, 2, 0, capacity, cap
        )
        f2, f3 = to_ep(f2, 2), to_ep(f3, 3)
        f0, f1, g2, g3, g0, g1 = dispatch(meta, info, tokens, grad_out, ((0, 0), (2, 1), (0, 1)), cap)
        f1 = to_ep(f1, 1)
        g2, g3 = to_ep(g2, 2), to_ep(g3, 3)
        g1 = to_ep(g1, 1)

        part = own_half(meta, f0, f1, w_in, w_out, chunk, 0, ())
        h, da, y, s, x, dy = own_half(meta, f2, f3, w_in, w_out, chunk, 1, part)
        y, s = far_half(x, dy, *far_w["a"], y, s, 2 * chunk, None, False)
        grads = finished_grads(meta, x, dy, h, da, w_in.shape[0], chunk)
        ys0, ys1 = far_half(x, dy, *far_w["b"], y, s, chunk, 0, True)
        y2, y3, s2, s3 = far_half(x, dy, *far_w["b"], y, s, chunk, 1, False)

        ys1 = to_ep(ys1, 1)
        y2, y3 = to_ep(y2, 2), to_ep(y3, 3)
        s2, s3 = to_ep(s2, 2), to_ep(s3, 3)
        twin0, twin1 = to_twin(ys0), to_twin(ys1)
        y_mine, s_mine = [(ys0, 0), (ys1, 0), y2, y3], [(ys0, 1), (ys1, 1), s2, s3]
        y_twin = [(twin0, 0), (twin1, 0), to_twin(y2), to_twin(y3)]
        s_twin = [(twin0, 1), (twin1, 1), to_twin(s2), to_twin(s3)]

        grad_w_in, grad_w_out = other_grads(meta, (g0, g1, g2, g3), w_in, w_out, *grads, chunk)

        y_all = {(d, k): v for k, side in enumerate((y_mine, y_twin)) for d, v in enumerate(side)}
        s_all = {(d, k): v for k, side in enumerate((s_mine, s_twin)) for d, v in enumerate(side)}
        s_late = {key: s_all.pop(key) for key in ((2, 1), (3, 1))}
        y_late = {key: y_all.pop(key) for key in ((1, 1), (2, 1), (3, 1))}
        y_first = combine_s(meta, y_all, info, n_tok // 2)
        moe_out, dlog, dwg = combine_y(meta, y_late, info, y_first, tokens, grad_out, n_tok // 4)
        dwg_of = [to_ep(dwg, d) for d in (1, 2, 3)]
        dwg = ((dwg + dwg_of[0]) + (dwg_of[1] + dwg_of[2])).T
        so_far = combine_s(meta, s_all, info, n_tok // 2)
        slot = info[0].astype(jnp.int32)
        dx = so_far.astype(F32) + nn(dlog, wg_t)
        for key in ((2, 1), (3, 1)):
            owner = jnp.bitwise_xor(ep, key[0]) * 2 + jnp.bitwise_xor(tp, key[1])
            pick = slot[:, None] - owner * cap == jnp.arange(cap)[None, :]
            dx = dx + nn(pick.astype(BF16), s_late[key])
        grad_tokens = dx.astype(BF16)
        return moe_out, grad_tokens, grad_w_in, grad_w_out, dwg

    in_specs = (row_spec, row_spec, P(None, None), P("ep", None, "tp"), P("ep", "tp", None), P(("dp", "ep")))
    out_specs = (row_spec, row_spec, P(("dp", "ep"), None, "tp"), P(("dp", "ep"), "tp", None), P("dp", None))
    return jax.shard_map(block, mesh=mesh, in_specs=in_specs, out_specs=out_specs, check_vma=False)
```
